128 devices in a mesh: rep: 1, r: 16 (over y, z), s: 8 (over x, core).
Axes of the slice: x: 4, y: 4, z: 4, core: 2. Of those that a mesh axis runs over, the one named last changes fastest.
Arguments:
- x: bfloat16 [128, 2048, 1024], P(('rep', 'r', 's'))
- dy: bfloat16 [128, 2048, 1024], P(('rep', 'r', 's'))
- w_gate: bfloat16 [2, 1024, 4096], P(None, 's')
- w_up: bfloat16 [2, 1024, 4096], P(None, 's')
- w_down: bfloat16 [2, 4096, 1024], P(None, 's')
- m_w_gate: float32 [2, 1024, 4096], P(None, 's')
- m_w_up: float32 [2, 1024, 4096], P(None, 's')
- m_w_down: float32 [2, 4096, 1024], P(None, 's')
- v_w_gate: float32 [2, 1024, 4096], P(None, 's')
- v_w_up: float32 [2, 1024, 4096], P(None, 's')
- v_w_down: float32 [2, 4096, 1024], P(None, 's')
Outputs:
- output 1: bfloat16 [2, 1024, 4096], P('rep', 's')
- output 2: bfloat16 [2, 1024, 4096], P('rep', 's')
- output 3: bfloat16 [2, 4096, 1024], P('rep', 's')
- output 4: float32 [2, 1024, 4096], P('rep', 's')
- output 5: float32 [2, 1024, 4096], P('rep', 's')
- output 6: float32 [2, 4096, 1024], P('rep', 's')
- output 7: float32 [2, 1024, 4096], P('rep', 's')
- output 8: float32 [2, 1024, 4096], P('rep', 's')
- output 9: float32 [2, 4096, 1024], P('rep', 's')
All inputs are finite; a program needn't handle non-finite values.
Results may differ from the reference program's by a relative error of at most 0.022.
Values are sent between devices in bfloat16 or wider.
A program may use at most 1.5 GiB of HBM per device.

```python
import jax
import jax.numpy as jnp
from jax import lax

SEQUENCES = 128
TOKENS = 2048
D = 1024
FF = 4096
LAYERS = 2
NAMES = ("w_gate", "w_up", "w_down")
SHAPES = {"w_gate": (LAYERS, D, FF), "w_up": (LAYERS, D, FF), "w_down": (LAYERS, FF, D)}


def bump(key, n, height):
    away = (jnp.arange(n, dtype=jnp.int32) - jax.random.randint(key, (), 0, n, jnp.int32)) % n
    return jnp.where(away < n // 8, height, 1.0)


def together(key, own, strength):
    shared = jax.random.normal(key, own.shape[1:], jnp.float32)
    return (own + strength * shared) * lax.rsqrt(1 + strength * strength)


def setup_inputs(seed: int = 0, part: int = 0) -> dict:
    kx, kdy, ka, kb, kz, kf, kh, kl, *keys = jax.random.split(jax.random.key(seed), 8 + 3 * len(NAMES))
    kx, kdy, ka, kb = (jax.random.fold_in(k, part) for k in (kx, kdy, ka, kb))
    kw, km, kv = (keys[i::3] for i in range(3))
    shape = (SEQUENCES, TOKENS, D)
    much_x, much_dy = jax.random.uniform(kz, (2,), jnp.float32, 0.0, 1.0)
    loud = 2.0 ** jax.random.uniform(jax.random.fold_in(kz, 1), (), jnp.float32, -1.0, 2.0)
    layers = 2.0 ** jax.random.uniform(kl, (LAYERS, 1, 1), jnp.float32, -1.0, 1.0)
    x = together(ka, jax.random.normal(kx, shape, jnp.float32), much_x) * bump(kf, D, 4.0)
    dy = together(kb, jax.random.normal(kdy, shape, jnp.float32), much_dy)
    drawn = {"x": x.astype(jnp.bfloat16), "dy": (loud * dy * (SEQUENCES * TOKENS) ** -0.5).astype(jnp.bfloat16)}
    for key, name in zip(kw, NAMES, strict=True):
        w = jax.random.normal(key, SHAPES[name], jnp.float32) * SHAPES[name][1] ** -0.5
        drawn[name] = (w * {"w_gate": 1.0, "w_up": bump(kh, FF, 4.0), "w_down": layers}[name]).astype(jnp.bfloat16)
    for key, name in zip(km, NAMES, strict=True):
        drawn[f"m_{name}"] = 0.1 * jax.random.normal(key, SHAPES[name], jnp.float32)
    for key, name in zip(kv, NAMES, strict=True):
        drawn[f"v_{name}"] = loud * loud * jax.random.uniform(key, SHAPES[name], jnp.float32, 0.05, 0.15)
    return drawn


def matmul(a, w):
    return jnp.dot(a, w, preferred_element_type=jnp.float32).astype(jnp.bfloat16)


def normed(h):
    wide = h.astype(jnp.float32)
    scale = lax.rsqrt(jnp.mean(wide**2, -1, keepdims=True) + 1e-6)
    return (wide * scale).astype(jnp.bfloat16)


def layer(h, w):
    a = normed(h)
    gate = jnp.dot(a, w["w_gate"], preferred_element_type=jnp.float32)
    up = jnp.dot(a, w["w_up"], preferred_element_type=jnp.float32)
    return h + matmul((jax.nn.silu(gate) * up).astype(jnp.bfloat16), w["w_down"])


def adamw(w, m, v, g):
    m = 0.9 * m + 0.1 * g
    v = 0.95 * v + 0.05 * g * g
    step = m * lax.rsqrt(v + 1e-8) + 0.1 * w
    return (w - 0.02 * step).astype(jnp.bfloat16), m, v


def stack(weights, h):
    return lax.scan(lambda h, w: (layer(h, w), None), h, weights)[0]


def reference(x, dy, w_gate, w_up, w_down, m_w_gate, m_w_up, m_w_down, v_w_gate, v_w_up, v_w_down):
    weights = dict(zip(NAMES, (w_gate, w_up, w_down), strict=True))

    def take(so_far, sequence):
        h, by_y = sequence
        _, back = jax.vjp(lambda w: stack(w, h), weights)
        return jax.tree.map(lambda total, term: total + term.astype(jnp.float32), so_far, back(by_y)[0]), None

    none_yet = {name: jnp.zeros(w.shape, jnp.float32) for name, w in weights.items()}
    by_weights, _ = lax.scan(take, none_yet, (x, dy))
    gradients = [by_weights[name].astype(jnp.bfloat16).astype(jnp.float32) for name in NAMES]
    new = [
        adamw(w.astype(jnp.float32), m, v, g)
        for w, m, v, g in zip((w_gate, w_up, w_down), (m_w_gate, m_w_up, m_w_down), (v_w_gate, v_w_up, v_w_down), gradients, strict=True)
    ]
    return tuple(one[which] for which in range(3) for one in new)
```

```python
import functools

import jax
import jax.numpy as jnp
from jax import lax
from jax.experimental import pallas as pl
from jax.experimental.pallas import tpu as pltpu
from jax.sharding import Mesh
from jax.sharding import PartitionSpec as P

NAMES = ("w_gate", "w_up", "w_down")
BF, F32 = jnp.bfloat16, jnp.float32
MESH = pl.DeviceIdType.MESH
N4 = 4


def matmul(a, w):
    return jnp.dot(a, w, preferred_element_type=jnp.float32).astype(jnp.bfloat16)


def normed(h):
    wide = h.astype(jnp.float32)
    scale = lax.rsqrt(jnp.mean(wide**2, -1, keepdims=True) + 1e-6)
    return (wide * scale).astype(jnp.bfloat16)


def layer(h, w):
    a = normed(h)
    gate = jnp.dot(a, w["w_gate"], preferred_element_type=jnp.float32)
    up = jnp.dot(a, w["w_up"], preferred_element_type=jnp.float32)
    return h + matmul((jax.nn.silu(gate) * up).astype(jnp.bfloat16), w["w_down"])


def adamw(w, m, v, g):
    m = 0.9 * m + 0.1 * g
    v = 0.95 * v + 0.05 * g * g
    step = m * lax.rsqrt(v + 1e-8) + 0.1 * w
    return (w - 0.02 * step).astype(jnp.bfloat16), m, v


class Where:
    def __init__(self):
        self.x, self.y, self.z, self.c = (lax.axis_index(a) for a in ("x", "y", "z", "core"))

    def at(self, **by):
        out = {}
        for axis, d in by.items():
            mine = {"x": self.x, "y": self.y, "z": self.z, "core": self.c}[axis]
            n = 2 if axis == "core" else N4
            out[axis] = lax.rem(mine + d, n)
        return out


def greet(ids):
    barrier = pltpu.get_barrier_semaphore()
    for d in ids:
        pl.semaphore_signal(barrier, inc=1, device_id=d, device_id_type=MESH)
    pl.semaphore_wait(barrier, len(ids))


def x_partners(me):
    return [(dx, dc) for dx in range(N4) for dc in range(2) if (dx, dc) != (0, 0)]


def remote(src, dst, ss, rs, to):
    return pltpu.make_async_remote_copy(src_ref=src, dst_ref=dst, send_sem=ss, recv_sem=rs, device_id=to, device_id_type=MESH)


def gather_kernel(layers, wg, wu, wd, gf, uf, df, ssem, rsem, lsem):
    me = Where()
    greet([me.at(x=dx, core=dc) for dx, dc in x_partners(me)] + [me.at(y=d) for d in (1, 2, 3)] + [me.at(z=d) for d in (1, 2, 3)])
    xc = me.x * 2 + me.c
    rows = pl.ds(pl.multiple_of(32 * me.z, 32), 32)

    def cols(c, k):
        return pl.ds(pl.multiple_of(me.y * 1024 + c * 512 + k * 128, 128), 128)

    def first(l, k, q, go):
        for i, (w, f) in enumerate(((wg, gf), (wu, uf))):
            dst = f.at[l, k, me.y, xc, me.z]
            for n, (dx, dc) in enumerate(x_partners(me)):
                c = lax.rem(me.c + dc, 2)
                go(remote(w.at[l, rows, cols(c, k)], dst, ssem.at[q, i, n], rsem.at[q, i, n], me.at(x=dx, core=dc)))
            go(pltpu.make_async_copy(w.at[l, rows, cols(me.c, k)], dst, lsem.at[i]))
        src = wd.at[l, pl.ds(pl.multiple_of(128 * k, 128), 128)]
        for n, dx in enumerate((1, 2, 3)):
            go(remote(src, df.at[l, k, me.x], ssem.at[q, 2, n], rsem.at[q, 2, n], me.at(x=dx)))
        go(pltpu.make_async_copy(src, df.at[l, k, me.x], lsem.at[2]))

    def second(l, k, q, go):
        for n, d in enumerate((1, 2, 3)):
            v = gf.at[l, k, me.y, :, me.z]
            go(remote(v, v, ssem.at[q, 3, n], rsem.at[q, 3, n], me.at(y=d)))
            v = uf.at[l, k, me.y, :, me.z]
            go(remote(v, v, ssem.at[q, 4, n], rsem.at[q, 4, n], me.at(z=d)))

    def third(l, k, q, go):
        for n, d in enumerate((1, 2, 3)):
            v = gf.at[l, k, :, :, me.z]
            go(remote(v, v, ssem.at[q, 5, n], rsem.at[q, 5, n], me.at(z=d)))
            v = uf.at[l, k, me.y]
            go(remote(v, v, ssem.at[q, 6, n], rsem.at[q, 6, n], me.at(y=d)))

    def one(i, _):
        l, k, q = i // 4, i % 4, i % 2
        for stage in (first, second, third):
            stage(l, k, q, lambda c: c.start())
            stage(l, k, q, lambda c: c.wait())
        return 0

    lax.fori_loop(0, layers * 4, one, 0)


def gathered(wg, wu, wd):
    layers = wg.shape[0]
    any_ = pl.BlockSpec(memory_space=pl.ANY)
    return pl.pallas_call(
        functools.partial(gather_kernel, layers),
        out_shape=[
            jax.ShapeDtypeStruct((layers, 4, 4, 8, 4, 32, 128), BF),
            jax.ShapeDtypeStruct((layers, 4, 4, 8, 4, 32, 128), BF),
            jax.ShapeDtypeStruct((layers, 4, 4, 128, 1024), BF),
        ],
        in_specs=[any_] * 3,
        out_specs=[any_] * 3,
        scratch_shapes=[pltpu.SemaphoreType.DMA((2, 7, 8)), pltpu.SemaphoreType.DMA((2, 7, 8)), pltpu.SemaphoreType.DMA((3,))],
        compiler_params=pltpu.CompilerParams(collective_id=1, has_side_effects=True),
        name="gather",
    )(wg, wu, wd)


def solution(mesh):
    fine = Mesh(mesh.devices.reshape(4, 4, 4, 2), ("y", "z", "x", "core"))
    S = ("x", "core")
    R = ("y", "z")

    def summed(term):
        return lax.psum(lax.psum_scatter(term, S, scatter_dimension=0, tiled=True), R)

    def step(x, dy, *arrays):
        weights, m, v = (arrays[i : i + 3] for i in (0, 3, 6))
        layers = weights[0].shape[0]
        gf, uf, df = gathered(*weights)
        c = lax.axis_index("core")

        def both(f):
            o = lax.ppermute(f, "core", [(0, 1), (1, 0)])
            pair = jnp.where(c == 0, jnp.stack([f, o]), jnp.stack([o, f]))
            return pair.transpose(1, 4, 5, 6, 3, 0, 2, 7).reshape(layers, 1024, 4096)

        def rows(f):
            o = lax.ppermute(f, "core", [(0, 1), (1, 0)])
            pair = jnp.where(c == 0, jnp.stack([f, o]), jnp.stack([o, f]))
            return pair.transpose(1, 3, 0, 2, 4, 5).reshape(layers, 4096, 1024)

        whole = dict(zip(NAMES, (both(gf), both(uf), rows(df))))
        full = [{n: whole[n][l] for n in NAMES} for l in range(layers)]
        h, kept = x[0], []
        for number in range(layers):
            kept.append(h)
            h = layer(h, full[number])
        by_h, mine = dy[0], [None] * layers
        for number in reversed(range(layers)):
            _, back = jax.vjp(lambda w, h: layer(h, w), full[number], kept[number])
            by_w, by_h = back(by_h)
            mine[number] = [summed(by_w[name]) for name in NAMES]
        gradients = [jnp.stack([mine[number][i] for number in range(layers)]).astype(jnp.float32) for i in range(3)]
        new = [adamw(w.astype(jnp.float32), m, v, g) for w, m, v, g in zip(weights, m, v, gradients, strict=True)]
        return tuple(one[which] for which in range(3) for one in new)

    states, cut = P(("y", "z", "x", "core"), None, None), P(None, S, None)
    return jax.shard_map(
        step,
        mesh=fine,
        in_specs=(states, states) + (cut,) * 9,
        out_specs=(P(None, S, None),) * 9,
        check_vma=False,
    )
```

```python
import functools

import jax
import jax.numpy as jnp
from jax import lax
from jax.experimental import pallas as pl
from jax.experimental.pallas import tpu as pltpu
from jax.sharding import Mesh
from jax.sharding import PartitionSpec as P

BF, F32 = jnp.bfloat16, jnp.float32
MESH = pl.DeviceIdType.MESH
ANY = pl.BlockSpec(memory_space=pl.ANY)
DMA = pltpu.SemaphoreType.DMA
AXES = ("y", "z", "x", "core")
SIDE = 4
D, FF = 1024, 4096
OWN = 2048
TOKENS = 2 * OWN
CHUNKS = 4
WIDE = 512
TILE = 512
TILES = TOKENS // TILE
MINE = OWN // TILE
START, WAIT = (lambda c: c.start()), (lambda c: c.wait())
LANES, PART, QUARTER, SLOTS = 128, 32, 256, 8
SLICED = (SIDE, 8, SIDE, PART, LANES)
BLOCKS = (SIDE, LANES, D)


def nn(a, b):
    return lax.dot_general(a, b, (((1,), (0,)), ((), ())), preferred_element_type=F32)


def nt(a, b):
    return lax.dot_general(a, b, (((1,), (1,)), ((), ())), preferred_element_type=F32)


def tn(a, b):
    return lax.dot_general(a, b, (((0,), (0,)), ((), ())), preferred_element_type=F32)


def normed(h):
    wide = h.astype(F32)
    scale = lax.rsqrt(jnp.mean(wide**2, -1, keepdims=True) + 1e-6)
    return (wide * scale).astype(BF)


def sigmoid(g):
    return 0.5 * jnp.tanh(0.5 * g) + 0.5


def block(i, n):
    return pl.ds(pl.multiple_of(i * n, n), n)


def when(*conditions):
    return pl.when(functools.reduce(jnp.logical_and, conditions))


class Place:
    def __init__(self):
        self.x, self.y, self.z, self.core = (lax.axis_index(a) for a in ("x", "y", "z", "core"))
        self.xc = self.x * 2 + self.core

    def plus(self, **by):
        return {a: lax.rem(getattr(self, a) + d, 2 if a == "core" else SIDE) for a, d in by.items()}

    def along(self, axis, d):
        return lax.rem(getattr(self, axis) + d, SIDE)


ROW = [(dx, dc) for dx in range(SIDE) for dc in range(2) if (dx, dc) != (0, 0)]
OTHERS = (1, 2, 3)


def greet(me):
    ids = [me.plus(x=dx, core=dc) for dx, dc in ROW] + [me.plus(**{a: d}) for a in ("y", "z") for d in OTHERS]
    barrier = pltpu.get_barrier_semaphore()
    for d in ids:
        pl.semaphore_signal(barrier, inc=1, device_id=d, device_id_type=MESH)
    pl.semaphore_wait(barrier, len(ids))


def remote(src, dst, ss, rs, to):
    return pltpu.make_async_remote_copy(src_ref=src, dst_ref=dst, send_sem=ss, recv_sem=rs, device_id=to, device_id_type=MESH)


class Gather:
    BASE = (0, 14, 17, 23)
    SEMS = 29

    def __init__(self, me, w, f, sems):
        self.me, (self.wg, self.wu, self.wd), (self.gf, self.uf, self.df), (self.ss, self.rs, self.ls) = me, w, f, sems

    def _go(self, act, q, base, copies):
        for n, (src, dst, to) in enumerate(copies, self.BASE[base]):
            act(remote(src, dst, self.ss.at[q, n], self.rs.at[q, n], to))

    def first(self, act, l, k, slot, q):
        me = self.me
        rows = block(me.z, PART)
        both = (self.wg, self.gf.at[slot, me.y, me.xc, me.z]), (self.wu, self.uf.at[slot, me.y, me.xc, me.z])

        def cols(c):
            return block((me.y * 2 + c) * CHUNKS + k, LANES)

        self._go(act, q, 0, [(w.at[l, rows, cols(lax.rem(me.core + dc, 2))], to, me.plus(x=dx, core=dc)) for dx, dc in ROW for w, to in both])
        for i, (w, to) in enumerate(both):
            act(pltpu.make_async_copy(w.at[l, rows, cols(me.core)], to, self.ls.at[q, i]))

    def down(self, act, l, k, slot, q):
        src, dst = self.wd.at[l, block(k, LANES)], self.df.at[slot, self.me.x]
        self._go(act, q, 1, [(src, dst, self.me.plus(x=d)) for d in OTHERS])
        act(pltpu.make_async_copy(src, dst, self.ls.at[q, 2]))

    def second(self, act, slot, q):
        me = self.me
        g, u = (f.at[slot, me.y, :, me.z] for f in (self.gf, self.uf))
        self._go(act, q, 2, [c for d in OTHERS for c in ((g, g, me.plus(y=d)), (u, u, me.plus(z=d)))])

    def third(self, act, slot, q):
        me = self.me
        g, u = self.gf.at[slot, :, :, me.z], self.uf.at[slot, me.y]
        self._go(act, q, 3, [c for d in OTHERS for c in ((g, g, me.plus(z=d)), (u, u, me.plus(y=d)))])

    def load(self, act, slot, v, sem):
        load(act, (self.gf, self.uf, self.df), slot, v, sem)


def load(act, f, slot, v, sem):
    src, to = slot
    for i in range(3):
        act(pltpu.make_async_copy(f[i].at[src], v[i].at[to], sem.at[i]))


def gather_scratch(chunks):
    return [DMA((chunks, Gather.SEMS)), DMA((chunks, Gather.SEMS)), DMA((chunks, 3))]


def matrix(v, slot):
    return jnp.concatenate([v[slot, u].reshape(D, LANES) for u in range(SIDE)], axis=1)


class Reduce:
    BASE = (0, 9, 18, 35, 44)
    SEMS = (2, 53)

    @staticmethod
    def scratch():
        v = pltpu.VMEM
        held = lambda *s: v(s, BF)
        came = lambda *s: v((2, 3) + s, BF)
        return [
            held(*SLICED), held(*SLICED), held(*BLOCKS),
            came(8, SIDE, PART, LANES), came(SIDE, 8, PART, LANES), came(LANES, D),
            held(8, SIDE, PART, LANES), held(SIDE, 8, PART, LANES), held(LANES, D),
            came(8, PART, LANES), came(8, PART, LANES), came(PART, D),
            held(8, PART, LANES), held(8, PART, LANES), held(PART, D),
            v((2, 8, PART, LANES), BF), v((2, 8, PART, LANES), BF), came(PART, QUARTER),
            held(2, PART, LANES), held(2, PART, LANES), held(PART, QUARTER),
            DMA(Reduce.SEMS), DMA(Reduce.SEMS), DMA((2, 3)),
        ]

    def __init__(self, me, scratch, out):
        self.me, self.out = me, out
        self.w, self.r1, self.b1, self.r2, self.b2, self.r3, self.b3 = (scratch[3 * i : 3 * i + 3] for i in range(7))
        self.ss, self.rs, self.ls = scratch[-3:]

    def put(self, g, u, d):
        for w, acc in ((self.w[0], g), (self.w[1], u)):
            for i in range(SIDE):
                w[i] = acc[:, LANES * i : LANES * (i + 1)].astype(BF).reshape(8, SIDE, PART, LANES)
        self.w[2][...] = d[...].astype(BF).reshape(BLOCKS)

    def copies(self, stage, slot, q):
        me = self.me
        (g, u, d), row = self.out, block(me.y, PART)
        if stage == 1:
            for n, by in enumerate(OTHERS):
                y, z, x = (me.along(a, by) for a in ("y", "z", "x"))
                yield self.w[0].at[y], self.r1[0].at[q, n], me.plus(y=by)
                yield self.w[1].at[:, :, z], self.r1[1].at[q, n], me.plus(z=by)
                yield self.w[2].at[x], self.r1[2].at[q, n], me.plus(x=by)
        elif stage == 2:
            for n, by in enumerate(OTHERS):
                y, z = (me.along(a, by) for a in ("y", "z"))
                yield self.b1[0].at[:, z], self.r2[0].at[q, n], me.plus(z=by)
                yield self.b1[1].at[y], self.r2[1].at[q, n], me.plus(y=by)
                yield self.b1[2].at[block(y, PART)], self.r2[2].at[q, n], me.plus(y=by)
        elif stage == 3:
            for dx, dc in ROW:
                x, c = me.along("x", dx), lax.rem(me.core + dc, 2)
                for i in range(2):
                    yield self.b2[i].at[2 * x + c], self.r3[i].at[q, me.xc], me.plus(x=dx, core=dc)
            for n, by in enumerate(OTHERS):
                cols = block(me.along("z", by), QUARTER)
                yield self.b2[2].at[:, cols], self.r3[2].at[q, n], me.plus(z=by)
        elif stage == 4:
            for by in OTHERS:
                yield self.b3[0], g.at[slot, :, me.y, me.z], me.plus(z=by)
                yield self.b3[1], u.at[slot, :, me.y, me.z], me.plus(y=by)
                yield self.b3[2], d.at[slot, row, block(me.z, QUARTER)], me.plus(z=by)
        else:
            for by in OTHERS:
                yield g.at[slot, :, me.y], g.at[slot, :, me.y], me.plus(y=by)
                yield u.at[slot, :, :, me.z], u.at[slot, :, :, me.z], me.plus(z=by)
                yield d.at[slot, row], d.at[slot, row], me.plus(y=by)

    def send(self, stage, act, slot, q):
        me = self.me
        for n, (src, dst, to) in enumerate(self.copies(stage, slot, q)):
            n += self.BASE[stage - 1]
            act(remote(src, dst, self.ss.at[q, n], self.rs.at[q, n], to))
        if stage == SIDE:
            g, u, d = self.out
            ends = g.at[slot, :, me.y, me.z], u.at[slot, :, me.y, me.z], d.at[slot, block(me.y, PART), block(me.z, QUARTER)]
            for i, dst in enumerate(ends):
                act(pltpu.make_async_copy(self.b3[i], dst, self.ls.at[q, i]))

    def add(self, stage, q):
        me = self.me
        cols = block(me.z, QUARTER)
        if stage == 3:
            for r, b, own in zip(self.r3[:2], self.b3, self.b2):
                r[q, me.xc] = own[me.xc]
                for c in range(2):
                    total = r[q, c].astype(F32)
                    for x in OTHERS:
                        total += r[q, 2 * x + c].astype(F32)
                    b[c] = total.astype(BF)
            parts = ((self.b2[2].at[:, cols], self.r3[2], self.b3[2]),)
        elif stage == 2:
            own = self.b1[0].at[:, me.z], self.b1[1].at[me.y], self.b1[2].at[block(me.y, PART)]
            parts = zip(own, self.r2, self.b2)
        else:
            own = self.w[0].at[me.y], self.w[1].at[:, :, me.z], self.w[2].at[me.x]
            parts = zip(own, self.r1, self.b1)
        for own, r, b in parts:
            total = own[...].astype(F32)
            for n in range(3):
                total += r[q, n].astype(F32)
            b[...] = total.astype(BF)

    def turn(self, stage, slot, q):
        self.send(stage, WAIT, slot, q)
        if stage < SIDE:
            self.add(stage, q)
        self.send(stage + 1, START, slot, q)


def reduced_shapes(n):
    s = jax.ShapeDtypeStruct((n, 2, SIDE, SIDE, PART, LANES), BF)
    return [s, s, jax.ShapeDtypeStruct((n, LANES, D), BF)]


def gathered_shapes(n):
    s = jax.ShapeDtypeStruct((n,) + SLICED, BF)
    return [s, s, jax.ShapeDtypeStruct((n,) + BLOCKS, BF)]


def chunk_buffers():
    return [pltpu.VMEM((2,) + SLICED, BF)] * 2 + [pltpu.VMEM((2,) + BLOCKS, BF)]


def tile_of(i):
    k, t = i // TILES, i % TILES
    return jnp.where(k == CHUNKS - 1, (t + MINE) % TILES, t)


def rows_of(tile):
    return block(tile, TILE)


def params(collective_id):
    return pltpu.CompilerParams(collective_id=collective_id, has_side_effects=True, vmem_limit_bytes=66_000_000, dimension_semantics=("arbitrary",))


def forward_kernel(x, dy, wg, wu, wd, g_out, u_out, a_out, h_out, n_out, dyp, gf, uf, df, a, xv, acc, prt, vg, vu, vd, ss, rs, ls, wsem, csem, esem, psem):
    i = pl.program_id(0)
    k, t = i // TILES, i % TILES
    me = Place()
    ga = Gather(me, (wg, wu, wd), (gf, uf, df), (ss, rs, ls))
    v = (vg, vu, vd)
    other = me.plus(core=1)
    mine, theirs = pl.ds(0, OWN), pl.ds(OWN, OWN)
    to_dy = remote(dy, dyp, esem.at[0], esem.at[1], other)
    to_a = remote(a.at[mine], a.at[theirs], esem.at[2], esem.at[3], other)
    save_a = pltpu.make_async_copy(a, a_out, csem.at[0])

    def spread(m, act, stage):
        if stage in ("first", "down"):
            getattr(ga, stage)(act, m // CHUNKS, m % CHUNKS, m, m)
        else:
            getattr(ga, stage)(act, m, m)

    def part(tile):
        return remote(acc.at[rows_of(tile)], prt.at[rows_of(tile - MINE)], psem.at[0, tile - MINE], psem.at[1, tile - MINE], other)

    @pl.when(i == 0)
    def _():
        fetch = pltpu.make_async_copy(x, xv, csem.at[1])
        fetch.start()
        greet(me)
        for m in range(3):
            spread(m, START, "first")
        spread(0, START, "down")
        fetch.wait()

        def norm(j, _):
            r = block(j, QUARTER)
            a[r] = normed(xv[r])
            return 0

        lax.fori_loop(0, OWN // QUARTER, norm, 0)
        spread(0, WAIT, "first")
        spread(0, START, "second")
        to_a.start()
        spread(0, WAIT, "second")
        spread(0, START, "third")
        spread(1, WAIT, "first")
        spread(1, START, "second")
        spread(0, WAIT, "third")
        spread(0, WAIT, "down")
        ga.load(START, (0, 0), v, wsem)

    @pl.when(t == 0)
    def _():
        ga.load(WAIT, (k, k % 2), v, wsem)
        spread(k + 1, WAIT, "second")
        spread(k + 1, START, "third")
        spread(k + 1, START, "down")

        @pl.when(k < 3)
        def _():
            spread(k + 2, WAIT, "first")
            spread(k + 2, START, "second")

        @pl.when(k < 2)
        def _():
            spread(k + 3, START, "first")

    @pl.when(i == MINE)
    def _():
        to_a.wait()
        save_a.start()
        to_dy.start()

    @when(t == TILES - 1, k < CHUNKS - 1)
    def _():
        spread(k + 1, WAIT, "third")
        spread(k + 1, WAIT, "down")
        ga.load(START, (k + 1, (k + 1) % 2), v, wsem)

    @when(k == CHUNKS - 1, t >= 1, t <= MINE)
    def _():
        part(t - 1 + MINE).start()

    tile = tile_of(i)
    rows = rows_of(tile)
    s = k % 2
    at = a[rows]
    g = nn(at, matrix(vg, s))
    u = nn(at, matrix(vu, s))
    g_out[0] = g
    u_out[0] = u
    hidden = (g * sigmoid(g) * u).astype(BF)
    acc[rows] = jnp.where(k == 0, 0.0, acc[rows]) + nn(hidden, vd[s].reshape(WIDE, D))

    @pl.when(i == CHUNKS * TILES - 1)
    def _():
        save_a.wait()
        for j in range(MINE):
            part(MINE + j).wait()

        def end(j, _):
            r = block(j, QUARTER)
            h = (xv[r].astype(F32) + (acc[r] + prt[r]).astype(BF).astype(F32)).astype(BF)
            xv[r] = h
            a[r] = normed(h)
            return 0

        lax.fori_loop(0, OWN // QUARTER, end, 0)
        keep = pltpu.make_async_copy(xv, h_out, csem.at[1])
        keep2 = pltpu.make_async_copy(a.at[mine], n_out, csem.at[2])
        keep.start()
        keep2.start()
        to_dy.wait()
        spread(CHUNKS, WAIT, "third")
        spread(CHUNKS, WAIT, "down")
        keep.wait()
        keep2.wait()


def forward(x, dy, weights):
    steps = CHUNKS * TILES
    wide = pl.BlockSpec((1, TILE, WIDE), lambda i: (i // TILES, tile_of(i), 0))
    big = jax.ShapeDtypeStruct((CHUNKS, TOKENS, WIDE), F32)
    own = jax.ShapeDtypeStruct((OWN, D), BF)
    return pl.pallas_call(
        forward_kernel,
        grid=(steps,),
        in_specs=[ANY] * 5,
        out_specs=[wide, wide] + [ANY] * 7,
        out_shape=[big, big, jax.ShapeDtypeStruct((TOKENS, D), BF), own, own, own] + gathered_shapes(CHUNKS + 1),
        scratch_shapes=[
            pltpu.VMEM((TOKENS, D), BF), pltpu.VMEM((OWN, D), BF), pltpu.VMEM((TOKENS, D), F32), pltpu.VMEM((OWN, D), F32),
            *chunk_buffers(), *gather_scratch(CHUNKS + 1), DMA((3,)), DMA((3,)), DMA((4,)), DMA((2, MINE)),
        ],
        compiler_params=params(1),
        name="forward",
    )(x, dy, *weights)


def gradients_of(g, u, dh):
    s = sigmoid(g)
    si = g * s
    return (si * u).astype(BF), (dh * u * (s + si * (1 - s))).astype(BF), (dh * si).astype(BF)


def middle_kernel(dy, dyp, n, g4, u4, d4, wg, wu, wd, dao, dar, rg, ru, rd, kg, ku, kd, gf, uf, df, *scratch):
    a, da, ag, au, ad, vg, vu, vd, ss, rs, ls, wsem, csem, esem, psem, *rest = scratch
    i = pl.program_id(0)
    k, t = i // TILES, i % TILES
    me = Place()
    ga = Gather(me, (wg, wu, wd), (gf, uf, df), (ss, rs, ls))
    re = Reduce(me, rest, (rg, ru, rd))
    v = (vg, vu, vd)
    other = me.plus(core=1)
    mine, theirs = block(0, OWN), block(1, OWN)
    to_a = remote(n, a.at[theirs], esem.at[0], esem.at[1], other)
    last = CHUNKS - 1

    def part(tile):
        return remote(da.at[rows_of(tile)], dar.at[rows_of(tile - MINE)], psem.at[0, tile - MINE], psem.at[1, tile - MINE], other)

    def keep(tile):
        return pltpu.make_async_copy(da.at[rows_of(tile)], dao.at[rows_of(tile)], csem.at[tile])

    def bring(stage, act, c):
        if stage in ("first", "down"):
            getattr(ga, stage)(act, 1, c + 1, c, c)
        else:
            getattr(ga, stage)(act, c, c)

    @when(i == 0)
    def _():
        fetch = pltpu.make_async_copy(n, a.at[mine], csem.at[0])
        fetch.start()
        load(START, (g4, u4, d4), (CHUNKS, 0), v, wsem)
        greet(me)
        to_a.start()
        for c in range(last):
            bring("first", START, c)
        bring("down", START, 0)
        fetch.wait()
        load(WAIT, (g4, u4, d4), (CHUNKS, 0), v, wsem)

    @when(t == 0, k > 0)
    def _():
        ga.load(WAIT, (k - 1, k % 2), v, wsem)
        re.send(1, START, k - 1, k % 2)

    for stage, at_step in ((1, 3), (2, 5), (3, 6), (4, 7)):

        @when(t == at_step, k > 0)
        def _(stage=stage):
            re.turn(stage, k - 1, k % 2)

    @when(t == 1, k > 1)
    def _():
        re.send(5, WAIT, k - 2, (k - 1) % 2)

    @when(i == 1)
    def _():
        for c in range(last):
            bring("first", WAIT, c)
            bring("second", START, c)

    @when(i == 3)
    def _():
        for c in range(last):
            bring("second", WAIT, c)
        bring("third", START, 0)
        bring("down", START, 1)

    @when(i == MINE)
    def _():
        to_a.wait()

    @when(i == 5)
    def _():
        bring("third", START, 1)

    @when(i == TILES - 1)
    def _():
        bring("third", WAIT, 0)
        bring("down", WAIT, 0)

    @when(i == TILES)
    def _():
        bring("third", START, 2)
        bring("down", START, 2)

    @when(i == TILES + 2)
    def _():
        bring("third", WAIT, 1)
        bring("down", WAIT, 1)

    @when(i == 2 * TILES)
    def _():
        bring("third", WAIT, 2)
        bring("down", WAIT, 2)

    @when(t == TILES - 1, k < last)
    def _():
        ga.load(START, (k, (k + 1) % 2), v, wsem)

    @when(k == last, t >= 1, t <= MINE)
    def _():
        part(t - 1 + MINE).start()

    @when(k == last, t > MINE)
    def _():
        keep(t - 1 - MINE).start()

    tile = tile_of(i)
    rows = rows_of(tile)
    s = k % 2
    at = a[rows]
    by = jnp.where(tile < MINE, dy[...], dyp[...])
    mg, mu, md = matrix(vg, s), matrix(vu, s), vd[s].reshape(WIDE, D)
    hidden, dg, du = gradients_of(nn(at, mg), nn(at, mu), nt(by, md).astype(BF).astype(F32))
    fresh = t == 0
    ag[...] = jnp.where(fresh, 0, ag[...]) + tn(at, dg)
    au[...] = jnp.where(fresh, 0, au[...]) + tn(at, du)
    ad[...] = jnp.where(fresh, 0, ad[...]) + tn(hidden, by)
    da[rows] = jnp.where(k == 0, 0, da[rows]) + (nt(dg, mg) + nt(du, mu))

    @when(t == TILES - 1)
    def _():
        re.put(ag, au, ad)

    @when(i == CHUNKS * TILES - 1)
    def _():
        keep(MINE - 1).start()
        outs = [pltpu.make_async_copy(re.w[j], (kg, ku, kd)[j], wsem.at[j]) for j in range(3)]
        for o in outs:
            o.start()
        for j in range(MINE):
            keep(j).wait()
            part(MINE + j).wait()
        for o in outs:
            o.wait()
        re.send(5, WAIT, last - 1, last % 2)


def middle(dy, dyp, n, f4, weights):
    near = pl.BlockSpec((TILE, D), lambda i: (jnp.minimum(tile_of(i), MINE - 1), 0))
    far = pl.BlockSpec((TILE, D), lambda i: (jnp.maximum(tile_of(i) - MINE, 0), 0))
    half = jax.ShapeDtypeStruct((OWN, D), F32)
    raw = jax.ShapeDtypeStruct(SLICED, BF)
    outs = [half, half, *reduced_shapes(SLOTS), raw, raw, jax.ShapeDtypeStruct(BLOCKS, BF)]
    shapes = outs + gathered_shapes(CHUNKS - 1)
    return pl.pallas_call(
        middle_kernel,
        grid=(CHUNKS * TILES,),
        in_specs=[near, far] + [ANY] * (1 + 3 + 3),
        out_specs=[ANY] * len(shapes),
        out_shape=shapes,
        scratch_shapes=[
            pltpu.VMEM((TOKENS, D), BF), pltpu.VMEM((TOKENS, D), F32), *sums(),
            *chunk_buffers(), *gather_scratch(CHUNKS - 1), DMA((3,)), DMA((MINE,)), DMA((2,)), DMA((2, MINE)), *Reduce.scratch(),
        ],
        compiler_params=params(2),
        name="middle",
    )(dy, dyp, n, *f4, *weights)[: len(outs)]


def sums():
    return [pltpu.VMEM((D, WIDE), F32), pltpu.VMEM((D, WIDE), F32), pltpu.VMEM((WIDE, D), F32)]


def back_kernel(g_in, u_in, a_in, down, dao, dar, h, dy, kg, ku, kd, *refs):
    sums_, scratch = refs[3:6], refs[6:]
    b, ag, au, ad, pf, pb, csem, esem, dsem = scratch[:9]
    i = pl.program_id(0)
    k, t = i // TILES, i % TILES
    me = Place()
    re = Reduce(me, scratch[9:], sums_)
    to_b = remote(b.at[block(0, OWN)], b.at[block(1, OWN)], esem.at[0], esem.at[1], me.plus(core=1))
    begun = CHUNKS - 1

    @when(i == 0)
    def _():
        raws = [pltpu.make_async_copy((kg, ku, kd)[j], re.w[j], csem.at[j]) for j in range(3)]
        for o in raws:
            o.start()

        def piece(act, j):
            r, s = block(j, QUARTER), j % 2
            for n, (src, dst) in enumerate(((dao, pf.at[s, 0]), (dar, pf.at[s, 1]), (h, pb.at[s, 0]), (dy, pb.at[s, 1]))):
                act(pltpu.make_async_copy(src.at[r], dst, dsem.at[s, n]))

        piece(START, 0)
        greet(me)
        for o in raws:
            o.wait()
        re.send(1, START, begun, 0)

        def one(j, _):
            @when(j + 1 < OWN // QUARTER)
            def _():
                piece(START, j + 1)

            piece(WAIT, j)
            s = j % 2
            by_a = (pf[s, 0] + pf[s, 1]).astype(BF)
            by_h = jax.vjp(normed, pb[s, 0])[1](by_a)[0]
            b[block(j, QUARTER)] = (pb[s, 1].astype(F32) + by_h.astype(F32)).astype(BF)
            return 0

        lax.fori_loop(0, OWN // QUARTER, one, 0)
        to_b.start()

    @when(i == MINE)
    def _():
        to_b.wait()

    now, before, q = begun + k, begun + k - 1, k % 2

    @when(t == 0, k > 0)
    def _():
        re.send(1, START, now, q)

    @when(t == 1, k > 0)
    def _():
        @when(k > 1)
        def _():
            re.send(5, WAIT, before - 1, q)

        re.turn(3, before, 1 - q)

    @when(t == 5)
    def _():
        re.turn(1, now, q)

        @when(k > 0)
        def _():
            re.turn(4, before, 1 - q)

    @when(t == 7)
    def _():
        re.turn(2, now, q)

    at, by = a_in[...], b[rows_of(tile_of(i))]
    hidden, dg, du = gradients_of(g_in[0], u_in[0], nt(by, down[0].reshape(WIDE, D)).astype(BF).astype(F32))
    fresh = t == 0
    ag[...] = jnp.where(fresh, 0, ag[...]) + tn(at, dg)
    au[...] = jnp.where(fresh, 0, au[...]) + tn(at, du)
    ad[...] = jnp.where(fresh, 0, ad[...]) + tn(hidden, by)

    @when(t == TILES - 1)
    def _():
        re.put(ag, au, ad)

    @when(i == CHUNKS * TILES - 1)
    def _():
        end = SLOTS - 1
        q, p = CHUNKS % 2, 1 - CHUNKS % 2
        re.send(1, START, end, q)
        re.send(5, WAIT, end - 2, q)
        re.turn(3, end - 1, p)
        re.turn(1, end, q)
        re.turn(4, end - 1, p)
        for stage in (2, 3, 4):
            re.turn(stage, end, q)
        re.send(5, WAIT, end - 1, p)
        re.send(5, WAIT, end, q)


def backward(g, u, a, down, half, raw, sums_):
    wide = pl.BlockSpec((1, TILE, WIDE), lambda i: (i // TILES, tile_of(i), 0))
    blocks = [wide, wide, pl.BlockSpec((TILE, D), lambda i: (tile_of(i), 0)), pl.BlockSpec((1,) + BLOCKS, lambda i: (i // TILES, 0, 0, 0))]
    args = (g, u, a, down, *half, *raw, *sums_)
    at = len(args) - len(sums_)
    return pl.pallas_call(
        back_kernel,
        grid=(CHUNKS * TILES,),
        in_specs=blocks + [ANY] * (len(args) - len(blocks)),
        out_specs=[ANY] * len(sums_),
        out_shape=reduced_shapes(SLOTS),
        input_output_aliases={at + i: i for i in range(len(sums_))},
        scratch_shapes=[
            pltpu.VMEM((TOKENS, D), BF), *sums(), pltpu.VMEM((2, 2, QUARTER, D), F32), pltpu.VMEM((2, 2, QUARTER, D), BF),
            DMA((3,)), DMA((2,)), DMA((2, 4)), *Reduce.scratch(),
        ],
        compiler_params=params(3),
        name="backward",
    )(*args)


def adamw(w, m, v, g):
    m = 0.9 * m + 0.1 * g
    v = 0.95 * v + 0.05 * g * g
    step = m * lax.rsqrt(v + 1e-8) + 0.1 * w
    return (w - 0.02 * step).astype(BF), m, v


def update_kernel(gg, gu, gd, *refs):
    ins, outs = refs[:9], refs[9:]
    deep = gd[0]
    sides = [jnp.concatenate([r[k, 0, 0].reshape(LANES, LANES) for k in range(CHUNKS)], axis=1) for r in (gg, gu)]
    for n, g in enumerate((*sides, deep)):
        w, m, v = (r[0] for r in ins[n::3])
        for out, new in zip(outs[n::3], adamw(w.astype(F32), m, v, g.astype(F32))):
            out[0] = new


def update(sums_, arrays):
    half = LANES // 2
    side = pl.BlockSpec((1, LANES, WIDE), lambda i: (i // SLOTS, 0, i % SLOTS))
    deep = pl.BlockSpec((1, half, D), lambda i: (i // SLOTS, i % SLOTS, 0))
    part = pl.BlockSpec((CHUNKS, 1, 1, SIDE, PART, LANES), lambda i: (1 - i // SLOTS, i % 2, i % SLOTS // 2, 0, 0, 0))
    down = pl.BlockSpec((1, half, D), lambda i: ((1 - i // SLOTS) * CHUNKS + i % SLOTS // 2, i % 2, 0))
    return pl.pallas_call(
        update_kernel,
        grid=(2 * SLOTS,),
        in_specs=[part, part, down] + [side, side, deep] * 3,
        out_specs=[side, side, deep] * 3,
        out_shape=[jax.ShapeDtypeStruct(x.shape, x.dtype) for x in arrays],
        compiler_params=pltpu.CompilerParams(vmem_limit_bytes=66_000_000, dimension_semantics=("arbitrary",)),
        name="update",
    )(*sums_, *arrays)


def solution(mesh):
    fine = Mesh(mesh.devices.reshape(SIDE, SIDE, SIDE, 2), AXES)

    def step(x, dy, *arrays):
        x, dy, weights = x[0], dy[0], arrays[:3]
        g0, u0, a0, h1, n1, dyp, *f = forward(x, dy, weights)
        dao, dar, *rest = middle(dy, dyp, n1, f, weights)
        return update(backward(g0, u0, a0, f[2], (dao, dar, h1, dy), rest[3:], rest[:3]), arrays)

    states, cut = P(AXES, None, None), P(None, ("x", "core"), None)
    return jax.shard_map(
        step,
        mesh=fine,
        in_specs=(states, states) + (cut,) * 9,
        out_specs=(cut,) * 9,
        check_vma=False,
    )
```

```python
import functools

import jax
import jax.numpy as jnp
from jax import lax
from jax.experimental import pallas as pl
from jax.experimental.pallas import tpu as pltpu
from jax.sharding import Mesh
from jax.sharding import PartitionSpec as P

BF, F32 = jnp.bfloat16, jnp.float32
MESH = pl.DeviceIdType.MESH
ANY = pl.BlockSpec(memory_space=pl.ANY)
DMA = pltpu.SemaphoreType.DMA
AXES = ("y", "z", "x", "core")
SIDE = 4
D, FF = 1024, 4096
OWN = 2048
TOKENS = 2 * OWN
CHUNKS = 4
WIDE = 512
HALVES = [slice(0, WIDE // 2), slice(WIDE // 2, WIDE)]
TILE = 1024
TILES = TOKENS // TILE
MINE = OWN // TILE
START, WAIT = (lambda c: c.start()), (lambda c: c.wait())
LANES, PART, QUARTER, SLOTS = 128, 32, 256, 8
PIECES = OWN // QUARTER
SLICED = (SIDE, 8, SIDE, PART, LANES)
BLOCKS = (SIDE, LANES, D)


def nn(a, b):
    return lax.dot_general(a, b, (((1,), (0,)), ((), ())), preferred_element_type=F32)


def nt(a, b):
    return lax.dot_general(a, b, (((1,), (1,)), ((), ())), preferred_element_type=F32)


def tn(a, b):
    return lax.dot_general(a, b, (((0,), (0,)), ((), ())), preferred_element_type=F32)


def normed(h):
    wide = h.astype(F32)
    scale = lax.rsqrt(jnp.mean(wide**2, -1, keepdims=True) + 1e-6)
    return (wide * scale).astype(BF)


def sigmoid(g):
    return 0.5 * jnp.tanh(0.5 * g) + 0.5


def block(i, n):
    return pl.ds(pl.multiple_of(i * n, n), n)


def when(*conditions):
    return pl.when(functools.reduce(jnp.logical_and, conditions))


class Place:
    def __init__(self):
        self.x, self.y, self.z, self.core = (lax.axis_index(a) for a in ("x", "y", "z", "core"))
        self.xc = self.x * 2 + self.core

    def plus(self, **by):
        return {a: lax.rem(getattr(self, a) + d, 2 if a == "core" else SIDE) for a, d in by.items()}

    def along(self, axis, d):
        return lax.rem(getattr(self, axis) + d, SIDE)


ROW = [(dx, dc) for dx in range(SIDE) for dc in range(2) if (dx, dc) != (0, 0)]
OTHERS = (1, 2, 3)


def greet(me):
    ids = [me.plus(x=dx, core=dc) for dx, dc in ROW] + [me.plus(**{a: d}) for a in ("y", "z") for d in OTHERS]
    barrier = pltpu.get_barrier_semaphore()
    for d in ids:
        pl.semaphore_signal(barrier, inc=1, device_id=d, device_id_type=MESH)
    pl.semaphore_wait(barrier, len(ids))


def remote(src, dst, ss, rs, to):
    return pltpu.make_async_remote_copy(src_ref=src, dst_ref=dst, send_sem=ss, recv_sem=rs, device_id=to, device_id_type=MESH)


class Gather:
    BASE = (0, 14, 17, 23)
    SEMS = 29

    def __init__(self, me, w, f, sems):
        self.me, (self.wg, self.wu, self.wd), (self.gf, self.uf, self.df), (self.ss, self.rs, self.ls) = me, w, f, sems

    def _go(self, act, q, base, copies):
        for n, (src, dst, to) in enumerate(copies, self.BASE[base]):
            act(remote(src, dst, self.ss.at[q, n], self.rs.at[q, n], to))

    def first(self, act, l, k, slot, q):
        me = self.me
        rows = block(me.z, PART)
        both = (self.wg, self.gf.at[slot, me.y, me.xc, me.z]), (self.wu, self.uf.at[slot, me.y, me.xc, me.z])

        def cols(c):
            return block((me.y * 2 + c) * CHUNKS + k, LANES)

        self._go(act, q, 0, [(w.at[l, rows, cols(lax.rem(me.core + dc, 2))], to, me.plus(x=dx, core=dc)) for dx, dc in ROW for w, to in both])
        for i, (w, to) in enumerate(both):
            act(pltpu.make_async_copy(w.at[l, rows, cols(me.core)], to, self.ls.at[q, i]))

    def down(self, act, l, k, slot, q):
        src, dst = self.wd.at[l, block(k, LANES)], self.df.at[slot, self.me.x]
        self._go(act, q, 1, [(src, dst, self.me.plus(x=d)) for d in OTHERS])
        act(pltpu.make_async_copy(src, dst, self.ls.at[q, 2]))

    def second(self, act, slot, q):
        me = self.me
        g, u = (f.at[slot, me.y, :, me.z] for f in (self.gf, self.uf))
        self._go(act, q, 2, [c for d in OTHERS for c in ((g, g, me.plus(y=d)), (u, u, me.plus(z=d)))])

    def third(self, act, slot, q):
        me = self.me
        g, u = self.gf.at[slot, :, :, me.z], self.uf.at[slot, me.y]
        self._go(act, q, 3, [c for d in OTHERS for c in ((g, g, me.plus(z=d)), (u, u, me.plus(y=d)))])

    def load(self, act, slot, v, sem):
        load(act, (self.gf, self.uf, self.df), slot, v, sem)


def load(act, f, slot, v, sem):
    src, to = slot
    for i in range(3):
        act(pltpu.make_async_copy(f[i].at[src], v[i].at[to], sem.at[i]))


def gather_scratch(chunks):
    return [DMA((chunks, Gather.SEMS)), DMA((chunks, Gather.SEMS)), DMA((chunks, 3))]


def matrix(v, slot):
    return jnp.concatenate([v[slot, u].reshape(D, LANES) for u in range(SIDE)], axis=1)


class Reduce:
    BASE = (0, 9, 18, 35)

    @staticmethod
    def scratch():
        v = pltpu.VMEM
        held = lambda *s: v(s, BF)
        came = lambda *s: v((2, 3) + s, BF)
        return [
            held(*SLICED), held(*SLICED), held(*BLOCKS),
            came(8, SIDE, PART, LANES), came(SIDE, 8, PART, LANES), came(LANES, D),
            held(8, SIDE, PART, LANES), held(SIDE, 8, PART, LANES), held(LANES, D),
            came(8, PART, LANES), came(8, PART, LANES), came(PART, D),
            held(8, PART, LANES), held(8, PART, LANES), held(PART, D),
            v((2, 8, PART, LANES), BF), v((2, 8, PART, LANES), BF), came(PART, QUARTER),
            held(2, 2, PART, LANES), held(2, 2, PART, LANES), held(2, PART, QUARTER),
            DMA((2, 44)), DMA((2, 44)), DMA((SIDE, 9)), DMA((SIDE, 9)), DMA((2, 3)),
        ]

    def __init__(self, me, scratch, out):
        self.me, self.out = me, out
        self.w, self.r1, self.b1, self.r2, self.b2, self.r3, self.b3 = (scratch[3 * i : 3 * i + 3] for i in range(7))
        self.ss, self.rs, self.sl, self.rl, self.ls = scratch[-5:]

    def put(self, g, u, d):
        for w, acc in ((self.w[0], g), (self.w[1], u)):
            for i in range(SIDE):
                w[i] = acc[:, LANES * i : LANES * (i + 1)].astype(BF).reshape(8, SIDE, PART, LANES)
        self.w[2][...] = d[...].astype(BF).reshape(BLOCKS)

    def copies(self, stage, slot, q):
        me = self.me
        (g, u, d), row, col = self.out, block(me.y, PART), block(me.z, QUARTER)
        if stage == 1:
            for n, by in enumerate(OTHERS):
                y, z, x = (me.along(a, by) for a in ("y", "z", "x"))
                yield self.w[0].at[y], self.r1[0].at[q, n], me.plus(y=by)
                yield self.w[1].at[:, :, z], self.r1[1].at[q, n], me.plus(z=by)
                yield self.w[2].at[x], self.r1[2].at[q, n], me.plus(x=by)
        elif stage == 2:
            for n, by in enumerate(OTHERS):
                y, z = (me.along(a, by) for a in ("y", "z"))
                yield self.b1[0].at[:, z], self.r2[0].at[q, n], me.plus(z=by)
                yield self.b1[1].at[y], self.r2[1].at[q, n], me.plus(y=by)
                yield self.b1[2].at[block(y, PART)], self.r2[2].at[q, n], me.plus(y=by)
        elif stage == 3:
            for dx, dc in ROW:
                x, c = me.along("x", dx), lax.rem(me.core + dc, 2)
                for i in range(2):
                    yield self.b2[i].at[2 * x + c], self.r3[i].at[q, me.xc], me.plus(x=dx, core=dc)
            for n, by in enumerate(OTHERS):
                cols = block(me.along("z", by), QUARTER)
                yield self.b2[2].at[:, cols], self.r3[2].at[q, n], me.plus(z=by)
        elif stage == 4:
            for by in OTHERS:
                yield self.b3[0].at[q], g.at[slot, :, me.y, me.z], me.plus(z=by)
                yield self.b3[1].at[q], u.at[slot, :, me.y, me.z], me.plus(y=by)
                yield self.b3[2].at[q], d.at[slot, row, col], me.plus(y=by)
        else:
            for by in OTHERS:
                yield g.at[slot, :, me.y], g.at[slot, :, me.y], me.plus(y=by)
                yield u.at[slot, :, :, me.z], u.at[slot, :, :, me.z], me.plus(z=by)
                yield d.at[slot, :, col], d.at[slot, :, col], me.plus(z=by)

    def send(self, stage, act, slot, q):
        me = self.me
        for n, (src, dst, to) in enumerate(self.copies(stage, slot, q)):
            if stage > SIDE:
                act(remote(src, dst, self.sl.at[slot % SIDE, n], self.rl.at[slot % SIDE, n], to))
            else:
                n += self.BASE[stage - 1]
                act(remote(src, dst, self.ss.at[q, n], self.rs.at[q, n], to))
        if stage == SIDE:
            g, u, d = self.out
            ends = g.at[slot, :, me.y, me.z], u.at[slot, :, me.y, me.z], d.at[slot, block(me.y, PART), block(me.z, QUARTER)]
            for i, dst in enumerate(ends):
                act(pltpu.make_async_copy(self.b3[i].at[q], dst, self.ls.at[q, i]))

    def add(self, stage, q):
        me = self.me
        cols = block(me.z, QUARTER)
        if stage == 3:
            for r, b, own in zip(self.r3[:2], self.b3, self.b2):
                r[q, me.xc] = own[me.xc]
                for c in range(2):
                    total = r[q, c].astype(F32)
                    for x in OTHERS:
                        total += r[q, 2 * x + c].astype(F32)
                    b[q, c] = total.astype(BF)
            parts = ((self.b2[2].at[:, cols], self.r3[2], self.b3[2].at[q]),)
        elif stage == 2:
            own = self.b1[0].at[:, me.z], self.b1[1].at[me.y], self.b1[2].at[block(me.y, PART)]
            parts = zip(own, self.r2, self.b2)
        else:
            own = self.w[0].at[me.y], self.w[1].at[:, :, me.z], self.w[2].at[me.x]
            parts = zip(own, self.r1, self.b1)
        for own, r, b in parts:
            total = own[...].astype(F32)
            for n in range(3):
                total += r[q, n].astype(F32)
            b[...] = total.astype(BF)

    def turn(self, stage, slot, q):
        self.send(stage, WAIT, slot, q)
        if stage < SIDE:
            self.add(stage, q)
        self.send(stage + 1, START, slot, q)


def reduced_shapes(n):
    s = jax.ShapeDtypeStruct((n, 2, SIDE, SIDE, PART, LANES), BF)
    return [s, s, jax.ShapeDtypeStruct((n, LANES, D), BF)]


def gathered_shapes(n):
    s = jax.ShapeDtypeStruct((n,) + SLICED, BF)
    return [s, s, jax.ShapeDtypeStruct((n,) + BLOCKS, BF)]


def chunk_buffers():
    return [pltpu.VMEM((2,) + SLICED, BF)] * 2 + [pltpu.VMEM((2,) + BLOCKS, BF)]


def tile_of(i):
    k, t = i // TILES, i % TILES
    return jnp.where(k == CHUNKS - 1, (t + MINE) % TILES, t)


def rows_of(tile):
    return block(tile, TILE)


def params(collective_id):
    return pltpu.CompilerParams(collective_id=collective_id, has_side_effects=True, vmem_limit_bytes=66_000_000, dimension_semantics=("arbitrary",))


def forward_kernel(x, dy, wg, wu, wd, g_out, u_out, a_out, h_out, n_out, dys, gf, uf, df, a, xv, acc, prt, held, vg, vu, vd, ss, rs, ls, wsem, csem, esem, psem, dsem):
    i = pl.program_id(0)
    k, t = i // TILES, i % TILES
    me = Place()
    ga = Gather(me, (wg, wu, wd), (gf, uf, df), (ss, rs, ls))
    v = (vg, vu, vd)
    other = me.plus(core=1)
    mine, theirs = pl.ds(0, OWN), pl.ds(OWN, OWN)
    to_dy = remote(dy, dys.at[theirs], esem.at[0], esem.at[1], other)

    def stage(out, j):
        s = j % 2
        if out:
            return pltpu.make_async_copy(held.at[s], dys.at[block(j, QUARTER)], dsem.at[1, s])
        return pltpu.make_async_copy(dy.at[block(j, QUARTER)], held.at[s], dsem.at[0, s])

    to_a = remote(a.at[mine], a.at[theirs], esem.at[2], esem.at[3], other)
    save_a = pltpu.make_async_copy(a, a_out, csem.at[0])

    def spread(m, act, stage):
        if stage in ("first", "down"):
            getattr(ga, stage)(act, m // CHUNKS, m % CHUNKS, m, m)
        else:
            getattr(ga, stage)(act, m, m)

    def part(tile):
        return remote(acc.at[rows_of(tile)], prt.at[rows_of(tile - MINE)], psem.at[0, tile - MINE], psem.at[1, tile - MINE], other)

    @pl.when(i == 0)
    def _():
        fetch = pltpu.make_async_copy(x, xv, csem.at[1])
        fetch.start()
        greet(me)
        spread(0, START, "first")
        spread(0, START, "down")
        for m in range(1, CHUNKS + 1):
            spread(m, START, "first")
        fetch.wait()

        def norm(j, _):
            r = block(j, QUARTER)
            a[r] = normed(xv[r])
            return 0

        lax.fori_loop(0, PIECES, norm, 0)
        spread(0, WAIT, "first")
        spread(0, START, "second")
        to_a.start()
        spread(0, WAIT, "second")
        spread(0, START, "third")
        for m in (1, 2):
            spread(m, WAIT, "first")
            spread(m, START, "second")
        spread(0, WAIT, "third")
        spread(0, WAIT, "down")
        ga.load(START, (0, 0), v, wsem)
        spread(1, WAIT, "second")
        spread(1, START, "third")

    @pl.when(t == 0)
    def _():
        ga.load(WAIT, (k, k % 2), v, wsem)
        spread(k + 1, START, "down")

    @when(t == 1, k < 3)
    def _():
        @when(k < 2)
        def _():
            spread(k + 3, WAIT, "first")
            spread(k + 3, START, "second")

        spread(k + 2, WAIT, "second")
        spread(k + 2, START, "third")

    @pl.when(i == MINE)
    def _():
        to_a.wait()
        save_a.start()
        to_dy.start()

    j = i - MINE

    @when(j >= 2, j < PIECES)
    def _():
        stage(True, j - 2).wait()

    @when(j >= 0, j < PIECES)
    def _():
        stage(False, j).start()

    @when(j >= 1, j <= PIECES)
    def _():
        stage(False, j - 1).wait()
        stage(True, j - 1).start()


    @when(t == TILES - 1, k < CHUNKS - 1)
    def _():
        spread(k + 1, WAIT, "third")
        spread(k + 1, WAIT, "down")
        ga.load(START, (k + 1, (k + 1) % 2), v, wsem)

    @when(k == CHUNKS - 1, t >= 1, t <= MINE)
    def _():
        part(t - 1 + MINE).start()

    tile = tile_of(i)
    rows = rows_of(tile)
    s = k % 2
    at = a[rows]
    g = nn(at, matrix(vg, s))
    u = nn(at, matrix(vu, s))
    g_out[0] = g
    u_out[0] = u
    hidden = (g * sigmoid(g) * u).astype(BF)
    acc[rows] = jnp.where(k == 0, 0.0, acc[rows]) + nn(hidden, vd[s].reshape(WIDE, D))

    @pl.when(i == CHUNKS * TILES - 1)
    def _():
        save_a.wait()
        for j in range(MINE):
            part(MINE + j).wait()

        keep = pltpu.make_async_copy(xv, h_out, csem.at[1])
        keep_n = pltpu.make_async_copy(a.at[mine], n_out, csem.at[2])

        def end(j, _):
            r = block(j, QUARTER)
            h = (xv[r].astype(F32) + (acc[r] + prt[r]).astype(BF).astype(F32)).astype(BF)
            xv[r] = h
            a[r] = normed(h)
            pltpu.make_async_copy(xv.at[r], h_out.at[r], csem.at[1]).start()
            pltpu.make_async_copy(a.at[r], n_out.at[r], csem.at[2]).start()
            return 0

        lax.fori_loop(0, PIECES, end, 0)
        to_dy.wait()
        for j in (2, 1):
            stage(True, PIECES - j).wait()
        spread(CHUNKS, WAIT, "third")
        spread(CHUNKS, WAIT, "down")
        keep.wait()
        keep_n.wait()


def forward(x, dy, weights):
    steps = CHUNKS * TILES
    wide = pl.BlockSpec((1, TILE, WIDE), lambda i: (i // TILES, tile_of(i), 0))
    big = jax.ShapeDtypeStruct((CHUNKS, TOKENS, WIDE), F32)
    own = jax.ShapeDtypeStruct((OWN, D), BF)
    return pl.pallas_call(
        forward_kernel,
        grid=(steps,),
        in_specs=[ANY] * 5,
        out_specs=[wide, wide] + [ANY] * 7,
        out_shape=[big, big, jax.ShapeDtypeStruct((TOKENS, D), BF), own, own, jax.ShapeDtypeStruct((TOKENS, D), BF)] + gathered_shapes(CHUNKS + 1),
        scratch_shapes=[
            pltpu.VMEM((TOKENS, D), BF), pltpu.VMEM((OWN, D), BF), pltpu.VMEM((TOKENS, D), F32), pltpu.VMEM((OWN, D), F32), pltpu.VMEM((2, QUARTER, D), BF),
            *chunk_buffers(), *gather_scratch(CHUNKS + 1), DMA((3,)), DMA((3,)), DMA((4,)), DMA((2, MINE)), DMA((2, 2)),
        ],
        compiler_params=params(1),
        name="forward",
    )(x, dy, *weights)


def gradients_of(g, u, dh):
    s = sigmoid(g)
    si = g * s
    return (si * u).astype(BF), (dh * u * (s + si * (1 - s))).astype(BF), (dh * si).astype(BF)


def middle_kernel(dy, n, g4, u4, d4, wg, wu, wd, dao, dar, rg, ru, rd, kg, ku, kd, gf, uf, df, *scratch):
    a, da, ag, au, ad, vg, vu, vd, ss, rs, ls, wsem, csem, esem, psem, *rest = scratch
    i = pl.program_id(0)
    k, t = i // TILES, i % TILES
    me = Place()
    ga = Gather(me, (wg, wu, wd), (gf, uf, df), (ss, rs, ls))
    re = Reduce(me, rest, (rg, ru, rd))
    v = (vg, vu, vd)
    other = me.plus(core=1)
    mine, theirs = block(0, OWN), block(1, OWN)
    to_a = remote(n, a.at[theirs], esem.at[0], esem.at[1], other)
    last = CHUNKS - 1

    def part(tile):
        return remote(da.at[rows_of(tile)], dar.at[rows_of(tile - MINE)], psem.at[0, tile - MINE], psem.at[1, tile - MINE], other)

    def keep(tile):
        return pltpu.make_async_copy(da.at[rows_of(tile)], dao.at[rows_of(tile)], csem.at[tile])

    def bring(stage, act, c):
        if stage in ("first", "down"):
            getattr(ga, stage)(act, 1, c + 1, c, c)
        else:
            getattr(ga, stage)(act, c, c)

    @when(i == 0)
    def _():
        fetch = pltpu.make_async_copy(n, a.at[mine], csem.at[0])
        fetch.start()
        load(START, (g4, u4, d4), (CHUNKS, 0), v, wsem)
        greet(me)
        to_a.start()
        for c in range(last):
            bring("first", START, c)
        bring("down", START, 0)
        fetch.wait()
        load(WAIT, (g4, u4, d4), (CHUNKS, 0), v, wsem)

    now, before, q = k - 1, k - 2, k % 2

    @when(t == 0, k > 0)
    def _():
        ga.load(WAIT, (k - 1, k % 2), v, wsem)

        @when(k > 1)
        def _():
            re.turn(3, before, 1 - q)

        re.send(1, START, now, q)

    @when(t == 1, k > 1)
    def _():
        re.turn(4, before, 1 - q)

    for stage in (1, 2):

        @when(t == stage + 1, k > 0)
        def _(stage=stage):
            re.turn(stage, now, q)

    @when(t == 3, k > 1)
    def _():
        re.send(5, WAIT, before, 1 - q)

    @when(i == 1)
    def _():
        for c in range(last):
            bring("first", WAIT, c)
        bring("second", START, 0)

    @when(i == MINE)
    def _():
        to_a.wait()
        bring("second", WAIT, 0)
        bring("third", START, 0)
        for c in range(1, last):
            bring("second", START, c)
        bring("down", START, 1)

    @when(i == TILES)
    def _():
        bring("second", WAIT, 1)
        bring("third", START, 1)

    @when(i == TILES + 1)
    def _():
        bring("down", WAIT, 1)
        bring("down", START, 2)

    @when(i == TILES + 3)
    def _():
        bring("third", WAIT, 1)
        bring("second", WAIT, 2)
        bring("third", START, 2)

    @when(i == 2 * TILES + 1)
    def _():
        bring("third", WAIT, 2)
        bring("down", WAIT, 2)

    @when(t == TILES - 1, k > 0, k < last)
    def _():
        ga.load(START, (k, (k + 1) % 2), v, wsem)

    @when(k == last, t >= 1, t <= MINE)
    def _():
        part(t - 1 + MINE).start()

    @when(k == last, t > MINE)
    def _():
        keep(t - 1 - MINE).start()

    tile = tile_of(i)
    rows = rows_of(tile)
    s = k % 2
    at = a[rows]
    by = dy[...]
    mg, mu, md = matrix(vg, s), matrix(vu, s), vd[s].reshape(WIDE, D)
    parts = [gradients_of(nn(at, mg[:, c]), nn(at, mu[:, c]), nt(by, md[c]).astype(BF).astype(F32)) for c in HALVES]
    sum_up(t == 0, (ag, au, ad), at, by, parts)
    dg, du = (jnp.concatenate([p[j] for p in parts], axis=1) for j in (1, 2))
    da[rows] = jnp.where(k == 0, 0, da[rows]) + (nt(dg, mg) + nt(du, mu))

    @when(i == TILES - 1)
    def _():
        bring("third", WAIT, 0)
        bring("down", WAIT, 0)
        ga.load(START, (0, 1), v, wsem)

    @when(t == TILES - 1)
    def _():
        re.put(ag, au, ad)

    @when(i == CHUNKS * TILES - 1)
    def _():
        re.turn(3, last - 1, last % 2)
        keep(MINE - 1).start()
        outs = [pltpu.make_async_copy(re.w[j], (kg, ku, kd)[j], wsem.at[j]) for j in range(3)]
        for o in outs:
            o.start()
        for j in range(MINE):
            keep(j).wait()
            part(MINE + j).wait()
        for o in outs:
            o.wait()
        re.send(4, WAIT, last - 1, last % 2)


def middle(dy, n, f4, weights):
    half = jax.ShapeDtypeStruct((OWN, D), F32)
    raw = jax.ShapeDtypeStruct(SLICED, BF)
    outs = [half, half, *reduced_shapes(SLOTS), raw, raw, jax.ShapeDtypeStruct(BLOCKS, BF)]
    shapes = outs + gathered_shapes(CHUNKS - 1)
    return pl.pallas_call(
        middle_kernel,
        grid=(CHUNKS * TILES,),
        in_specs=[pl.BlockSpec((TILE, D), lambda i: (tile_of(i), 0))] + [ANY] * (1 + 3 + 3),
        out_specs=[ANY] * len(shapes),
        out_shape=shapes,
        scratch_shapes=[
            pltpu.VMEM((TOKENS, D), BF), pltpu.VMEM((TOKENS, D), F32), *sums(),
            *chunk_buffers(), *gather_scratch(CHUNKS - 1), DMA((3,)), DMA((MINE,)), DMA((2,)), DMA((2, MINE)), *Reduce.scratch(),
        ],
        compiler_params=params(2),
        name="middle",
    )(dy, n, *f4, *weights)[: len(outs)]


def sum_up(fresh, sums_, at, by, parts):
    ag, au, ad = sums_
    for c, (hidden, dg, du) in zip(HALVES, parts):
        ag[:, c] = jnp.where(fresh, 0, ag[:, c]) + tn(at, dg)
        au[:, c] = jnp.where(fresh, 0, au[:, c]) + tn(at, du)
        ad[c] = jnp.where(fresh, 0, ad[c]) + tn(hidden, by)


def sums():
    return [pltpu.VMEM((D, WIDE), F32), pltpu.VMEM((D, WIDE), F32), pltpu.VMEM((WIDE, D), F32)]


def back_kernel(g_in, u_in, a_in, down, dao, dar, h, dy, kg, ku, kd, *refs):
    sums_, scratch = refs[3:6], refs[6:]
    b, ag, au, ad, pf, pb, csem, esem, dsem = scratch[:9]
    i = pl.program_id(0)
    k, t = i // TILES, i % TILES
    me = Place()
    re = Reduce(me, scratch[9:], sums_)
    to_b = remote(b.at[block(0, OWN)], b.at[block(1, OWN)], esem.at[0], esem.at[1], me.plus(core=1))
    begun = CHUNKS - 1

    @when(i == 0)
    def _():
        raws = [pltpu.make_async_copy((kg, ku, kd)[j], re.w[j], csem.at[j]) for j in range(3)]
        for o in raws:
            o.start()

        def piece(act, j):
            r, s = block(j, QUARTER), j % 2
            for n, (src, dst) in enumerate(((dao, pf.at[s, 0]), (dar, pf.at[s, 1]), (h, pb.at[s, 0]), (dy, pb.at[s, 1]))):
                act(pltpu.make_async_copy(src.at[r], dst, dsem.at[s, n]))

        piece(START, 0)
        greet(me)
        for o in raws:
            o.wait()
        re.send(5, START, begun - 1, 1)
        re.send(1, START, begun, 0)

        def one(j, _):
            @when(j + 1 < PIECES)
            def _():
                piece(START, j + 1)

            piece(WAIT, j)
            s = j % 2
            by_a = (pf[s, 0] + pf[s, 1]).astype(BF)
            by_h = jax.vjp(normed, pb[s, 0])[1](by_a)[0]
            b[block(j, QUARTER)] = (pb[s, 1].astype(F32) + by_h.astype(F32)).astype(BF)
            return 0

        lax.fori_loop(0, PIECES, one, 0)
        to_b.start()

    @when(i == MINE)
    def _():
        to_b.wait()

    now, before, q = begun + k, begun + k - 1, k % 2

    @when(t == 0, k > 0)
    def _():
        re.send(1, START, now, q)

    @when(t == 1, k > 0)
    def _():
        re.turn(2, before, 1 - q)

        @when(k == 3)
        def _():
            re.send(5, WAIT, before - 2, 1 - q)

        @when(k > 1)
        def _():
            re.turn(4, before - 1, q)

    @when(t == 3)
    def _():
        @when(k == 1)
        def _():
            re.send(5, WAIT, before - 1, q)

        re.turn(1, now, q)

        @when(k > 0)
        def _():
            re.turn(3, before, 1 - q)

    at, by = a_in[...], b[rows_of(tile_of(i))]
    md = down[0].reshape(WIDE, D)
    parts = [gradients_of(g_in[0, :, c], u_in[0, :, c], nt(by, md[c]).astype(BF).astype(F32)) for c in HALVES]
    sum_up(t == 0, (ag, au, ad), at, by, parts)

    @when(t == TILES - 1)
    def _():
        re.put(ag, au, ad)

    @when(i == CHUNKS * TILES - 1)
    def _():
        end = SLOTS - 1
        q, p = CHUNKS % 2, 1 - CHUNKS % 2
        re.send(1, START, end, q)
        re.send(5, WAIT, end - 3, p)
        re.turn(4, end - 2, q)
        re.turn(2, end - 1, p)
        re.turn(1, end, q)
        re.turn(3, end - 1, p)
        re.turn(2, end, q)
        re.turn(3, end, q)
        re.turn(4, end - 1, p)
        re.send(5, WAIT, end - 2, q)
        re.turn(4, end, q)
        re.send(5, WAIT, end - 1, p)
        re.send(5, WAIT, end, q)


def backward(g, u, a, down, half, raw, sums_):
    wide = pl.BlockSpec((1, TILE, WIDE), lambda i: (i // TILES, tile_of(i), 0))
    blocks = [wide, wide, pl.BlockSpec((TILE, D), lambda i: (tile_of(i), 0)), pl.BlockSpec((1,) + BLOCKS, lambda i: (i // TILES, 0, 0, 0))]
    args = (g, u, a, down, *half, *raw, *sums_)
    at = len(args) - len(sums_)
    return pl.pallas_call(
        back_kernel,
        grid=(CHUNKS * TILES,),
        in_specs=blocks + [ANY] * (len(args) - len(blocks)),
        out_specs=[ANY] * len(sums_),
        out_shape=reduced_shapes(SLOTS),
        input_output_aliases={at + i: i for i in range(len(sums_))},
        scratch_shapes=[
            pltpu.VMEM((TOKENS, D), BF), *sums(), pltpu.VMEM((2, 2, QUARTER, D), F32), pltpu.VMEM((2, 2, QUARTER, D), BF),
            DMA((3,)), DMA((2,)), DMA((2, 4)), *Reduce.scratch(),
        ],
        compiler_params=params(3),
        name="backward",
    )(*args)


def adamw(w, m, v, g):
    m = 0.9 * m + 0.1 * g
    v = 0.95 * v + 0.05 * g * g
    step = m * lax.rsqrt(v + 1e-8) + 0.1 * w
    return (w - 0.02 * step).astype(BF), m, v


def update_kernel(gg, gu, gd, *refs):
    ins, outs = refs[:9], refs[9:]
    sides = [jnp.concatenate([r[k, c, 0].reshape(LANES, LANES) for c in range(2) for k in range(CHUNKS)], axis=1) for r in (gg, gu)]
    for n, g in enumerate((*sides, gd[0])):
        w, m, v = (r[0] for r in ins[n::3])
        for out, new in zip(outs[n::3], adamw(w.astype(F32), m, v, g.astype(F32))):
            out[0] = new


def update(sums_, arrays):
    side = pl.BlockSpec((1, LANES, D), lambda i: (i // SIDE, 0, i % SIDE))
    deep = pl.BlockSpec((1, LANES, D), lambda i: (i // SIDE, i % SIDE, 0))
    part = pl.BlockSpec((CHUNKS, 2, 1, SIDE, PART, LANES), lambda i: (1 - i // SIDE, 0, i % SIDE, 0, 0, 0))
    down = pl.BlockSpec((1, LANES, D), lambda i: ((1 - i // SIDE) * CHUNKS + i % SIDE, 0, 0))
    return pl.pallas_call(
        update_kernel,
        grid=(SLOTS,),
        in_specs=[part, part, down] + [side, side, deep] * 3,
        out_specs=[side, side, deep] * 3,
        out_shape=[jax.ShapeDtypeStruct(x.shape, x.dtype) for x in arrays],
        compiler_params=pltpu.CompilerParams(vmem_limit_bytes=66_000_000, dimension_semantics=("arbitrary",)),
        name="update",
    )(*sums_, *arrays)


def solution(mesh):
    fine = Mesh(mesh.devices.reshape(SIDE, SIDE, SIDE, 2), AXES)

    def step(x, dy, *arrays):
        x, dy, weights = x[0], dy[0], arrays[:3]
        g0, u0, a0, h1, n1, dys, *f = forward(x, dy, weights)
        dao, dar, *rest = middle(dys, n1, f, weights)
        return update(backward(g0, u0, a0, f[2], (dao, dar, h1, dy), rest[3:], rest[:3]), arrays)

    states, cut = P(AXES, None, None), P(None, ("x", "core"), None)
    return jax.shard_map(
        step,
        mesh=fine,
        in_specs=(states, states) + (cut,) * 9,
        out_specs=(cut,) * 9,
        check_vma=False,
    )
```

```python
import functools

import jax
import jax.numpy as jnp
from jax import lax
from jax.experimental import pallas as pl
from jax.experimental.pallas import tpu as pltpu
from jax.sharding import Mesh
from jax.sharding import PartitionSpec as P

BF, F32 = jnp.bfloat16, jnp.float32
MESH = pl.DeviceIdType.MESH
ANY = pl.BlockSpec(memory_space=pl.ANY)
DMA = pltpu.SemaphoreType.DMA
AXES = ("y", "z", "x", "core")
SIDE = 4
D, FF = 1024, 4096
OWN = 2048
TOKENS = 2 * OWN
CHUNKS = 4
WIDE = 512
HALVES = [slice(0, WIDE // 2), slice(WIDE // 2, WIDE)]
TILE = 1024
TILES = TOKENS // TILE
MINE = OWN // TILE
START, WAIT = (lambda c: c.start()), (lambda c: c.wait())
LANES, PART, QUARTER, SLOTS = 128, 32, 256, 8
PIECES = OWN // QUARTER
SLICED = (SIDE, 8, SIDE, PART, LANES)
BLOCKS = (SIDE, LANES, D)


def nn(a, b):
    return lax.dot_general(a, b, (((1,), (0,)), ((), ())), preferred_element_type=F32)


def nt(a, b):
    return lax.dot_general(a, b, (((1,), (1,)), ((), ())), preferred_element_type=F32)


def tn(a, b):
    return lax.dot_general(a, b, (((0,), (0,)), ((), ())), preferred_element_type=F32)


def normed(h):
    wide = h.astype(F32)
    scale = lax.rsqrt(jnp.mean(wide**2, -1, keepdims=True) + 1e-6)
    return (wide * scale).astype(BF)


def sigmoid(g):
    return 0.5 * jnp.tanh(0.5 * g) + 0.5


def block(i, n):
    return pl.ds(pl.multiple_of(i * n, n), n)


def when(*conditions):
    return pl.when(functools.reduce(jnp.logical_and, conditions))


class Place:
    def __init__(self):
        self.x, self.y, self.z, self.core = (lax.axis_index(a) for a in ("x", "y", "z", "core"))
        self.xc = self.x * 2 + self.core

    def plus(self, **by):
        return {a: lax.rem(getattr(self, a) + d, 2 if a == "core" else SIDE) for a, d in by.items()}

    def along(self, axis, d):
        return lax.rem(getattr(self, axis) + d, SIDE)


ROW = [(dx, dc) for dx in range(SIDE) for dc in range(2) if (dx, dc) != (0, 0)]
OTHERS = (1, 2, 3)


def greet(me):
    ids = [me.plus(x=dx, core=dc) for dx, dc in ROW] + [me.plus(**{a: d}) for a in ("y", "z") for d in OTHERS]
    barrier = pltpu.get_barrier_semaphore()
    for d in ids:
        pl.semaphore_signal(barrier, inc=1, device_id=d, device_id_type=MESH)
    pl.semaphore_wait(barrier, len(ids))


def remote(src, dst, ss, rs, to):
    return pltpu.make_async_remote_copy(src_ref=src, dst_ref=dst, send_sem=ss, recv_sem=rs, device_id=to, device_id_type=MESH)


def pair(sems, *at):
    return sems.at[(0, *at)], sems.at[(1, *at)]


class Gather:
    BASE = (0, 14, 17, 23)
    SEMS = 29

    def __init__(self, me, w, f, sems):
        self.me, (self.wg, self.wu, self.wd), (self.gf, self.uf, self.df), (self.ss, self.rs, self.ls) = me, w, f, sems

    def _go(self, act, q, base, copies):
        for n, (src, dst, to) in enumerate(copies, self.BASE[base]):
            act(remote(src, dst, self.ss.at[q, n], self.rs.at[q, n], to))

    def first(self, act, l, k, slot, q):
        me = self.me
        rows = block(me.z, PART)
        both = (self.wg, self.gf.at[slot, me.y, me.xc, me.z]), (self.wu, self.uf.at[slot, me.y, me.xc, me.z])

        def cols(c):
            return block((me.y * 2 + c) * CHUNKS + k, LANES)

        self._go(act, q, 0, [(w.at[l, rows, cols(lax.rem(me.core + dc, 2))], to, me.plus(x=dx, core=dc)) for dx, dc in ROW for w, to in both])
        for i, (w, to) in enumerate(both):
            act(pltpu.make_async_copy(w.at[l, rows, cols(me.core)], to, self.ls.at[q, i]))

    def down(self, act, l, k, slot, q):
        src, dst = self.wd.at[l, block(k, LANES)], self.df.at[slot, self.me.x]
        self._go(act, q, 1, [(src, dst, self.me.plus(x=d)) for d in OTHERS])
        act(pltpu.make_async_copy(src, dst, self.ls.at[q, 2]))

    def second(self, act, slot, q):
        me = self.me
        g, u = (f.at[slot, me.y, :, me.z] for f in (self.gf, self.uf))
        self._go(act, q, 2, [c for d in OTHERS for c in ((g, g, me.plus(y=d)), (u, u, me.plus(z=d)))])

    def third(self, act, slot, q):
        me = self.me
        g, u = self.gf.at[slot, :, :, me.z], self.uf.at[slot, me.y]
        self._go(act, q, 3, [c for d in OTHERS for c in ((g, g, me.plus(z=d)), (u, u, me.plus(y=d)))])

    def load(self, act, slot, v, sem):
        load(act, (self.gf, self.uf, self.df), slot, v, sem)


def load(act, f, slot, v, sem):
    src, to = slot
    for i in range(3):
        act(pltpu.make_async_copy(f[i].at[src], v[i].at[to], sem.at[i]))


def gather_scratch(chunks):
    return [DMA((chunks, Gather.SEMS)), DMA((chunks, Gather.SEMS)), DMA((chunks, 3))]


def matrix(v, slot):
    return jnp.concatenate([v[slot, u].reshape(D, LANES) for u in range(SIDE)], axis=1)


class Reduce:
    BASE = (0, 9, 18, 35)

    @staticmethod
    def scratch():
        v = pltpu.VMEM
        held = lambda *s: v(s, BF)
        came = lambda *s: v((2, 3) + s, BF)
        return [
            held(*SLICED), held(*SLICED), held(*BLOCKS),
            came(8, SIDE, PART, LANES), came(SIDE, 8, PART, LANES), came(LANES, D),
            held(8, SIDE, PART, LANES), held(SIDE, 8, PART, LANES), held(LANES, D),
            came(8, PART, LANES), came(8, PART, LANES), came(PART, D),
            held(8, PART, LANES), held(8, PART, LANES), held(PART, D),
            v((2, 8, PART, LANES), BF), v((2, 8, PART, LANES), BF), came(PART, QUARTER),
            held(2, 2, PART, LANES), held(2, 2, PART, LANES), held(2, PART, QUARTER),
            DMA((2, 44)), DMA((2, 44)), DMA((SIDE, 9)), DMA((SIDE, 9)), DMA((2, 3)),
        ]

    def __init__(self, me, scratch, out):
        self.me, self.out = me, out
        self.w, self.r1, self.b1, self.r2, self.b2, self.r3, self.b3 = (scratch[3 * i : 3 * i + 3] for i in range(7))
        self.ss, self.rs, self.sl, self.rl, self.ls = scratch[-5:]

    def put(self, g, u, d):
        for w, acc in ((self.w[0], g), (self.w[1], u)):
            for i in range(SIDE):
                w[i] = acc[:, LANES * i : LANES * (i + 1)].astype(BF).reshape(8, SIDE, PART, LANES)
        self.w[2][...] = d[...].astype(BF).reshape(BLOCKS)

    def copies(self, stage, slot, q):
        me = self.me
        (g, u, d), row, col = self.out, block(me.y, PART), block(me.z, QUARTER)
        if stage == 1:
            for n, by in enumerate(OTHERS):
                y, z, x = (me.along(a, by) for a in ("y", "z", "x"))
                yield self.w[0].at[y], self.r1[0].at[q, n], me.plus(y=by)
                yield self.w[1].at[:, :, z], self.r1[1].at[q, n], me.plus(z=by)
                yield self.w[2].at[x], self.r1[2].at[q, n], me.plus(x=by)
        elif stage == 2:
            for n, by in enumerate(OTHERS):
                y, z = (me.along(a, by) for a in ("y", "z"))
                yield self.b1[0].at[:, z], self.r2[0].at[q, n], me.plus(z=by)
                yield self.b1[1].at[y], self.r2[1].at[q, n], me.plus(y=by)
                yield self.b1[2].at[block(y, PART)], self.r2[2].at[q, n], me.plus(y=by)
        elif stage == 3:
            for dx, dc in ROW:
                x, c = me.along("x", dx), lax.rem(me.core + dc, 2)
                for i in range(2):
                    yield self.b2[i].at[2 * x + c], self.r3[i].at[q, me.xc], me.plus(x=dx, core=dc)
            for n, by in enumerate(OTHERS):
                cols = block(me.along("z", by), QUARTER)
                yield self.b2[2].at[:, cols], self.r3[2].at[q, n], me.plus(z=by)
        elif stage == 4:
            for by in OTHERS:
                yield self.b3[0].at[q], g.at[slot, :, me.y, me.z], me.plus(z=by)
                yield self.b3[1].at[q], u.at[slot, :, me.y, me.z], me.plus(y=by)
                yield self.b3[2].at[q], d.at[slot, row, col], me.plus(y=by)
        else:
            for by in OTHERS:
                yield g.at[slot, :, me.y], g.at[slot, :, me.y], me.plus(y=by)
                yield u.at[slot, :, :, me.z], u.at[slot, :, :, me.z], me.plus(z=by)
                yield d.at[slot, :, col], d.at[slot, :, col], me.plus(z=by)

    def send(self, stage, act, slot, q):
        me = self.me
        for n, (src, dst, to) in enumerate(self.copies(stage, slot, q)):
            if stage > SIDE:
                act(remote(src, dst, self.sl.at[slot % SIDE, n], self.rl.at[slot % SIDE, n], to))
            else:
                n += self.BASE[stage - 1]
                act(remote(src, dst, self.ss.at[q, n], self.rs.at[q, n], to))
        if stage == SIDE:
            g, u, d = self.out
            ends = g.at[slot, :, me.y, me.z], u.at[slot, :, me.y, me.z], d.at[slot, block(me.y, PART), block(me.z, QUARTER)]
            for i, dst in enumerate(ends):
                act(pltpu.make_async_copy(self.b3[i].at[q], dst, self.ls.at[q, i]))

    def add(self, stage, q):
        me = self.me
        cols = block(me.z, QUARTER)
        if stage == 3:
            for r, b, own in zip(self.r3[:2], self.b3, self.b2):
                r[q, me.xc] = own[me.xc]
                for c in range(2):
                    total = r[q, c].astype(F32)
                    for x in OTHERS:
                        total += r[q, 2 * x + c].astype(F32)
                    b[q, c] = total.astype(BF)
            parts = ((self.b2[2].at[:, cols], self.r3[2], self.b3[2].at[q]),)
        elif stage == 2:
            own = self.b1[0].at[:, me.z], self.b1[1].at[me.y], self.b1[2].at[block(me.y, PART)]
            parts = zip(own, self.r2, self.b2)
        else:
            own = self.w[0].at[me.y], self.w[1].at[:, :, me.z], self.w[2].at[me.x]
            parts = zip(own, self.r1, self.b1)
        for own, r, b in parts:
            total = own[...].astype(F32)
            for n in range(3):
                total += r[q, n].astype(F32)
            b[...] = total.astype(BF)

    def turn(self, stage, slot, q):
        self.send(stage, WAIT, slot, q)
        if stage < SIDE:
            self.add(stage, q)
        self.send(stage + 1, START, slot, q)


def reduced_shapes(n):
    s = jax.ShapeDtypeStruct((n, 2, SIDE, SIDE, PART, LANES), BF)
    return [s, s, jax.ShapeDtypeStruct((n, LANES, D), BF)]


def gathered_shapes(n):
    s = jax.ShapeDtypeStruct((n,) + SLICED, BF)
    return [s, s, jax.ShapeDtypeStruct((n,) + BLOCKS, BF)]


def chunk_buffers():
    return [pltpu.VMEM((2,) + SLICED, BF)] * 2 + [pltpu.VMEM((2,) + BLOCKS, BF)]


def tile_of(i):
    k, t = i // TILES, i % TILES
    return jnp.where(k == CHUNKS - 1, (t + MINE) % TILES, t)


def rows_of(tile):
    return block(tile, TILE)


def params(collective_id):
    return pltpu.CompilerParams(collective_id=collective_id, has_side_effects=True, vmem_limit_bytes=67_000_000, dimension_semantics=("arbitrary",))


def forward_kernel(x, dy, wg, wu, wd, g_out, u_out, a_out, h_out, n_out, dys, gf, uf, df, a, xv, acc, prt, held, vg, vu, vd, ss, rs, ls, wsem, csem, esem, psem, dsem):
    i = pl.program_id(0)
    k, t = i // TILES, i % TILES
    me = Place()
    ga = Gather(me, (wg, wu, wd), (gf, uf, df), (ss, rs, ls))
    v = (vg, vu, vd)
    early = Gather(me, (wg, wu, wd), v, (ss, rs, ls))
    save_d = pltpu.make_async_copy(vd.at[0], df.at[0], csem.at[3])
    other = me.plus(core=1)
    mine, theirs = block(0, OWN), block(1, OWN)
    to_dy = remote(dy, dys.at[theirs], *pair(esem, 0), other)

    def stage(out, j):
        s = j % 2
        if out:
            return pltpu.make_async_copy(held.at[s], dys.at[block(j, QUARTER)], dsem.at[1, s])
        return pltpu.make_async_copy(dy.at[block(j, QUARTER)], held.at[s], dsem.at[0, s])

    to_a = remote(a.at[mine], a.at[theirs], *pair(esem, 1), other)
    save_a = pltpu.make_async_copy(a, a_out, csem.at[0])

    def spread(m, act, stage):
        to = getattr(early if isinstance(m, int) and m == 0 else ga, stage)
        if stage in ("first", "down"):
            to(act, m // CHUNKS, m % CHUNKS, m, m)
        else:
            to(act, m, m)

    def part(tile):
        return remote(acc.at[rows_of(tile)], prt.at[rows_of(tile - MINE)], *pair(psem, tile - MINE), other)

    @pl.when(i == 0)
    def _():
        fetch = pltpu.make_async_copy(x, xv, csem.at[1])
        fetch.start()
        greet(me)
        spread(0, START, "first")
        spread(1, START, "first")
        spread(0, START, "down")
        for m in range(2, CHUNKS + 1):
            spread(m, START, "first")
        spread(1, START, "down")
        fetch.wait()

        def norm(j, _):
            r = block(j, QUARTER)
            a[r] = normed(xv[r])
            return 0

        lax.fori_loop(0, PIECES, norm, 0)
        spread(0, WAIT, "first")
        spread(0, START, "second")
        to_a.start()
        spread(1, WAIT, "first")
        spread(1, START, "second")
        spread(0, WAIT, "second")
        spread(0, START, "third")
        spread(2, WAIT, "first")
        spread(2, START, "second")
        spread(0, WAIT, "third")
        spread(0, WAIT, "down")
        save_d.start()
        spread(1, WAIT, "second")
        spread(1, START, "third")

    @when(t == 0)
    def _():
        @when(k < CHUNKS - 1)
        def _():
            spread(k + 2, START, "down")

        @when(k > 0)
        def _():
            ga.load(WAIT, (k, k % 2), v, wsem)

        @when(k == 1)
        def _():
            save_d.wait()

    @when(t == 1, k < 3)
    def _():
        @when(k < 2)
        def _():
            spread(k + 3, WAIT, "first")
            spread(k + 3, START, "second")

        spread(k + 2, WAIT, "second")
        spread(k + 2, START, "third")

    @pl.when(i == MINE)
    def _():
        to_a.wait()
        save_a.start()
        to_dy.start()

    j = i - MINE

    @when(j >= 2, j < PIECES)
    def _():
        stage(True, j - 2).wait()

    @when(j >= 0, j < PIECES)
    def _():
        stage(False, j).start()

    @when(j >= 1, j <= PIECES)
    def _():
        stage(False, j - 1).wait()
        stage(True, j - 1).start()


    @when(t == TILES - 1, k < CHUNKS - 1)
    def _():
        spread(k + 1, WAIT, "third")
        spread(k + 1, WAIT, "down")
        ga.load(START, (k + 1, (k + 1) % 2), v, wsem)

    @when(k == CHUNKS - 1, t >= 1, t <= MINE)
    def _():
        part(t - 1 + MINE).start()

    tile = tile_of(i)
    rows = rows_of(tile)
    s = k % 2
    at = a[rows]
    g = nn(at, matrix(vg, s))
    u = nn(at, matrix(vu, s))
    g_out[0] = g
    u_out[0] = u
    hidden = (g * sigmoid(g) * u).astype(BF)
    acc[rows] = jnp.where(k == 0, 0.0, acc[rows]) + nn(hidden, vd[s].reshape(WIDE, D))

    @pl.when(i == CHUNKS * TILES - 1)
    def _():
        save_a.wait()
        for j in range(MINE):
            part(MINE + j).wait()

        keep = pltpu.make_async_copy(xv, h_out, csem.at[1])
        keep_n = pltpu.make_async_copy(a.at[mine], n_out, csem.at[2])

        def end(j, _):
            r = block(j, QUARTER)
            h = (xv[r].astype(F32) + (acc[r] + prt[r]).astype(BF).astype(F32)).astype(BF)
            xv[r] = h
            a[r] = normed(h)
            pltpu.make_async_copy(xv.at[r], h_out.at[r], csem.at[1]).start()
            pltpu.make_async_copy(a.at[r], n_out.at[r], csem.at[2]).start()
            return 0

        lax.fori_loop(0, PIECES, end, 0)
        to_dy.wait()
        for j in (2, 1):
            stage(True, PIECES - j).wait()
        spread(CHUNKS, WAIT, "third")
        spread(CHUNKS, WAIT, "down")
        keep.wait()
        keep_n.wait()


def forward(x, dy, weights):
    steps = CHUNKS * TILES
    wide = pl.BlockSpec((1, TILE, WIDE), lambda i: (i // TILES, tile_of(i), 0))
    big = jax.ShapeDtypeStruct((CHUNKS, TOKENS, WIDE), F32)
    own = jax.ShapeDtypeStruct((OWN, D), BF)
    return pl.pallas_call(
        forward_kernel,
        grid=(steps,),
        in_specs=[ANY] * 5,
        out_specs=[wide, wide] + [ANY] * 7,
        out_shape=[big, big, jax.ShapeDtypeStruct((TOKENS, D), BF), own, own, jax.ShapeDtypeStruct((TOKENS, D), BF)] + gathered_shapes(CHUNKS + 1),
        scratch_shapes=[
            pltpu.VMEM((TOKENS, D), BF), pltpu.VMEM((OWN, D), BF), pltpu.VMEM((TOKENS, D), F32), pltpu.VMEM((OWN, D), F32), pltpu.VMEM((2, QUARTER, D), BF),
            *chunk_buffers(), *gather_scratch(CHUNKS + 1), DMA((3,)), DMA((4,)), DMA((2, 2)), DMA((2, MINE)), DMA((2, 2)),
        ],
        compiler_params=params(1),
        name="forward",
    )(x, dy, *weights)


def gradients_of(g, u, dh):
    s = sigmoid(g)
    si = g * s
    return (si * u).astype(BF), (dh * u * (s + si * (1 - s))).astype(BF), (dh * si).astype(BF)


def middle_kernel(dy, dys, h, n, g4, u4, d4, wg, wu, wd, dh, dar, rg, ru, rd, kg, ku, kd, gf, uf, df, *scratch):
    a, da, ag, au, ad, vg, vu, vd, ss, rs, ls, wsem, csem, esem, psem, dsem, *rest = scratch
    i = pl.program_id(0)
    k, t = i // TILES, i % TILES
    me = Place()
    ga = Gather(me, (wg, wu, wd), (gf, uf, df), (ss, rs, ls))
    re = Reduce(me, rest, (rg, ru, rd))
    v = (vg, vu, vd)
    other = me.plus(core=1)
    mine, theirs = block(0, OWN), block(1, OWN)
    to_a = remote(n, a.at[theirs], *pair(esem, 0), other)
    last = CHUNKS - 1

    def part(tile):
        return remote(da.at[rows_of(tile)], dar.at[rows_of(tile - MINE)], *pair(psem, tile - MINE), other)

    def bring(stage, act, c):
        if stage in ("first", "down"):
            getattr(ga, stage)(act, 1, c + 1, c, c)
        else:
            getattr(ga, stage)(act, c, c)

    @when(i == 0)
    def _():
        fetch = pltpu.make_async_copy(n, a.at[mine], csem.at[0])
        fetch.start()
        load(START, (g4, u4, d4), (CHUNKS, 0), v, wsem)
        greet(me)
        to_a.start()
        for c in range(last):
            bring("first", START, c)
        bring("down", START, 0)
        fetch.wait()
        load(WAIT, (g4, u4, d4), (CHUNKS, 0), v, wsem)

    now, before, q = k - 1, k - 2, k % 2

    @when(t == 0, k > 0)
    def _():
        ga.load(WAIT, (k - 1, k % 2), v, wsem)

        @when(k > 1)
        def _():
            re.turn(3, before, 1 - q)

        re.send(1, START, now, q)

    @when(t == 1, k > 1)
    def _():
        re.turn(4, before, 1 - q)

    for stage in (1, 2):

        @when(t == stage + 1, k > 0)
        def _(stage=stage):
            re.turn(stage, now, q)

    @when(t == 3, k > 1)
    def _():
        re.send(5, WAIT, before, 1 - q)

    @when(i == 1)
    def _():
        for c in range(last):
            bring("first", WAIT, c)
            bring("second", START, c)

    @when(i == MINE)
    def _():
        to_a.wait()
        for c in range(last):
            bring("second", WAIT, c)
        bring("third", START, 0)
        bring("down", START, 1)

    @when(i == TILES - 1)
    def _():
        bring("third", START, 1)

    @when(i == TILES + 1)
    def _():
        bring("third", WAIT, 1)
        bring("down", WAIT, 1)
        bring("down", START, 2)

    @when(i == 2 * TILES - 1)
    def _():
        bring("third", START, 2)

    @when(i == 2 * TILES + 2)
    def _():
        bring("third", WAIT, 2)
        bring("down", WAIT, 2)

    @when(t == TILES - 1, k > 0, k < last)
    def _():
        ga.load(START, (k, (k + 1) % 2), v, wsem)

    @when(k == last, t >= 1, t <= MINE)
    def _():
        part(t - 1 + MINE).start()

    tile = tile_of(i)
    rows = rows_of(tile)
    s = k % 2
    at = a[rows]
    by = dy[...]
    mg, mu, md = matrix(vg, s), matrix(vu, s), vd[s].reshape(WIDE, D)
    parts = [gradients_of(nn(at, mg[:, c]), nn(at, mu[:, c]), nt(by, md[c]).astype(BF).astype(F32)) for c in HALVES]
    sum_up(t == 0, (ag, au, ad), at, by, parts)
    dg, du = (jnp.concatenate([p[j] for p in parts], axis=1) for j in (1, 2))
    da[rows] = jnp.where(k == 0, 0, da[rows]) + (nt(dg, mg) + nt(du, mu))

    @when(i == TILES - 1)
    def _():
        bring("third", WAIT, 0)
        bring("down", WAIT, 0)
        ga.load(START, (0, 1), v, wsem)

    @when(t == TILES - 1)
    def _():
        re.put(ag, au, ad)

    @when(i == CHUNKS * TILES - 1)
    def _():
        re.turn(3, last - 1, last % 2)
        outs = [pltpu.make_async_copy(re.w[j], (kg, ku, kd)[j], wsem.at[j]) for j in range(3)]
        for o in outs:
            o.start()
        for j in range(MINE):
            part(MINE + j).wait()

        def piece(act, j):
            r, s = block(j, LANES), j % SIDE
            for n, (src, dst) in enumerate(((dar, ad.at[block(s, LANES)]), (h, vd.at[0, s]), (dys, vd.at[1, s]))):
                act(pltpu.make_async_copy(src.at[r], dst, dsem.at[s, n]))

        count = OWN // LANES
        for j in range(SIDE - 1):
            piece(START, j)

        def one(j, _):
            @when(j + SIDE - 1 < count)
            def _():
                piece(START, j + SIDE - 1)

            piece(WAIT, j)
            r, s = block(j, LANES), j % SIDE
            by_h = jax.vjp(normed, vd[0, s])[1]((da[r] + ad[block(s, LANES)]).astype(BF))[0]
            a[r] = (vd[1, s].astype(F32) + by_h.astype(F32)).astype(BF)
            pltpu.make_async_copy(a.at[r], dh.at[r], csem.at[0]).start()
            return 0

        lax.fori_loop(0, count, one, 0)
        for o in outs:
            o.wait()
        re.send(SIDE, WAIT, last - 1, last % 2)
        pltpu.make_async_copy(a.at[mine], dh, csem.at[0]).wait()


def middle(dy, h, n, f4, weights):
    raw = jax.ShapeDtypeStruct(SLICED, BF)
    outs = [jax.ShapeDtypeStruct((OWN, D), BF), jax.ShapeDtypeStruct((OWN, D), F32), *reduced_shapes(SLOTS), raw, raw, jax.ShapeDtypeStruct(BLOCKS, BF)]
    shapes = outs + gathered_shapes(CHUNKS - 1)
    return pl.pallas_call(
        middle_kernel,
        grid=(CHUNKS * TILES,),
        in_specs=[pl.BlockSpec((TILE, D), lambda i: (tile_of(i), 0))] + [ANY] * 9,
        out_specs=[ANY] * len(shapes),
        out_shape=shapes,
        scratch_shapes=[
            pltpu.VMEM((TOKENS, D), BF), pltpu.VMEM((TOKENS, D), F32), *sums(),
            *chunk_buffers(), *gather_scratch(CHUNKS - 1), DMA((3,)), DMA((1,)), DMA((2, 1)), DMA((2, MINE)),
            DMA((SIDE, 3)), *Reduce.scratch(),
        ],
        compiler_params=params(2),
        name="middle",
    )(dy, dy, h, n, *f4, *weights)[: len(outs)]


def sum_up(fresh, sums_, at, by, parts):
    ag, au, ad = sums_
    for c, (hidden, dg, du) in zip(HALVES, parts):
        ag[:, c] = jnp.where(fresh, 0, ag[:, c]) + tn(at, dg)
        au[:, c] = jnp.where(fresh, 0, au[:, c]) + tn(at, du)
        ad[c] = jnp.where(fresh, 0, ad[c]) + tn(hidden, by)


def sums():
    return [pltpu.VMEM((D, WIDE), F32), pltpu.VMEM((D, WIDE), F32), pltpu.VMEM((WIDE, D), F32)]


def back_kernel(g_in, u_in, a_in, down, dh, kg, ku, kd, *refs):
    sums_, scratch = refs[3:6], refs[6:]
    b, ag, au, ad, csem, esem, *scratch = scratch
    i = pl.program_id(0)
    k, t = i // TILES, i % TILES
    me = Place()
    re = Reduce(me, scratch, sums_)
    to_b = remote(dh, b.at[block(1, OWN)], *pair(esem, 0), me.plus(core=1))
    begun = CHUNKS - 1

    @when(i == 0)
    def _():
        raws = [pltpu.make_async_copy((kg, ku, kd)[j], re.w[j], csem.at[j]) for j in range(3)]
        raws.append(pltpu.make_async_copy(dh, b.at[block(0, OWN)], csem.at[3]))
        for o in raws:
            o.start()
        greet(me)
        to_b.start()
        for o in raws:
            o.wait()
        re.send(1, START, begun, 0)
        re.send(5, START, begun - 1, 1)

    @when(i == MINE)
    def _():
        to_b.wait()

    now, before, q = begun + k, begun + k - 1, k % 2

    @when(t == 0, k > 0)
    def _():
        re.send(1, START, now, q)

    @when(t == 1, k > 0)
    def _():
        re.turn(2, before, 1 - q)

        @when(k == 3)
        def _():
            re.send(5, WAIT, before - 2, 1 - q)

        @when(k > 1)
        def _():
            re.turn(4, before - 1, q)

    @when(t == 3)
    def _():
        @when(k == 1)
        def _():
            re.send(5, WAIT, before - 1, q)

        re.turn(1, now, q)

        @when(k > 0)
        def _():
            re.turn(3, before, 1 - q)

    at, by = a_in[...], b[rows_of(tile_of(i))]
    md = down[0].reshape(WIDE, D)
    parts = [gradients_of(g_in[0, :, c], u_in[0, :, c], nt(by, md[c]).astype(BF).astype(F32)) for c in HALVES]
    sum_up(t == 0, (ag, au, ad), at, by, parts)

    @when(t == TILES - 1)
    def _():
        re.put(ag, au, ad)

    @when(i == CHUNKS * TILES - 1)
    def _():
        end = SLOTS - 1
        q, p = CHUNKS % 2, 1 - CHUNKS % 2
        re.send(1, START, end, q)
        re.send(5, WAIT, end - 3, p)
        re.turn(4, end - 2, q)
        re.turn(2, end - 1, p)
        re.turn(1, end, q)
        re.turn(3, end - 1, p)
        re.turn(2, end, q)
        re.turn(4, end - 1, p)
        re.send(5, WAIT, end - 2, q)
        re.turn(3, end, q)
        re.turn(4, end, q)
        re.send(5, WAIT, end - 1, p)
        re.send(5, WAIT, end, q)


def backward(g, u, a, down, dh, raw, sums_):
    wide = pl.BlockSpec((1, TILE, WIDE), lambda i: (i // TILES, tile_of(i), 0))
    blocks = [wide, wide, pl.BlockSpec((TILE, D), lambda i: (tile_of(i), 0)), pl.BlockSpec((1,) + BLOCKS, lambda i: (i // TILES, 0, 0, 0))]
    args = (g, u, a, down, dh, *raw, *sums_)
    at = len(args) - len(sums_)
    return pl.pallas_call(
        back_kernel,
        grid=(CHUNKS * TILES,),
        in_specs=blocks + [ANY] * (len(args) - len(blocks)),
        out_specs=[ANY] * len(sums_),
        out_shape=reduced_shapes(SLOTS),
        input_output_aliases={at + i: i for i in range(len(sums_))},
        scratch_shapes=[
            pltpu.VMEM((TOKENS, D), BF), *sums(), DMA((4,)), DMA((2, 1)), *Reduce.scratch(),
        ],
        compiler_params=params(3),
        name="backward",
    )(*args)


def adamw(w, m, v, g):
    m = 0.9 * m + 0.1 * g
    v = 0.95 * v + 0.05 * g * g
    step = m * lax.rsqrt(v + 1e-8) + 0.1 * w
    return (w - 0.02 * step).astype(BF), m, v


def update_kernel(gg, gu, gd, *refs):
    ins, outs = refs[:9], refs[9:]
    sides = [jnp.concatenate([r[k, c, 0].reshape(LANES, LANES) for c in range(2) for k in range(CHUNKS)], axis=1) for r in (gg, gu)]
    for n, g in enumerate((*sides, gd[0])):
        w, m, v = (r[0] for r in ins[n::3])
        for out, new in zip(outs[n::3], adamw(w.astype(F32), m, v, g.astype(F32))):
            out[0] = new


def update(sums_, arrays):
    side = pl.BlockSpec((1, LANES, D), lambda i: (i // SIDE, 0, i % SIDE))
    deep = pl.BlockSpec((1, LANES, D), lambda i: (i // SIDE, i % SIDE, 0))
    part = pl.BlockSpec((CHUNKS, 2, 1, SIDE, PART, LANES), lambda i: (1 - i // SIDE, 0, i % SIDE, 0, 0, 0))
    down = pl.BlockSpec((1, LANES, D), lambda i: ((1 - i // SIDE) * CHUNKS + i % SIDE, 0, 0))
    return pl.pallas_call(
        update_kernel,
        grid=(SLOTS,),
        in_specs=[part, part, down] + [side, side, deep] * 3,
        out_specs=[side, side, deep] * 3,
        out_shape=[jax.ShapeDtypeStruct(x.shape, x.dtype) for x in arrays],
        compiler_params=pltpu.CompilerParams(vmem_limit_bytes=67_000_000, dimension_semantics=("arbitrary",)),
        name="update",
    )(*sums_, *arrays)


def solution(mesh):
    fine = Mesh(mesh.devices.reshape(SIDE, SIDE, SIDE, 2), AXES)

    def step(x, dy, *arrays):
        x, dy, weights = x[0], dy[0], arrays[:3]
        g0, u0, a0, h1, n1, dys, *f = forward(x, dy, weights)
        dh, _, *rest = middle(dys, h1, n1, f, weights)
        return update(backward(g0, u0, a0, f[2], dh, rest[3:], rest[:3]), arrays)

    states, cut = P(AXES, None, None), P(None, ("x", "core"), None)
    return jax.shard_map(
        step,
        mesh=fine,
        in_specs=(states, states) + (cut,) * 9,
        out_specs=(cut,) * 9,
        check_vma=False,
    )
```

```python
import functools

import jax
import jax.numpy as jnp
from jax import lax
from jax.experimental import pallas as pl
from jax.experimental.pallas import tpu as pltpu
from jax.sharding import Mesh
from jax.sharding import PartitionSpec as P

BF, F32 = jnp.bfloat16, jnp.float32
MESH = pl.DeviceIdType.MESH
ANY = pl.BlockSpec(memory_space=pl.ANY)
DMA = pltpu.SemaphoreType.DMA
AXES = ("y", "z", "x", "core")
SIDE = 4
D, FF = 1024, 4096
OWN = 2048
TOKENS = 2 * OWN
CHUNKS = 4
WIDE = 512
HALVES = [slice(0, WIDE // 2), slice(WIDE // 2, WIDE)]
TILE = 1024
TILES = TOKENS // TILE
MINE = OWN // TILE
START, WAIT = (lambda c: c.start()), (lambda c: c.wait())
LANES, PART, QUARTER, SLOTS = 128, 32, 256, 8
PIECES = OWN // QUARTER
SLICED = (SIDE, 8, SIDE, PART, LANES)
BLOCKS = (SIDE, LANES, D)


def nn(a, b):
    return lax.dot_general(a, b, (((1,), (0,)), ((), ())), preferred_element_type=F32)


def nt(a, b):
    return lax.dot_general(a, b, (((1,), (1,)), ((), ())), preferred_element_type=F32)


def tn(a, b):
    return lax.dot_general(a, b, (((0,), (0,)), ((), ())), preferred_element_type=F32)


def normed(h):
    wide = h.astype(F32)
    scale = lax.rsqrt(jnp.mean(wide**2, -1, keepdims=True) + 1e-6)
    return (wide * scale).astype(BF)


def sigmoid(g):
    return 0.5 * jnp.tanh(0.5 * g) + 0.5


def block(i, n):
    return pl.ds(pl.multiple_of(i * n, n), n)


def when(*conditions):
    return pl.when(functools.reduce(jnp.logical_and, conditions))


class Place:
    def __init__(self):
        self.x, self.y, self.z, self.core = (lax.axis_index(a) for a in ("x", "y", "z", "core"))
        self.xc = self.x * 2 + self.core

    def plus(self, **by):
        return {a: lax.rem(getattr(self, a) + d, 2 if a == "core" else SIDE) for a, d in by.items()}

    def along(self, axis, d):
        return lax.rem(getattr(self, axis) + d, SIDE)


ROW = [(dx, dc) for dx in range(SIDE) for dc in range(2) if (dx, dc) != (0, 0)]
OTHERS = (1, 2, 3)


def greet(me):
    ids = [me.plus(x=dx, core=dc) for dx, dc in ROW] + [me.plus(**{a: d}) for a in ("y", "z") for d in OTHERS]
    barrier = pltpu.get_barrier_semaphore()
    for d in ids:
        pl.semaphore_signal(barrier, inc=1, device_id=d, device_id_type=MESH)
    pl.semaphore_wait(barrier, len(ids))


def remote(src, dst, ss, rs, to):
    return pltpu.make_async_remote_copy(src_ref=src, dst_ref=dst, send_sem=ss, recv_sem=rs, device_id=to, device_id_type=MESH)


def pair(sems, *at):
    return sems.at[(0, *at)], sems.at[(1, *at)]


def wait_for(whole, sem):
    pltpu.make_async_copy(whole, whole, sem).wait()


class Gather:
    SEMS = 5

    def __init__(self, me, w, f, sems):
        self.me, (self.wg, self.wu, self.wd), (self.gf, self.uf, self.df), (self.ss, self.rs, self.ls) = me, w, f, sems

    def _go(self, act, q, n, whole, copies):
        sems = self.ss.at[q, n], self.rs.at[q, n]
        if act is START:
            for src, dst, to in copies:
                remote(src, dst, *sems, to).start()
        else:
            for sem in sems:
                wait_for(whole, sem)

    def first(self, act, l, k, slot, q):
        me = self.me
        rows = block(me.z, PART)
        both = (self.wg, self.gf.at[slot, me.y, me.xc, me.z]), (self.wu, self.uf.at[slot, me.y, me.xc, me.z])

        def cols(c):
            return block((me.y * 2 + c) * CHUNKS + k, LANES)

        whole = self.gf.at[slot, 0, pl.ds(0, len(ROW)), pl.ds(0, 2)]
        self._go(act, q, 0, whole, [(w.at[l, rows, cols(lax.rem(me.core + dc, 2))], to, me.plus(x=dx, core=dc)) for dx, dc in ROW for w, to in both])
        for i, (w, to) in enumerate(both):
            act(pltpu.make_async_copy(w.at[l, rows, cols(me.core)], to, self.ls.at[q, i]))

    def down(self, act, l, k, slot, q):
        src, dst = self.wd.at[l, block(k, LANES)], self.df.at[slot, self.me.x]
        self._go(act, q, 1, self.df.at[slot, pl.ds(0, 3)], [(src, dst, self.me.plus(x=d)) for d in OTHERS])
        act(pltpu.make_async_copy(src, dst, self.ls.at[q, 2]))

    def second(self, act, slot, q):
        me = self.me
        g, u = (f.at[slot, me.y, :, me.z] for f in (self.gf, self.uf))
        whole = self.gf.at[slot, pl.ds(0, 3), :, pl.ds(0, 2)]
        self._go(act, q, 2, whole, [c for d in OTHERS for c in ((g, g, me.plus(y=d)), (u, u, me.plus(z=d)))])

    def third(self, act, slot, q):
        me = self.me
        g, u = self.gf.at[slot, :, :, me.z], self.uf.at[slot, me.y]
        self._go(act, q, 3, self.gf.at[slot, pl.ds(0, 3)], [(g, g, me.plus(z=d)) for d in OTHERS])
        self._go(act, q, SIDE, self.uf.at[slot, pl.ds(0, 3)], [(u, u, me.plus(y=d)) for d in OTHERS])

    def load(self, act, slot, v, sem):
        load(act, (self.gf, self.uf, self.df), slot, v, sem)


def load(act, f, slot, v, sem):
    src, to = slot
    for i in range(3):
        act(pltpu.make_async_copy(f[i].at[src], v[i].at[to], sem.at[i]))


def gather_scratch(chunks):
    return [DMA((chunks, Gather.SEMS)), DMA((chunks, Gather.SEMS)), DMA((chunks, 3))]


def matrix(v, slot):
    return jnp.concatenate([v[slot, u].reshape(D, LANES) for u in range(SIDE)], axis=1)


class Reduce:
    @staticmethod
    def scratch():
        v = pltpu.VMEM
        held = lambda *s: v(s, BF)
        came = lambda *s: v((2, 3) + s, BF)
        return [
            held(*SLICED), held(*SLICED), held(*BLOCKS),
            came(8, SIDE, PART, LANES), came(SIDE, 8, PART, LANES), came(LANES, D),
            held(8, SIDE, PART, LANES), held(SIDE, 8, PART, LANES), held(LANES, D),
            came(8, PART, LANES), came(8, PART, LANES), came(PART, D),
            held(8, PART, LANES), held(8, PART, LANES), held(PART, D),
            v((2, 8, PART, LANES), BF), v((2, 8, PART, LANES), BF), came(PART, QUARTER),
            held(2, 2, PART, LANES), held(2, 2, PART, LANES), held(2, PART, QUARTER),
            DMA((2, SIDE, 3)), DMA((2, SIDE, 3)), DMA((SIDE, 3)), DMA((SIDE, 3)), DMA((2, 3)),
        ]

    def __init__(self, me, scratch, out):
        self.me, self.out = me, out
        self.w, self.r1, self.b1, self.r2, self.b2, self.r3, self.b3 = (scratch[3 * i : 3 * i + 3] for i in range(7))
        self.ss, self.rs, self.sl, self.rl, self.ls = scratch[-5:]

    def put(self, g, u, d):
        for w, acc in ((self.w[0], g), (self.w[1], u)):
            for i in range(SIDE):
                w[i] = acc[:, LANES * i : LANES * (i + 1)].astype(BF).reshape(8, SIDE, PART, LANES)
        self.w[2][...] = d[...].astype(BF).reshape(BLOCKS)

    def copies(self, stage, slot, q):
        me = self.me
        (g, u, d), row, col = self.out, block(me.y, PART), block(me.z, QUARTER)
        if stage == 1:
            for n, by in enumerate(OTHERS):
                y, z, x = (me.along(a, by) for a in ("y", "z", "x"))
                yield self.w[0].at[y], self.r1[0].at[q, n], me.plus(y=by)
                yield self.w[1].at[:, :, z], self.r1[1].at[q, n], me.plus(z=by)
                yield self.w[2].at[x], self.r1[2].at[q, n], me.plus(x=by)
        elif stage == 2:
            for n, by in enumerate(OTHERS):
                y, z = (me.along(a, by) for a in ("y", "z"))
                yield self.b1[0].at[:, z], self.r2[0].at[q, n], me.plus(z=by)
                yield self.b1[1].at[y], self.r2[1].at[q, n], me.plus(y=by)
                yield self.b1[2].at[block(y, PART)], self.r2[2].at[q, n], me.plus(y=by)
        elif stage == 3:
            for dx, dc in ROW:
                x, c = me.along("x", dx), lax.rem(me.core + dc, 2)
                for i in range(2):
                    yield self.b2[i].at[2 * x + c], self.r3[i].at[q, me.xc], me.plus(x=dx, core=dc)
            for n, by in enumerate(OTHERS):
                cols = block(me.along("z", by), QUARTER)
                yield self.b2[2].at[:, cols], self.r3[2].at[q, n], me.plus(z=by)
        elif stage == 4:
            for by in OTHERS:
                yield self.b3[0].at[q], g.at[slot, :, me.y, me.z], me.plus(z=by)
                yield self.b3[1].at[q], u.at[slot, :, me.y, me.z], me.plus(y=by)
                yield self.b3[2].at[q], d.at[slot, row, col], me.plus(y=by)
        else:
            for by in OTHERS:
                yield g.at[slot, :, me.y], g.at[slot, :, me.y], me.plus(y=by)
                yield u.at[slot, :, :, me.z], u.at[slot, :, :, me.z], me.plus(z=by)
                yield d.at[slot, :, col], d.at[slot, :, col], me.plus(z=by)

    def sems(self, stage, slot, q, i):
        if stage > SIDE:
            return self.sl.at[slot % SIDE, i], self.rl.at[slot % SIDE, i]
        return self.ss.at[q, stage - 1, i], self.rs.at[q, stage - 1, i]

    def send(self, stage, act, slot, q):
        me = self.me
        if act is START:
            for n, (src, dst, to) in enumerate(self.copies(stage, slot, q)):
                i = n % 3 if stage != 3 else n % 2 if n < 2 * len(ROW) else 2
                remote(src, dst, *self.sems(stage, slot, q, i), to).start()
        else:
            for i in range(3):
                whole = (self.r1, self.r2, self.r3, self.r3, self.r2)[stage - 1][i].at[q]
                if stage in (3, SIDE) and i < 2:
                    whole = self.r3[i].at[q, pl.ds(0, len(ROW) if stage == 3 else 6)]
                for sem in self.sems(stage, slot, q, i):
                    wait_for(whole, sem)
        if stage == SIDE:
            g, u, d = self.out
            ends = g.at[slot, :, me.y, me.z], u.at[slot, :, me.y, me.z], d.at[slot, block(me.y, PART), block(me.z, QUARTER)]
            for i, dst in enumerate(ends):
                act(pltpu.make_async_copy(self.b3[i].at[q], dst, self.ls.at[q, i]))

    def add(self, stage, q):
        me = self.me
        cols = block(me.z, QUARTER)
        if stage == 3:
            for r, b, own in zip(self.r3[:2], self.b3, self.b2):
                r[q, me.xc] = own[me.xc]
                for c in range(2):
                    total = r[q, c].astype(F32)
                    for x in OTHERS:
                        total += r[q, 2 * x + c].astype(F32)
                    b[q, c] = total.astype(BF)
            parts = ((self.b2[2].at[:, cols], self.r3[2], self.b3[2].at[q]),)
        elif stage == 2:
            own = self.b1[0].at[:, me.z], self.b1[1].at[me.y], self.b1[2].at[block(me.y, PART)]
            parts = zip(own, self.r2, self.b2)
        else:
            own = self.w[0].at[me.y], self.w[1].at[:, :, me.z], self.w[2].at[me.x]
            parts = zip(own, self.r1, self.b1)
        for own, r, b in parts:
            total = own[...].astype(F32)
            for n in range(3):
                total += r[q, n].astype(F32)
            b[...] = total.astype(BF)

    def turn(self, stage, slot, q):
        self.send(stage, WAIT, slot, q)
        if stage < SIDE:
            self.add(stage, q)
        self.send(stage + 1, START, slot, q)


def reduced_shapes(n):
    s = jax.ShapeDtypeStruct((n, 2, SIDE, SIDE, PART, LANES), BF)
    return [s, s, jax.ShapeDtypeStruct((n, LANES, D), BF)]


def gathered_shapes(n):
    s = jax.ShapeDtypeStruct((n,) + SLICED, BF)
    return [s, s, jax.ShapeDtypeStruct((n,) + BLOCKS, BF)]


def chunk_buffers():
    return [pltpu.VMEM((2,) + SLICED, BF)] * 2 + [pltpu.VMEM((2,) + BLOCKS, BF)]


def tile_of(i):
    k, t = i // TILES, i % TILES
    return jnp.where(k == CHUNKS - 1, (t + MINE) % TILES, t)


def rows_of(tile):
    return block(tile, TILE)


def params(collective_id):
    return pltpu.CompilerParams(collective_id=collective_id, has_side_effects=True, vmem_limit_bytes=67_000_000, dimension_semantics=("arbitrary",))


def forward_kernel(x, dy, wg, wu, wd, g_out, u_out, a_out, h_out, n_out, dys, gf, uf, df, a, xv, acc, prt, held, vg, vu, vd, ss, rs, ls, wsem, csem, esem, psem, dsem):
    i = pl.program_id(0)
    k, t = i // TILES, i % TILES
    me = Place()
    ga = Gather(me, (wg, wu, wd), (gf, uf, df), (ss, rs, ls))
    v = (vg, vu, vd)
    early = Gather(me, (wg, wu, wd), v, (ss, rs, ls))
    save_d = pltpu.make_async_copy(vd.at[0], df.at[0], csem.at[3])
    other = me.plus(core=1)
    mine, theirs = block(0, OWN), block(1, OWN)
    to_dy = remote(dy, dys.at[theirs], *pair(esem, 0), other)

    def stage(out, j):
        s = j % 2
        if out:
            return pltpu.make_async_copy(held.at[s], dys.at[block(j, QUARTER)], dsem.at[1, s])
        return pltpu.make_async_copy(dy.at[block(j, QUARTER)], held.at[s], dsem.at[0, s])

    to_a = remote(a.at[mine], a.at[theirs], *pair(esem, 1), other)
    save_a = pltpu.make_async_copy(a, a_out, csem.at[0])

    def spread(m, act, stage):
        to = getattr(early if isinstance(m, int) and m == 0 else ga, stage)
        if stage in ("first", "down"):
            to(act, m // CHUNKS, m % CHUNKS, m, m)
        else:
            to(act, m, m)

    def part(tile):
        return remote(acc.at[rows_of(tile)], prt.at[rows_of(tile - MINE)], *pair(psem, tile - MINE), other)

    @pl.when(i == 0)
    def _():
        fetch = pltpu.make_async_copy(x, xv, csem.at[1])
        fetch.start()
        greet(me)
        spread(0, START, "first")
        spread(1, START, "first")
        spread(0, START, "down")
        for m in range(2, CHUNKS + 1):
            spread(m, START, "first")
        spread(1, START, "down")
        fetch.wait()

        def norm(j, _):
            r = block(j, QUARTER)
            a[r] = normed(xv[r])
            return 0

        lax.fori_loop(0, PIECES, norm, 0)
        spread(0, WAIT, "first")
        spread(0, START, "second")
        to_a.start()
        spread(1, WAIT, "first")
        spread(1, START, "second")
        spread(0, WAIT, "second")
        spread(0, START, "third")
        spread(2, WAIT, "first")
        spread(2, START, "second")
        spread(0, WAIT, "third")
        spread(0, WAIT, "down")
        save_d.start()
        spread(1, WAIT, "second")
        spread(1, START, "third")

    @when(t == 0)
    def _():
        @when(k < CHUNKS - 1)
        def _():
            spread(k + 2, START, "down")

        @when(k > 0)
        def _():
            ga.load(WAIT, (k, k % 2), v, wsem)

        @when(k == 1)
        def _():
            save_d.wait()

    @when(t == 1, k < 3)
    def _():
        @when(k < 2)
        def _():
            spread(k + 3, WAIT, "first")
            spread(k + 3, START, "second")

        spread(k + 2, WAIT, "second")
        spread(k + 2, START, "third")

    @pl.when(i == MINE)
    def _():
        to_a.wait()
        save_a.start()
        to_dy.start()

    j = i - MINE

    @when(j >= 2, j < PIECES)
    def _():
        stage(True, j - 2).wait()

    @when(j >= 0, j < PIECES)
    def _():
        stage(False, j).start()

    @when(j >= 1, j <= PIECES)
    def _():
        stage(False, j - 1).wait()
        stage(True, j - 1).start()


    @when(t == TILES - 1, k < CHUNKS - 1)
    def _():
        spread(k + 1, WAIT, "third")
        spread(k + 1, WAIT, "down")
        ga.load(START, (k + 1, (k + 1) % 2), v, wsem)

    @when(k == CHUNKS - 1, t >= 1, t <= MINE)
    def _():
        part(t - 1 + MINE).start()

    tile = tile_of(i)
    rows = rows_of(tile)
    s = k % 2
    at = a[rows]
    g = nn(at, matrix(vg, s))
    u = nn(at, matrix(vu, s))
    g_out[0] = g
    u_out[0] = u
    hidden = (g * sigmoid(g) * u).astype(BF)
    acc[rows] = jnp.where(k == 0, 0.0, acc[rows]) + nn(hidden, vd[s].reshape(WIDE, D))

    @pl.when(i == CHUNKS * TILES - 1)
    def _():
        save_a.wait()
        for j in range(MINE):
            part(MINE + j).wait()

        keep = pltpu.make_async_copy(xv, h_out, csem.at[1])
        keep_n = pltpu.make_async_copy(a.at[mine], n_out, csem.at[2])

        def end(j, _):
            r = block(j, QUARTER)
            h = (xv[r].astype(F32) + (acc[r] + prt[r]).astype(BF).astype(F32)).astype(BF)
            xv[r] = h
            a[r] = normed(h)
            pltpu.make_async_copy(xv.at[r], h_out.at[r], csem.at[1]).start()
            pltpu.make_async_copy(a.at[r], n_out.at[r], csem.at[2]).start()
            return 0

        lax.fori_loop(0, PIECES, end, 0)
        to_dy.wait()
        for j in (2, 1):
            stage(True, PIECES - j).wait()
        spread(CHUNKS, WAIT, "third")
        spread(CHUNKS, WAIT, "down")
        keep.wait()
        keep_n.wait()


def forward(x, dy, weights):
    steps = CHUNKS * TILES
    wide = pl.BlockSpec((1, TILE, WIDE), lambda i: (i // TILES, tile_of(i), 0))
    big = jax.ShapeDtypeStruct((CHUNKS, TOKENS, WIDE), F32)
    own = jax.ShapeDtypeStruct((OWN, D), BF)
    return pl.pallas_call(
        forward_kernel,
        grid=(steps,),
        in_specs=[ANY] * 5,
        out_specs=[wide, wide] + [ANY] * 7,
        out_shape=[big, big, jax.ShapeDtypeStruct((TOKENS, D), BF), own, own, jax.ShapeDtypeStruct((TOKENS, D), BF)] + gathered_shapes(CHUNKS + 1),
        scratch_shapes=[
            pltpu.VMEM((TOKENS, D), BF), pltpu.VMEM((OWN, D), BF), pltpu.VMEM((TOKENS, D), F32), pltpu.VMEM((OWN, D), F32), pltpu.VMEM((2, QUARTER, D), BF),
            *chunk_buffers(), *gather_scratch(CHUNKS + 1), DMA((3,)), DMA((4,)), DMA((2, 2)), DMA((2, MINE)), DMA((2, 2)),
        ],
        compiler_params=params(1),
        name="forward",
    )(x, dy, *weights)


def gradients_of(g, u, dh):
    s = sigmoid(g)
    si = g * s
    return (si * u).astype(BF), (dh * u * (s + si * (1 - s))).astype(BF), (dh * si).astype(BF)


def middle_kernel(dy, dys, h, n, g4, u4, d4, wg, wu, wd, dh, dar, rg, ru, rd, kg, ku, kd, gf, uf, df, *scratch):
    a, da, ag, au, ad, vg, vu, vd, ss, rs, ls, wsem, csem, esem, psem, dsem, *rest = scratch
    i = pl.program_id(0)
    k, t = i // TILES, i % TILES
    me = Place()
    ga = Gather(me, (wg, wu, wd), (gf, uf, df), (ss, rs, ls))
    re = Reduce(me, rest, (rg, ru, rd))
    v = (vg, vu, vd)
    other = me.plus(core=1)
    mine, theirs = block(0, OWN), block(1, OWN)
    to_a = remote(n, a.at[theirs], *pair(esem, 0), other)
    last = CHUNKS - 1

    def part(tile):
        return remote(da.at[rows_of(tile)], dar.at[rows_of(tile - MINE)], *pair(psem, tile - MINE), other)

    def bring(stage, act, c):
        if stage in ("first", "down"):
            getattr(ga, stage)(act, 1, c + 1, c, c)
        else:
            getattr(ga, stage)(act, c, c)

    @when(i == 0)
    def _():
        fetch = pltpu.make_async_copy(n, a.at[mine], csem.at[0])
        fetch.start()
        load(START, (g4, u4, d4), (CHUNKS, 0), v, wsem)
        greet(me)
        to_a.start()
        for c in range(last):
            bring("first", START, c)
        bring("down", START, 0)
        fetch.wait()
        load(WAIT, (g4, u4, d4), (CHUNKS, 0), v, wsem)

    now, before, q = k - 1, k - 2, k % 2

    @when(t == 0, k > 0)
    def _():
        ga.load(WAIT, (k - 1, k % 2), v, wsem)

        @when(k > 1)
        def _():
            re.turn(3, before, 1 - q)

        re.send(1, START, now, q)

    @when(t == 1, k > 1)
    def _():
        re.turn(4, before, 1 - q)

    for stage in (1, 2):

        @when(t == stage + 1, k > 0)
        def _(stage=stage):
            re.turn(stage, now, q)

    @when(t == 3, k > 1)
    def _():
        re.send(5, WAIT, before, 1 - q)

    @when(i == 1)
    def _():
        for c in range(last):
            bring("first", WAIT, c)
            bring("second", START, c)

    @when(i == MINE)
    def _():
        to_a.wait()
        for c in range(last):
            bring("second", WAIT, c)
        bring("third", START, 0)
        bring("down", START, 1)

    @when(i == TILES - 1)
    def _():
        bring("third", START, 1)

    @when(i == TILES + 1)
    def _():
        bring("third", WAIT, 1)
        bring("down", WAIT, 1)
        bring("down", START, 2)

    @when(i == 2 * TILES - 1)
    def _():
        bring("third", START, 2)

    @when(i == 2 * TILES + 2)
    def _():
        bring("third", WAIT, 2)
        bring("down", WAIT, 2)

    @when(t == TILES - 1, k > 0, k < last)
    def _():
        ga.load(START, (k, (k + 1) % 2), v, wsem)

    @when(k == last, t >= 1, t <= MINE)
    def _():
        part(t - 1 + MINE).start()

    tile = tile_of(i)
    rows = rows_of(tile)
    s = k % 2
    at = a[rows]
    by = dy[...]
    mg, mu, md = matrix(vg, s), matrix(vu, s), vd[s].reshape(WIDE, D)
    parts = [gradients_of(nn(at, mg[:, c]), nn(at, mu[:, c]), nt(by, md[c]).astype(BF).astype(F32)) for c in HALVES]
    sum_up(t == 0, (ag, au, ad), at, by, parts)
    dg, du = (jnp.concatenate([p[j] for p in parts], axis=1) for j in (1, 2))
    da[rows] = jnp.where(k == 0, 0, da[rows]) + (nt(dg, mg) + nt(du, mu))

    @when(i == TILES - 1)
    def _():
        bring("third", WAIT, 0)
        bring("down", WAIT, 0)
        ga.load(START, (0, 1), v, wsem)

    @when(t == TILES - 1)
    def _():
        re.put(ag, au, ad)

    @when(i == CHUNKS * TILES - 1)
    def _():
        re.turn(3, last - 1, last % 2)
        outs = [pltpu.make_async_copy(re.w[j], (kg, ku, kd)[j], wsem.at[j]) for j in range(3)]
        for o in outs:
            o.start()
        for j in range(MINE):
            part(MINE + j).wait()

        def piece(act, j):
            r, s = block(j, LANES), j % SIDE
            for n, (src, dst) in enumerate(((dar, ad.at[block(s, LANES)]), (h, vd.at[0, s]), (dys, vd.at[1, s]))):
                act(pltpu.make_async_copy(src.at[r], dst, dsem.at[s, n]))

        count = OWN // LANES
        for j in range(SIDE - 1):
            piece(START, j)

        def one(j, _):
            @when(j + SIDE - 1 < count)
            def _():
                piece(START, j + SIDE - 1)

            piece(WAIT, j)
            r, s = block(j, LANES), j % SIDE
            by_h = jax.vjp(normed, vd[0, s])[1]((da[r] + ad[block(s, LANES)]).astype(BF))[0]
            a[r] = (vd[1, s].astype(F32) + by_h.astype(F32)).astype(BF)
            pltpu.make_async_copy(a.at[r], dh.at[r], csem.at[0]).start()
            return 0

        lax.fori_loop(0, count, one, 0)
        for o in outs:
            o.wait()
        re.send(SIDE, WAIT, last - 1, last % 2)
        pltpu.make_async_copy(a.at[mine], dh, csem.at[0]).wait()


def middle(dy, h, n, f4, weights):
    raw = jax.ShapeDtypeStruct(SLICED, BF)
    outs = [jax.ShapeDtypeStruct((OWN, D), BF), jax.ShapeDtypeStruct((OWN, D), F32), *reduced_shapes(SLOTS), raw, raw, jax.ShapeDtypeStruct(BLOCKS, BF)]
    shapes = outs + gathered_shapes(CHUNKS - 1)
    return pl.pallas_call(
        middle_kernel,
        grid=(CHUNKS * TILES,),
        in_specs=[pl.BlockSpec((TILE, D), lambda i: (tile_of(i), 0))] + [ANY] * 9,
        out_specs=[ANY] * len(shapes),
        out_shape=shapes,
        scratch_shapes=[
            pltpu.VMEM((TOKENS, D), BF), pltpu.VMEM((TOKENS, D), F32), *sums(),
            *chunk_buffers(), *gather_scratch(CHUNKS - 1), DMA((3,)), DMA((1,)), DMA((2, 1)), DMA((2, MINE)),
            DMA((SIDE, 3)), *Reduce.scratch(),
        ],
        compiler_params=params(2),
        name="middle",
    )(dy, dy, h, n, *f4, *weights)[: len(outs)]


def sum_up(fresh, sums_, at, by, parts):
    ag, au, ad = sums_
    for c, (hidden, dg, du) in zip(HALVES, parts):
        ag[:, c] = jnp.where(fresh, 0, ag[:, c]) + tn(at, dg)
        au[:, c] = jnp.where(fresh, 0, au[:, c]) + tn(at, du)
        ad[c] = jnp.where(fresh, 0, ad[c]) + tn(hidden, by)


def sums():
    return [pltpu.VMEM((D, WIDE), F32), pltpu.VMEM((D, WIDE), F32), pltpu.VMEM((WIDE, D), F32)]


def back_kernel(g_in, u_in, a_in, down, dh, kg, ku, kd, *refs):
    sums_, scratch = refs[3:6], refs[6:]
    b, ag, au, ad, csem, esem, *scratch = scratch
    i = pl.program_id(0)
    k, t = i // TILES, i % TILES
    me = Place()
    re = Reduce(me, scratch, sums_)
    to_b = remote(dh, b.at[block(1, OWN)], *pair(esem, 0), me.plus(core=1))
    begun = CHUNKS - 1

    @when(i == 0)
    def _():
        raws = [pltpu.make_async_copy((kg, ku, kd)[j], re.w[j], csem.at[j]) for j in range(3)]
        raws.append(pltpu.make_async_copy(dh, b.at[block(0, OWN)], csem.at[3]))
        for o in raws:
            o.start()
        greet(me)
        to_b.start()
        for o in raws:
            o.wait()
        re.send(1, START, begun, 0)
        re.send(5, START, begun - 1, 1)

    @when(i == MINE)
    def _():
        to_b.wait()

    now, before, q = begun + k, begun + k - 1, k % 2

    @when(t == 0, k > 0)
    def _():
        re.send(1, START, now, q)

    @when(t == 1, k > 0)
    def _():
        re.turn(2, before, 1 - q)

        @when(k == 3)
        def _():
            re.send(5, WAIT, before - 2, 1 - q)

        @when(k > 1)
        def _():
            re.turn(4, before - 1, q)

    @when(t == 3)
    def _():
        @when(k == 1)
        def _():
            re.send(5, WAIT, before - 1, q)

        re.turn(1, now, q)

        @when(k > 0)
        def _():
            re.turn(3, before, 1 - q)

    at, by = a_in[...], b[rows_of(tile_of(i))]
    md = down[0].reshape(WIDE, D)
    parts = [gradients_of(g_in[0, :, c], u_in[0, :, c], nt(by, md[c]).astype(BF).astype(F32)) for c in HALVES]
    sum_up(t == 0, (ag, au, ad), at, by, parts)

    @when(t == TILES - 1)
    def _():
        re.put(ag, au, ad)

    @when(i == CHUNKS * TILES - 1)
    def _():
        end = SLOTS - 1
        q, p = CHUNKS % 2, 1 - CHUNKS % 2
        re.send(1, START, end, q)
        re.send(5, WAIT, end - 3, p)
        re.turn(4, end - 2, q)
        re.turn(2, end - 1, p)
        re.turn(1, end, q)
        re.turn(3, end - 1, p)
        re.turn(2, end, q)
        re.turn(4, end - 1, p)
        re.send(5, WAIT, end - 2, q)
        re.turn(3, end, q)
        re.turn(4, end, q)
        re.send(5, WAIT, end - 1, p)
        re.send(5, WAIT, end, q)


def backward(g, u, a, down, dh, raw, sums_):
    wide = pl.BlockSpec((1, TILE, WIDE), lambda i: (i // TILES, tile_of(i), 0))
    blocks = [wide, wide, pl.BlockSpec((TILE, D), lambda i: (tile_of(i), 0)), pl.BlockSpec((1,) + BLOCKS, lambda i: (i // TILES, 0, 0, 0))]
    args = (g, u, a, down, dh, *raw, *sums_)
    at = len(args) - len(sums_)
    return pl.pallas_call(
        back_kernel,
        grid=(CHUNKS * TILES,),
        in_specs=blocks + [ANY] * (len(args) - len(blocks)),
        out_specs=[ANY] * len(sums_),
        out_shape=reduced_shapes(SLOTS),
        input_output_aliases={at + i: i for i in range(len(sums_))},
        scratch_shapes=[
            pltpu.VMEM((TOKENS, D), BF), *sums(), DMA((4,)), DMA((2, 1)), *Reduce.scratch(),
        ],
        compiler_params=params(3),
        name="backward",
    )(*args)


def adamw(w, m, v, g):
    m = 0.9 * m + 0.1 * g
    v = 0.95 * v + 0.05 * g * g
    step = m * lax.rsqrt(v + 1e-8) + 0.1 * w
    return (w - 0.02 * step).astype(BF), m, v


def update_kernel(gg, gu, gd, *refs):
    ins, outs = refs[:9], refs[9:]
    sides = [jnp.concatenate([r[k, c, 0].reshape(LANES, LANES) for c in range(2) for k in range(CHUNKS)], axis=1) for r in (gg, gu)]
    for n, g in enumerate((*sides, gd[0])):
        w, m, v = (r[0] for r in ins[n::3])
        for out, new in zip(outs[n::3], adamw(w.astype(F32), m, v, g.astype(F32))):
            out[0] = new


def update(sums_, arrays):
    side = pl.BlockSpec((1, LANES, D), lambda i: (i // SIDE, 0, i % SIDE))
    deep = pl.BlockSpec((1, LANES, D), lambda i: (i // SIDE, i % SIDE, 0))
    part = pl.BlockSpec((CHUNKS, 2, 1, SIDE, PART, LANES), lambda i: (1 - i // SIDE, 0, i % SIDE, 0, 0, 0))
    down = pl.BlockSpec((1, LANES, D), lambda i: ((1 - i // SIDE) * CHUNKS + i % SIDE, 0, 0))
    return pl.pallas_call(
        update_kernel,
        grid=(SLOTS,),
        in_specs=[part, part, down] + [side, side, deep] * 3,
        out_specs=[side, side, deep] * 3,
        out_shape=[jax.ShapeDtypeStruct(x.shape, x.dtype) for x in arrays],
        compiler_params=pltpu.CompilerParams(vmem_limit_bytes=67_000_000, dimension_semantics=("arbitrary",)),
        name="update",
    )(*sums_, *arrays)


def solution(mesh):
    fine = Mesh(mesh.devices.reshape(SIDE, SIDE, SIDE, 2), AXES)

    def step(x, dy, *arrays):
        x, dy, weights = x[0], dy[0], arrays[:3]
        g0, u0, a0, h1, n1, dys, *f = forward(x, dy, weights)
        dh, _, *rest = middle(dys, h1, n1, f, weights)
        return update(backward(g0, u0, a0, f[2], dh, rest[3:], rest[:3]), arrays)

    states, cut = P(AXES, None, None), P(None, ("x", "core"), None)
    return jax.shard_map(
        step,
        mesh=fine,
        in_specs=(states, states) + (cut,) * 9,
        out_specs=(cut,) * 9,
        check_vma=False,
    )
```

```python
import functools

import jax
import jax.numpy as jnp
from jax import lax
from jax.experimental import pallas as pl
from jax.experimental.pallas import tpu as pltpu
from jax.sharding import Mesh
from jax.sharding import PartitionSpec as P

BF, F32 = jnp.bfloat16, jnp.float32
MESH = pl.DeviceIdType.MESH
ANY = pl.BlockSpec(memory_space=pl.ANY)
DMA = pltpu.SemaphoreType.DMA
AXES = ("y", "z", "x", "core")
SIDE = 4
D, FF = 1024, 4096
OWN = 2048
TOKENS = 2 * OWN
CHUNKS = 4
WIDE = 512
HALVES = [slice(0, WIDE // 2), slice(WIDE // 2, WIDE)]
TILE = 1024
TILES = TOKENS // TILE
MINE = OWN // TILE
START, WAIT = (lambda c: c.start()), (lambda c: c.wait())
LANES, PART, QUARTER, SLOTS = 128, 32, 256, 8
PIECES = OWN // QUARTER
SLICED = (SIDE, 8, SIDE, PART, LANES)
BLOCKS = (SIDE, LANES, D)


def nn(a, b):
    return lax.dot_general(a, b, (((1,), (0,)), ((), ())), preferred_element_type=F32)


def nt(a, b):
    return lax.dot_general(a, b, (((1,), (1,)), ((), ())), preferred_element_type=F32)


def tn(a, b):
    return lax.dot_general(a, b, (((0,), (0,)), ((), ())), preferred_element_type=F32)


def mean(rows):
    return jnp.mean(rows, -1, keepdims=True)


def scale_of(wide):
    return lax.rsqrt(mean(wide * wide) + 1e-6)


def normed(h):
    wide = h.astype(F32)
    return (wide * scale_of(wide)).astype(BF)


def norm_back(h, by_a):
    wide, g = h.astype(F32), by_a.astype(F32)
    s = scale_of(wide)
    return (s * g - wide * (s * s * s * mean(g * wide))).astype(BF)


def sigmoid(g):
    return 0.5 * jnp.tanh(0.5 * g) + 0.5


def block(i, n):
    return pl.ds(pl.multiple_of(i * n, n), n)


def when(*conditions):
    return pl.when(functools.reduce(jnp.logical_and, conditions))


class Place:
    def __init__(self):
        self.x, self.y, self.z, self.core = (lax.axis_index(a) for a in ("x", "y", "z", "core"))
        self.xc = self.x * 2 + self.core

    def plus(self, **by):
        return {a: lax.rem(getattr(self, a) + d, 2 if a == "core" else SIDE) for a, d in by.items()}

    def along(self, axis, d):
        return lax.rem(getattr(self, axis) + d, SIDE)


ROW = [(dx, dc) for dx in range(SIDE) for dc in range(2) if (dx, dc) != (0, 0)]
OTHERS = (1, 2, 3)


def greet(me):
    ids = [me.plus(x=dx, core=dc) for dx, dc in ROW] + [me.plus(**{a: d}) for a in ("y", "z") for d in OTHERS]
    barrier = pltpu.get_barrier_semaphore()
    for d in ids:
        pl.semaphore_signal(barrier, inc=1, device_id=d, device_id_type=MESH)
    pl.semaphore_wait(barrier, len(ids))


def remote(src, dst, ss, rs, to):
    return pltpu.make_async_remote_copy(src_ref=src, dst_ref=dst, send_sem=ss, recv_sem=rs, device_id=to, device_id_type=MESH)


def pair(sems, *at):
    return sems.at[(0, *at)], sems.at[(1, *at)]


def wait_for(whole, sem):
    pltpu.make_async_copy(whole, whole, sem).wait()


class Gather:
    SEMS = 5

    def __init__(self, me, w, f, sems):
        self.me, (self.wg, self.wu, self.wd), (self.gf, self.uf, self.df), (self.ss, self.rs, self.ls) = me, w, f, sems

    def _go(self, act, q, n, whole, copies):
        sems = self.ss.at[q, n], self.rs.at[q, n]
        if act is START:
            for src, dst, to in copies:
                remote(src, dst, *sems, to).start()
        else:
            for sem in sems:
                wait_for(whole, sem)

    def first(self, act, l, k, slot, q):
        me = self.me
        rows = block(me.z, PART)
        both = (self.wg, self.gf.at[slot, me.y, me.xc, me.z]), (self.wu, self.uf.at[slot, me.y, me.xc, me.z])

        def cols(c):
            return block((me.y * 2 + c) * CHUNKS + k, LANES)

        whole = self.gf.at[slot, 0, pl.ds(0, len(ROW)), pl.ds(0, 2)]
        self._go(act, q, 0, whole, [(w.at[l, rows, cols(lax.rem(me.core + dc, 2))], to, me.plus(x=dx, core=dc)) for dx, dc in ROW for w, to in both])
        for i, (w, to) in enumerate(both):
            act(pltpu.make_async_copy(w.at[l, rows, cols(me.core)], to, self.ls.at[q, i]))

    def down(self, act, l, k, slot, q):
        src, dst = self.wd.at[l, block(k, LANES)], self.df.at[slot, self.me.x]
        self._go(act, q, 1, self.df.at[slot, pl.ds(0, 3)], [(src, dst, self.me.plus(x=d)) for d in OTHERS])
        act(pltpu.make_async_copy(src, dst, self.ls.at[q, 2]))

    def second(self, act, slot, q):
        me = self.me
        g, u = (f.at[slot, me.y, :, me.z] for f in (self.gf, self.uf))
        whole = self.gf.at[slot, pl.ds(0, 3), :, pl.ds(0, 2)]
        self._go(act, q, 2, whole, [c for d in OTHERS for c in ((g, g, me.plus(y=d)), (u, u, me.plus(z=d)))])

    def third(self, act, slot, q):
        me = self.me
        g, u = self.gf.at[slot, :, :, me.z], self.uf.at[slot, me.y]
        self._go(act, q, 3, self.gf.at[slot, pl.ds(0, 3)], [(g, g, me.plus(z=d)) for d in OTHERS])
        self._go(act, q, SIDE, self.uf.at[slot, pl.ds(0, 3)], [(u, u, me.plus(y=d)) for d in OTHERS])

    def load(self, act, slot, v, sem):
        load(act, (self.gf, self.uf, self.df), slot, v, sem)


def load(act, f, slot, v, sem):
    src, to = slot
    for i in range(3):
        act(pltpu.make_async_copy(f[i].at[src], v[i].at[to], sem.at[i]))


def gather_scratch(chunks):
    return [DMA((chunks, Gather.SEMS)), DMA((chunks, Gather.SEMS)), DMA((chunks, 3))]


def matrix(v, slot):
    return jnp.concatenate([v[slot, u].reshape(D, LANES) for u in range(SIDE)], axis=1)


class Reduce:
    @staticmethod
    def scratch():
        v = pltpu.VMEM
        held = lambda *s: v(s, BF)
        came = lambda *s: v((2, 3) + s, BF)
        return [
            held(*SLICED), held(*SLICED), held(*BLOCKS),
            came(8, SIDE, PART, LANES), came(SIDE, 8, PART, LANES), came(LANES, D),
            held(8, SIDE, PART, LANES), held(SIDE, 8, PART, LANES), held(LANES, D),
            came(8, PART, LANES), came(8, PART, LANES), came(PART, D),
            held(8, PART, LANES), held(8, PART, LANES), held(PART, D),
            v((2, 8, PART, LANES), BF), v((2, 8, PART, LANES), BF), came(PART, QUARTER),
            held(2, 2, PART, LANES), held(2, 2, PART, LANES), held(2, PART, QUARTER),
            DMA((2, SIDE, 3)), DMA((2, SIDE, 3)), DMA((SIDE, 3)), DMA((SIDE, 3)), DMA((2, 3)),
        ]

    def __init__(self, me, scratch, out):
        self.me, self.out = me, out
        self.w, self.r1, self.b1, self.r2, self.b2, self.r3, self.b3 = (scratch[3 * i : 3 * i + 3] for i in range(7))
        self.ss, self.rs, self.sl, self.rl, self.ls = scratch[-5:]

    def put(self, g, u, d):
        for w, acc in ((self.w[0], g), (self.w[1], u)):
            for i in range(SIDE):
                w[i] = acc[:, LANES * i : LANES * (i + 1)].astype(BF).reshape(8, SIDE, PART, LANES)
        self.w[2][...] = d[...].astype(BF).reshape(BLOCKS)

    def copies(self, stage, slot, q):
        me = self.me
        (g, u, d), row, col = self.out, block(me.y, PART), block(me.z, QUARTER)
        if stage == 1:
            for n, by in enumerate(OTHERS):
                y, z, x = (me.along(a, by) for a in ("y", "z", "x"))
                yield self.w[0].at[y], self.r1[0].at[q, n], me.plus(y=by)
                yield self.w[1].at[:, :, z], self.r1[1].at[q, n], me.plus(z=by)
                yield self.w[2].at[x], self.r1[2].at[q, n], me.plus(x=by)
        elif stage == 2:
            for n, by in enumerate(OTHERS):
                y, z = (me.along(a, by) for a in ("y", "z"))
                yield self.b1[0].at[:, z], self.r2[0].at[q, n], me.plus(z=by)
                yield self.b1[1].at[y], self.r2[1].at[q, n], me.plus(y=by)
                yield self.b1[2].at[block(y, PART)], self.r2[2].at[q, n], me.plus(y=by)
        elif stage == 3:
            for dx, dc in ROW:
                x, c = me.along("x", dx), lax.rem(me.core + dc, 2)
                for i in range(2):
                    yield self.b2[i].at[2 * x + c], self.r3[i].at[q, me.xc], me.plus(x=dx, core=dc)
            for n, by in enumerate(OTHERS):
                cols = block(me.along("z", by), QUARTER)
                yield self.b2[2].at[:, cols], self.r3[2].at[q, n], me.plus(z=by)
        elif stage == 4:
            for by in OTHERS:
                yield self.b3[0].at[q], g.at[slot, :, me.y, me.z], me.plus(z=by)
                yield self.b3[1].at[q], u.at[slot, :, me.y, me.z], me.plus(y=by)
                yield self.b3[2].at[q], d.at[slot, row, col], me.plus(y=by)
        else:
            for by in OTHERS:
                yield g.at[slot, :, me.y], g.at[slot, :, me.y], me.plus(y=by)
                yield u.at[slot, :, :, me.z], u.at[slot, :, :, me.z], me.plus(z=by)
                yield d.at[slot, :, col], d.at[slot, :, col], me.plus(z=by)

    def sems(self, stage, slot, q, i):
        if stage > SIDE:
            return self.sl.at[slot % SIDE, i], self.rl.at[slot % SIDE, i]
        return self.ss.at[q, stage - 1, i], self.rs.at[q, stage - 1, i]

    def send(self, stage, act, slot, q):
        me = self.me
        if act is START:
            for n, (src, dst, to) in enumerate(self.copies(stage, slot, q)):
                i = n % 3 if stage != 3 else n % 2 if n < 2 * len(ROW) else 2
                remote(src, dst, *self.sems(stage, slot, q, i), to).start()
        else:
            for i in range(3):
                whole = (self.r1, self.r2, self.r3, self.r3, self.r2)[stage - 1][i].at[q]
                if stage in (3, SIDE) and i < 2:
                    whole = self.r3[i].at[q, pl.ds(0, len(ROW) if stage == 3 else 6)]
                for sem in self.sems(stage, slot, q, i):
                    wait_for(whole, sem)
        if stage == SIDE:
            g, u, d = self.out
            ends = g.at[slot, :, me.y, me.z], u.at[slot, :, me.y, me.z], d.at[slot, block(me.y, PART), block(me.z, QUARTER)]
            for i, dst in enumerate(ends):
                act(pltpu.make_async_copy(self.b3[i].at[q], dst, self.ls.at[q, i]))

    def add(self, stage, q):
        me = self.me
        cols = block(me.z, QUARTER)
        if stage == 3:
            for r, b, own in zip(self.r3[:2], self.b3, self.b2):
                r[q, me.xc] = own[me.xc]
                for c in range(2):
                    total = r[q, c].astype(F32)
                    for x in OTHERS:
                        total += r[q, 2 * x + c].astype(F32)
                    b[q, c] = total.astype(BF)
            parts = ((self.b2[2].at[:, cols], self.r3[2], self.b3[2].at[q]),)
        elif stage == 2:
            own = self.b1[0].at[:, me.z], self.b1[1].at[me.y], self.b1[2].at[block(me.y, PART)]
            parts = zip(own, self.r2, self.b2)
        else:
            own = self.w[0].at[me.y], self.w[1].at[:, :, me.z], self.w[2].at[me.x]
            parts = zip(own, self.r1, self.b1)
        for own, r, b in parts:
            total = own[...].astype(F32)
            for n in range(3):
                total += r[q, n].astype(F32)
            b[...] = total.astype(BF)

    def turn(self, stage, slot, q):
        self.send(stage, WAIT, slot, q)
        if stage < SIDE:
            self.add(stage, q)
        self.send(stage + 1, START, slot, q)


def reduced_shapes(n):
    s = jax.ShapeDtypeStruct((n, 2, SIDE, SIDE, PART, LANES), BF)
    return [s, s, jax.ShapeDtypeStruct((n, LANES, D), BF)]


def gathered_shapes(n):
    s = jax.ShapeDtypeStruct((n,) + SLICED, BF)
    return [s, s, jax.ShapeDtypeStruct((n,) + BLOCKS, BF)]


def chunk_buffers():
    return [pltpu.VMEM((2,) + SLICED, BF)] * 2 + [pltpu.VMEM((2,) + BLOCKS, BF)]


def tile_of(i):
    k, t = i // TILES, i % TILES
    return jnp.where(k == CHUNKS - 1, (t + MINE) % TILES, t)


def rows_of(tile):
    return block(tile, TILE)


def params(collective_id):
    return pltpu.CompilerParams(collective_id=collective_id, has_side_effects=True, vmem_limit_bytes=67_000_000, dimension_semantics=("arbitrary",))


def forward_kernel(x, dy, wg, wu, wd, g_out, u_out, a_out, h_out, n_out, dys, gf, uf, df, a, xv, acc, prt, held, vg, vu, vd, ss, rs, ls, wsem, csem, esem, psem, dsem):
    i = pl.program_id(0)
    k, t = i // TILES, i % TILES
    me = Place()
    ga = Gather(me, (wg, wu, wd), (gf, uf, df), (ss, rs, ls))
    v = (vg, vu, vd)
    early = Gather(me, (wg, wu, wd), v, (ss, rs, ls))
    save_d = pltpu.make_async_copy(vd.at[0], df.at[0], csem.at[3])
    other = me.plus(core=1)
    mine, theirs = block(0, OWN), block(1, OWN)
    to_dy = remote(dy, dys.at[theirs], *pair(esem, 0), other)

    def stage(out, j):
        s = j % 2
        if out:
            return pltpu.make_async_copy(held.at[s], dys.at[block(j, QUARTER)], dsem.at[1, s])
        return pltpu.make_async_copy(dy.at[block(j, QUARTER)], held.at[s], dsem.at[0, s])

    to_a = remote(a.at[mine], a.at[theirs], *pair(esem, 1), other)
    save_a = pltpu.make_async_copy(a, a_out, csem.at[0])

    def spread(m, act, stage):
        to = getattr(early if isinstance(m, int) and m == 0 else ga, stage)
        if stage in ("first", "down"):
            to(act, m // CHUNKS, m % CHUNKS, m, m)
        else:
            to(act, m, m)

    def part(tile):
        return remote(acc.at[rows_of(tile)], prt.at[rows_of(tile - MINE)], *pair(psem, tile - MINE), other)

    @pl.when(i == 0)
    def _():
        fetch = pltpu.make_async_copy(x, xv, csem.at[1])
        fetch.start()
        greet(me)
        for m in range(3):
            spread(m, START, "first")
        spread(0, START, "down")
        for m in range(3, CHUNKS + 1):
            spread(m, START, "first")
        spread(1, START, "down")
        fetch.wait()

        def norm(j, _):
            r = block(j, QUARTER)
            a[r] = normed(xv[r])
            return 0

        lax.fori_loop(0, PIECES, norm, 0)
        spread(0, WAIT, "first")
        spread(0, START, "second")
        to_a.start()
        spread(1, WAIT, "first")
        spread(1, START, "second")
        spread(0, WAIT, "second")
        spread(0, START, "third")
        spread(2, WAIT, "first")
        spread(2, START, "second")
        spread(1, WAIT, "second")
        spread(1, START, "third")
        spread(0, WAIT, "third")
        spread(0, WAIT, "down")
        save_d.start()

    @when(t == 0)
    def _():
        @when(k < CHUNKS - 1)
        def _():
            spread(k + 2, START, "down")

        @when(k > 0)
        def _():
            ga.load(WAIT, (k, k % 2), v, wsem)

        @when(k == 1)
        def _():
            save_d.wait()

    @when(t == 1, k < 3)
    def _():
        @when(k < 2)
        def _():
            spread(k + 3, WAIT, "first")
            spread(k + 3, START, "second")

        spread(k + 2, WAIT, "second")
        spread(k + 2, START, "third")

    @pl.when(i == MINE)
    def _():
        to_a.wait()
        save_a.start()
        to_dy.start()

    j = i - MINE

    @when(j >= 2, j < PIECES)
    def _():
        stage(True, j - 2).wait()

    @when(j >= 0, j < PIECES)
    def _():
        stage(False, j).start()

    @when(j >= 1, j <= PIECES)
    def _():
        stage(False, j - 1).wait()
        stage(True, j - 1).start()


    @when(t == TILES - 1, k < CHUNKS - 1)
    def _():
        spread(k + 1, WAIT, "third")
        spread(k + 1, WAIT, "down")
        ga.load(START, (k + 1, (k + 1) % 2), v, wsem)

    @when(k == CHUNKS - 1, t >= 1, t <= MINE)
    def _():
        part(t - 1 + MINE).start()

    tile = tile_of(i)
    rows = rows_of(tile)
    s = k % 2
    at = a[rows]
    g = nn(at, matrix(vg, s))
    u = nn(at, matrix(vu, s))
    g_out[0] = g
    u_out[0] = u
    hidden = (g * sigmoid(g) * u).astype(BF)
    acc[rows] = jnp.where(k == 0, 0.0, acc[rows]) + nn(hidden, vd[s].reshape(WIDE, D))

    @pl.when(i == CHUNKS * TILES - 1)
    def _():
        save_a.wait()
        for j in range(MINE):
            part(MINE + j).wait()

        keep = pltpu.make_async_copy(xv, h_out, csem.at[1])
        keep_n = pltpu.make_async_copy(a.at[mine], n_out, csem.at[2])

        def end(j, _):
            r = block(j, QUARTER)
            h = (xv[r].astype(F32) + (acc[r] + prt[r]).astype(BF).astype(F32)).astype(BF)
            xv[r] = h
            a[r] = normed(h)
            pltpu.make_async_copy(xv.at[r], h_out.at[r], csem.at[1]).start()
            pltpu.make_async_copy(a.at[r], n_out.at[r], csem.at[2]).start()
            return 0

        lax.fori_loop(0, PIECES, end, 0)
        to_dy.wait()
        for j in (2, 1):
            stage(True, PIECES - j).wait()
        spread(CHUNKS, WAIT, "third")
        spread(CHUNKS, WAIT, "down")
        keep.wait()
        keep_n.wait()


def forward(x, dy, weights):
    steps = CHUNKS * TILES
    wide = pl.BlockSpec((1, TILE, WIDE), lambda i: (i // TILES, tile_of(i), 0))
    big = jax.ShapeDtypeStruct((CHUNKS, TOKENS, WIDE), F32)
    own = jax.ShapeDtypeStruct((OWN, D), BF)
    return pl.pallas_call(
        forward_kernel,
        grid=(steps,),
        in_specs=[ANY] * 5,
        out_specs=[wide, wide] + [ANY] * 7,
        out_shape=[big, big, jax.ShapeDtypeStruct((TOKENS, D), BF), own, own, jax.ShapeDtypeStruct((TOKENS, D), BF)] + gathered_shapes(CHUNKS + 1),
        scratch_shapes=[
            pltpu.VMEM((TOKENS, D), BF), pltpu.VMEM((OWN, D), BF), pltpu.VMEM((TOKENS, D), F32), pltpu.VMEM((OWN, D), F32), pltpu.VMEM((2, QUARTER, D), BF),
            *chunk_buffers(), *gather_scratch(CHUNKS + 1), DMA((3,)), DMA((4,)), DMA((2, 2)), DMA((2, MINE)), DMA((2, 2)),
        ],
        compiler_params=params(1),
        name="forward",
    )(x, dy, *weights)


def gradients_of(g, u, dh):
    s = sigmoid(g)
    si = g * s
    return (si * u).astype(BF), (dh * u * (s + si * (1 - s))).astype(BF), (dh * si).astype(BF)


def middle_kernel(dy, dys, h, n, g4, u4, d4, wg, wu, wd, dh, dar, rg, ru, rd, kg, ku, kd, gf, uf, df, *scratch):
    a, da, ag, au, ad, vg, vu, vd, ss, rs, ls, wsem, csem, esem, psem, dsem, *rest = scratch
    i = pl.program_id(0)
    k, t = i // TILES, i % TILES
    me = Place()
    ga = Gather(me, (wg, wu, wd), (gf, uf, df), (ss, rs, ls))
    re = Reduce(me, rest, (rg, ru, rd))
    v = (vg, vu, vd)
    other = me.plus(core=1)
    mine, theirs = block(0, OWN), block(1, OWN)
    to_a = remote(n, a.at[theirs], *pair(esem, 0), other)
    last = CHUNKS - 1

    def part(tile):
        return remote(da.at[rows_of(tile)], dar.at[rows_of(tile - MINE)], *pair(psem, tile - MINE), other)

    def bring(stage, act, c):
        if stage in ("first", "down"):
            getattr(ga, stage)(act, 1, c + 1, c, c)
        else:
            getattr(ga, stage)(act, c, c)

    @when(i == 0)
    def _():
        fetch = pltpu.make_async_copy(n, a.at[mine], csem.at[0])
        fetch.start()
        load(START, (g4, u4, d4), (CHUNKS, 0), v, wsem)
        greet(me)
        to_a.start()
        for c in range(last):
            bring("first", START, c)
        bring("down", START, 0)
        fetch.wait()
        load(WAIT, (g4, u4, d4), (CHUNKS, 0), v, wsem)

    now, before, q = k - 1, k - 2, k % 2

    @when(t == 0, k > 0)
    def _():
        ga.load(WAIT, (k - 1, k % 2), v, wsem)

        @when(k > 1)
        def _():
            re.turn(3, before, 1 - q)

        re.send(1, START, now, q)

    @when(t == 1, k > 1)
    def _():
        re.turn(4, before, 1 - q)

    for stage in (1, 2):

        @when(t == stage + 1, k > 0)
        def _(stage=stage):
            re.turn(stage, now, q)

    @when(t == 3, k > 1)
    def _():
        re.send(5, WAIT, before, 1 - q)

    @when(i == 1)
    def _():
        for c in range(last):
            bring("first", WAIT, c)
            bring("second", START, c)

    @when(i == MINE)
    def _():
        to_a.wait()
        bring("second", WAIT, 0)
        bring("third", START, 0)
        bring("down", START, 1)

    @when(i == TILES - 1)
    def _():
        for c in range(1, last):
            bring("second", WAIT, c)
        bring("third", START, 1)

    @when(i == TILES + 1)
    def _():
        bring("third", WAIT, 1)
        bring("down", WAIT, 1)
        bring("down", START, 2)

    @when(i == 2 * TILES - 1)
    def _():
        bring("third", START, 2)

    @when(i == 2 * TILES + 2)
    def _():
        bring("third", WAIT, 2)
        bring("down", WAIT, 2)

    @when(t == TILES - 1, k > 0, k < last)
    def _():
        ga.load(START, (k, (k + 1) % 2), v, wsem)

    @when(k == last, t >= 1, t <= MINE)
    def _():
        part(t - 1 + MINE).start()

    tile = tile_of(i)
    rows = rows_of(tile)
    s = k % 2
    at = a[rows]
    by = dy[...]
    mg, mu, md = matrix(vg, s), matrix(vu, s), vd[s].reshape(WIDE, D)
    parts = [gradients_of(nn(at, mg[:, c]), nn(at, mu[:, c]), nt(by, md[c]).astype(BF).astype(F32)) for c in HALVES]
    sum_up(t == 0, (ag, au, ad), at, by, parts)
    dg, du = (jnp.concatenate([p[j] for p in parts], axis=1) for j in (1, 2))
    da[rows] = jnp.where(k == 0, 0, da[rows]) + (nt(dg, mg) + nt(du, mu))

    @when(i == TILES - 1)
    def _():
        bring("third", WAIT, 0)
        bring("down", WAIT, 0)
        ga.load(START, (0, 1), v, wsem)

    @when(t == TILES - 1)
    def _():
        re.put(ag, au, ad)

    @when(i == CHUNKS * TILES - 1)
    def _():
        re.turn(3, last - 1, last % 2)
        outs = [pltpu.make_async_copy(re.w[j], (kg, ku, kd)[j], wsem.at[j]) for j in range(3)]
        for o in outs:
            o.start()
        for j in range(MINE):
            part(MINE + j).wait()

        def piece(act, j):
            r, s = block(j, LANES), j % SIDE
            for n, (src, dst) in enumerate(((dar, ad.at[block(s, LANES)]), (h, vd.at[0, s]), (dys, vd.at[1, s]))):
                act(pltpu.make_async_copy(src.at[r], dst, dsem.at[s, n]))

        count = OWN // LANES
        for j in range(SIDE - 1):
            piece(START, j)

        def one(j, _):
            @when(j + SIDE - 1 < count)
            def _():
                piece(START, j + SIDE - 1)

            piece(WAIT, j)
            r, s = block(j, LANES), j % SIDE
            by_h = norm_back(vd[0, s], (da[r] + ad[block(s, LANES)]).astype(BF))
            a[r] = (vd[1, s].astype(F32) + by_h.astype(F32)).astype(BF)
            pltpu.make_async_copy(a.at[r], dh.at[r], csem.at[0]).start()
            return 0

        lax.fori_loop(0, count, one, 0)
        for o in outs:
            o.wait()
        re.send(SIDE, WAIT, last - 1, last % 2)
        pltpu.make_async_copy(a.at[mine], dh, csem.at[0]).wait()


def middle(dy, h, n, f4, weights):
    raw = jax.ShapeDtypeStruct(SLICED, BF)
    outs = [jax.ShapeDtypeStruct((OWN, D), BF), jax.ShapeDtypeStruct((OWN, D), F32), *reduced_shapes(SLOTS), raw, raw, jax.ShapeDtypeStruct(BLOCKS, BF)]
    shapes = outs + gathered_shapes(CHUNKS - 1)
    return pl.pallas_call(
        middle_kernel,
        grid=(CHUNKS * TILES,),
        in_specs=[pl.BlockSpec((TILE, D), lambda i: (tile_of(i), 0))] + [ANY] * 9,
        out_specs=[ANY] * len(shapes),
        out_shape=shapes,
        scratch_shapes=[
            pltpu.VMEM((TOKENS, D), BF), pltpu.VMEM((TOKENS, D), F32), *sums(),
            *chunk_buffers(), *gather_scratch(CHUNKS - 1), DMA((3,)), DMA((1,)), DMA((2, 1)), DMA((2, MINE)),
            DMA((SIDE, 3)), *Reduce.scratch(),
        ],
        compiler_params=params(2),
        name="middle",
    )(dy, dy, h, n, *f4, *weights)[: len(outs)]


def sum_up(fresh, sums_, at, by, parts):
    ag, au, ad = sums_
    for c, (hidden, dg, du) in zip(HALVES, parts):
        ag[:, c] = jnp.where(fresh, 0, ag[:, c]) + tn(at, dg)
        au[:, c] = jnp.where(fresh, 0, au[:, c]) + tn(at, du)
        ad[c] = jnp.where(fresh, 0, ad[c]) + tn(hidden, by)


def sums():
    return [pltpu.VMEM((D, WIDE), F32), pltpu.VMEM((D, WIDE), F32), pltpu.VMEM((WIDE, D), F32)]


def back_kernel(g_in, u_in, a_in, down, dh, kg, ku, kd, *refs):
    sums_, scratch = refs[3:6], refs[6:]
    b, ag, au, ad, csem, esem, *scratch = scratch
    i = pl.program_id(0)
    k, t = i // TILES, i % TILES
    me = Place()
    re = Reduce(me, scratch, sums_)
    to_b = remote(dh, b.at[block(1, OWN)], *pair(esem, 0), me.plus(core=1))
    begun = CHUNKS - 1

    @when(i == 0)
    def _():
        raws = [pltpu.make_async_copy((kg, ku, kd)[j], re.w[j], csem.at[j]) for j in range(3)]
        raws.append(pltpu.make_async_copy(dh, b.at[block(0, OWN)], csem.at[3]))
        for o in raws:
            o.start()
        greet(me)
        to_b.start()
        for o in raws:
            o.wait()
        re.send(1, START, begun, 0)
        re.send(5, START, begun - 1, 1)

    @when(i == MINE)
    def _():
        to_b.wait()

    now, before, q = begun + k, begun + k - 1, k % 2

    @when(t == 0, k > 0)
    def _():
        re.send(1, START, now, q)

    @when(t == 1, k > 0)
    def _():
        re.turn(2, before, 1 - q)

        @when(k == 3)
        def _():
            re.send(5, WAIT, before - 2, 1 - q)

        @when(k > 1)
        def _():
            re.turn(4, before - 1, q)

    @when(t == 3)
    def _():
        @when(k == 1)
        def _():
            re.send(5, WAIT, before - 1, q)

        re.turn(1, now, q)

        @when(k > 0)
        def _():
            re.turn(3, before, 1 - q)

    at, by = a_in[...], b[rows_of(tile_of(i))]
    md = down[0].reshape(WIDE, D)
    parts = [gradients_of(g_in[0, :, c], u_in[0, :, c], nt(by, md[c]).astype(BF).astype(F32)) for c in HALVES]
    sum_up(t == 0, (ag, au, ad), at, by, parts)

    @when(t == TILES - 1)
    def _():
        re.put(ag, au, ad)

    @when(i == CHUNKS * TILES - 1)
    def _():
        end = SLOTS - 1
        q, p = CHUNKS % 2, 1 - CHUNKS % 2
        re.send(1, START, end, q)
        re.send(5, WAIT, end - 3, p)
        re.turn(2, end - 1, p)
        re.turn(4, end - 2, q)
        re.turn(1, end, q)
        re.turn(3, end - 1, p)
        re.turn(2, end, q)
        re.turn(4, end - 1, p)
        re.send(5, WAIT, end - 2, q)
        re.turn(3, end, q)
        re.turn(4, end, q)
        re.send(5, WAIT, end - 1, p)
        re.send(5, WAIT, end, q)


def backward(g, u, a, down, dh, raw, sums_):
    wide = pl.BlockSpec((1, TILE, WIDE), lambda i: (i // TILES, tile_of(i), 0))
    blocks = [wide, wide, pl.BlockSpec((TILE, D), lambda i: (tile_of(i), 0)), pl.BlockSpec((1,) + BLOCKS, lambda i: (i // TILES, 0, 0, 0))]
    args = (g, u, a, down, dh, *raw, *sums_)
    at = len(args) - len(sums_)
    return pl.pallas_call(
        back_kernel,
        grid=(CHUNKS * TILES,),
        in_specs=blocks + [ANY] * (len(args) - len(blocks)),
        out_specs=[ANY] * len(sums_),
        out_shape=reduced_shapes(SLOTS),
        input_output_aliases={at + i: i for i in range(len(sums_))},
        scratch_shapes=[
            pltpu.VMEM((TOKENS, D), BF), *sums(), DMA((4,)), DMA((2, 1)), *Reduce.scratch(),
        ],
        compiler_params=params(3),
        name="backward",
    )(*args)


def adamw(w, m, v, g):
    m = 0.9 * m + 0.1 * g
    v = 0.95 * v + 0.05 * g * g
    step = m * lax.rsqrt(v + 1e-8) + 0.1 * w
    return (w - 0.02 * step).astype(BF), m, v


def update_kernel(gg, gu, gd, *refs):
    ins, outs = refs[:9], refs[9:]
    sides = [jnp.concatenate([r[k, c, 0].reshape(LANES, LANES) for c in range(2) for k in range(CHUNKS)], axis=1) for r in (gg, gu)]
    for n, g in enumerate((*sides, gd[0])):
        w, m, v = (r[0] for r in ins[n::3])
        for out, new in zip(outs[n::3], adamw(w.astype(F32), m, v, g.astype(F32))):
            out[0] = new


def update(sums_, arrays):
    side = pl.BlockSpec((1, LANES, D), lambda i: (i // SIDE, 0, i % SIDE))
    deep = pl.BlockSpec((1, LANES, D), lambda i: (i // SIDE, i % SIDE, 0))
    part = pl.BlockSpec((CHUNKS, 2, 1, SIDE, PART, LANES), lambda i: (1 - i // SIDE, 0, i % SIDE, 0, 0, 0))
    down = pl.BlockSpec((1, LANES, D), lambda i: ((1 - i // SIDE) * CHUNKS + i % SIDE, 0, 0))
    return pl.pallas_call(
        update_kernel,
        grid=(SLOTS,),
        in_specs=[part, part, down] + [side, side, deep] * 3,
        out_specs=[side, side, deep] * 3,
        out_shape=[jax.ShapeDtypeStruct(x.shape, x.dtype) for x in arrays],
        compiler_params=pltpu.CompilerParams(vmem_limit_bytes=67_000_000, dimension_semantics=("arbitrary",)),
        name="update",
    )(*sums_, *arrays)


def solution(mesh):
    fine = Mesh(mesh.devices.reshape(SIDE, SIDE, SIDE, 2), AXES)

    def step(x, dy, *arrays):
        x, dy, weights = x[0], dy[0], arrays[:3]
        g0, u0, a0, h1, n1, dys, *f = forward(x, dy, weights)
        dh, _, *rest = middle(dys, h1, n1, f, weights)
        return update(backward(g0, u0, a0, f[2], dh, rest[3:], rest[:3]), arrays)

    states, cut = P(AXES, None, None), P(None, ("x", "core"), None)
    return jax.shard_map(
        step,
        mesh=fine,
        in_specs=(states, states) + (cut,) * 9,
        out_specs=(cut,) * 9,
        check_vma=False,
    )
```

```python
import functools

import jax
import jax.numpy as jnp
from jax import lax
from jax.experimental import pallas as pl
from jax.experimental.pallas import tpu as pltpu
from jax.sharding import Mesh
from jax.sharding import PartitionSpec as P

BF, F32 = jnp.bfloat16, jnp.float32
MESH = pl.DeviceIdType.MESH
ANY = pl.BlockSpec(memory_space=pl.ANY)
DMA = pltpu.SemaphoreType.DMA
AXES = ("y", "z", "x", "core")
SIDE = 4
D, FF = 1024, 4096
OWN = 2048
TOKENS = 2 * OWN
CHUNKS = 4
WIDE = 512
HALVES = [slice(0, WIDE // 2), slice(WIDE // 2, WIDE)]
TILE = 1024
TILES = TOKENS // TILE
MINE = OWN // TILE
START, WAIT = (lambda c: c.start()), (lambda c: c.wait())
LANES, PART, QUARTER, SLOTS = 128, 32, 256, 8
PIECES = OWN // QUARTER
PAIR, UNITS = 2, 3
SLICED = (SIDE, 8, SIDE, PART, LANES)
BLOCKS = (SIDE, LANES, D)


def nn(a, b):
    return lax.dot_general(a, b, (((1,), (0,)), ((), ())), preferred_element_type=F32)


def nt(a, b):
    return lax.dot_general(a, b, (((1,), (1,)), ((), ())), preferred_element_type=F32)


def tn(a, b):
    return lax.dot_general(a, b, (((0,), (0,)), ((), ())), preferred_element_type=F32)


def mean(rows):
    return jnp.mean(rows, -1, keepdims=True)


def scale_of(wide):
    return lax.rsqrt(mean(wide * wide) + 1e-6)


def normed(h):
    wide = h.astype(F32)
    return (wide * scale_of(wide)).astype(BF)


def norm_back(h, by_a):
    wide, g = h.astype(F32), by_a.astype(F32)
    s = scale_of(wide)
    return (s * g - wide * (s * s * s * mean(g * wide))).astype(BF)


def sigmoid(g):
    return 0.5 * jnp.tanh(0.5 * g) + 0.5


def block(i, n):
    return pl.ds(pl.multiple_of(i * n, n), n)


def when(*conditions):
    return pl.when(functools.reduce(jnp.logical_and, conditions))


class Place:
    def __init__(self):
        self.x, self.y, self.z, self.core = (lax.axis_index(a) for a in ("x", "y", "z", "core"))
        self.xc = self.x * 2 + self.core

    def plus(self, **by):
        return {a: lax.rem(getattr(self, a) + d, 2 if a == "core" else SIDE) for a, d in by.items()}

    def along(self, axis, d):
        return lax.rem(getattr(self, axis) + d, SIDE)


ROW = [(dx, dc) for dx in range(SIDE) for dc in range(2) if (dx, dc) != (0, 0)]
OTHERS = (1, 2, 3)


def greet(me):
    ids = [me.plus(x=dx, core=dc) for dx, dc in ROW] + [me.plus(**{a: d}) for a in ("y", "z") for d in OTHERS]
    barrier = pltpu.get_barrier_semaphore()
    for d in ids:
        pl.semaphore_signal(barrier, inc=1, device_id=d, device_id_type=MESH)
    pl.semaphore_wait(barrier, len(ids))


def remote(src, dst, ss, rs, to):
    return pltpu.make_async_remote_copy(src_ref=src, dst_ref=dst, send_sem=ss, recv_sem=rs, device_id=to, device_id_type=MESH)


def pair(sems, *at):
    return sems.at[(0, *at)], sems.at[(1, *at)]


def wait_for(whole, sem):
    pltpu.make_async_copy(whole, whole, sem).wait()


class Gather:
    SEMS = 5

    def __init__(self, me, w, f, sems):
        self.me, (self.wg, self.wu, self.wd), (self.gf, self.uf, self.df), (self.ss, self.rs, self.ls) = me, w, f, sems

    def _go(self, act, q, n, whole, copies):
        sems = self.ss.at[q, n], self.rs.at[q, n]
        if act is START:
            for src, dst, to in copies:
                remote(src, dst, *sems, to).start()
        else:
            for sem in sems:
                wait_for(whole, sem)

    def first(self, act, l, k, slot, q):
        me = self.me
        rows = block(me.z, PART)
        both = (self.wg, self.gf.at[slot, me.y, me.xc, me.z]), (self.wu, self.uf.at[slot, me.y, me.xc, me.z])

        def cols(c):
            return block((me.y * 2 + c) * CHUNKS + k, LANES)

        whole = self.gf.at[slot, 0, pl.ds(0, len(ROW)), pl.ds(0, 2)]
        self._go(act, q, 0, whole, [(w.at[l, rows, cols(lax.rem(me.core + dc, 2))], to, me.plus(x=dx, core=dc)) for dx, dc in ROW for w, to in both])
        for i, (w, to) in enumerate(both):
            act(pltpu.make_async_copy(w.at[l, rows, cols(me.core)], to, self.ls.at[q, i]))

    def down(self, act, l, k, slot, q):
        src, dst = self.wd.at[l, block(k, LANES)], self.df.at[slot, self.me.x]
        self._go(act, q, 1, self.df.at[slot, pl.ds(0, 3)], [(src, dst, self.me.plus(x=d)) for d in OTHERS])
        act(pltpu.make_async_copy(src, dst, self.ls.at[q, 2]))

    def second(self, act, slot, q):
        me = self.me
        g, u = (f.at[slot, me.y, :, me.z] for f in (self.gf, self.uf))
        whole = self.gf.at[slot, pl.ds(0, 3), :, pl.ds(0, 2)]
        self._go(act, q, 2, whole, [c for d in OTHERS for c in ((g, g, me.plus(y=d)), (u, u, me.plus(z=d)))])

    def third(self, act, slot, q):
        me = self.me
        g, u = self.gf.at[slot, :, :, me.z], self.uf.at[slot, me.y]
        self._go(act, q, 3, self.gf.at[slot, pl.ds(0, 3)], [(g, g, me.plus(z=d)) for d in OTHERS])
        self._go(act, q, SIDE, self.uf.at[slot, pl.ds(0, 3)], [(u, u, me.plus(y=d)) for d in OTHERS])

    def load(self, act, slot, v, sem):
        load(act, (self.gf, self.uf, self.df), slot, v, sem)


def load(act, f, slot, v, sem):
    src, to = slot
    for i in range(3):
        act(pltpu.make_async_copy(f[i].at[src], v[i].at[to], sem.at[i]))


def gather_scratch(chunks):
    return [DMA((chunks, Gather.SEMS)), DMA((chunks, Gather.SEMS)), DMA((chunks, 3))]


def matrix(v, slot):
    return jnp.concatenate([v[slot, u].reshape(D, LANES) for u in range(SIDE)], axis=1)


class Reduce:
    @staticmethod
    def scratch():
        v = pltpu.VMEM
        held = lambda *s: v(s, BF)
        came = lambda *s: v((PAIR, UNITS) + s, BF)
        return [
            held(*SLICED), held(*SLICED), held(*BLOCKS),
            came(8, SIDE, PART, LANES), came(SIDE, 8, PART, LANES), came(LANES, D),
            held(8, SIDE, PART, LANES), held(SIDE, 8, PART, LANES), held(LANES, D),
            came(8, PART, LANES), came(8, PART, LANES), came(PART, D),
            held(8, PART, LANES), held(8, PART, LANES), held(PART, D),
            v((PAIR, 8, PART, LANES), BF), v((PAIR, 8, PART, LANES), BF), came(PART, QUARTER),
            held(PAIR, PAIR, PART, LANES), held(PAIR, PAIR, PART, LANES), held(PAIR, PART, QUARTER),
            DMA((PAIR, SIDE, UNITS)), DMA((PAIR, SIDE, UNITS)), DMA((SIDE, UNITS)), DMA((SIDE, UNITS)), DMA((PAIR, UNITS)),
        ]

    def __init__(self, me, scratch, out):
        self.me, self.out = me, out
        self.w, self.r1, self.b1, self.r2, self.b2, self.r3, self.b3 = (scratch[3 * i : 3 * i + 3] for i in range(7))
        self.ss, self.rs, self.sl, self.rl, self.ls = scratch[-5:]

    def put(self, g, u, d):
        for w, acc in ((self.w[0], g), (self.w[1], u)):
            for i in range(SIDE):
                w[i] = acc[:, LANES * i : LANES * (i + 1)].astype(BF).reshape(8, SIDE, PART, LANES)
        self.w[2][...] = d[...].astype(BF).reshape(BLOCKS)

    def copies(self, stage, slot, q):
        me = self.me
        (g, u, d), row, col = self.out, block(me.y, PART), block(me.z, QUARTER)
        if stage == 1:
            for n, by in enumerate(OTHERS):
                y, z, x = (me.along(a, by) for a in ("y", "z", "x"))
                yield self.w[0].at[y], self.r1[0].at[q, n], me.plus(y=by)
                yield self.w[1].at[:, :, z], self.r1[1].at[q, n], me.plus(z=by)
                yield self.w[2].at[x], self.r1[2].at[q, n], me.plus(x=by)
        elif stage == 2:
            for n, by in enumerate(OTHERS):
                y, z = (me.along(a, by) for a in ("y", "z"))
                yield self.b1[0].at[:, z], self.r2[0].at[q, n], me.plus(z=by)
                yield self.b1[1].at[y], self.r2[1].at[q, n], me.plus(y=by)
                yield self.b1[2].at[block(y, PART)], self.r2[2].at[q, n], me.plus(y=by)
        elif stage == 3:
            for dx, dc in ROW:
                x, c = me.along("x", dx), lax.rem(me.core + dc, 2)
                for i in range(2):
                    yield self.b2[i].at[2 * x + c], self.r3[i].at[q, me.xc], me.plus(x=dx, core=dc)
            for n, by in enumerate(OTHERS):
                cols = block(me.along("z", by), QUARTER)
                yield self.b2[2].at[:, cols], self.r3[2].at[q, n], me.plus(z=by)
        elif stage == 4:
            for by in OTHERS:
                yield self.b3[0].at[q], g.at[slot, :, me.y, me.z], me.plus(z=by)
                yield self.b3[1].at[q], u.at[slot, :, me.y, me.z], me.plus(y=by)
                yield self.b3[2].at[q], d.at[slot, row, col], me.plus(y=by)
        else:
            for by in OTHERS:
                yield g.at[slot, :, me.y], g.at[slot, :, me.y], me.plus(y=by)
                yield u.at[slot, :, :, me.z], u.at[slot, :, :, me.z], me.plus(z=by)
                yield d.at[slot, :, col], d.at[slot, :, col], me.plus(z=by)

    def sems(self, stage, slot, q, i):
        if stage > SIDE:
            return self.sl.at[slot % SIDE, i], self.rl.at[slot % SIDE, i]
        return self.ss.at[q, stage - 1, i], self.rs.at[q, stage - 1, i]

    def send(self, stage, act, slot, q):
        me = self.me
        if act is START:
            for n, (src, dst, to) in enumerate(self.copies(stage, slot, q)):
                i = n % 3 if stage != 3 else n % 2 if n < 2 * len(ROW) else 2
                remote(src, dst, *self.sems(stage, slot, q, i), to).start()
        else:
            for i in range(3):
                whole = (self.r1, self.r2, self.r3, self.r3, self.r2)[stage - 1][i].at[q]
                if stage in (3, SIDE) and i < 2:
                    whole = self.r3[i].at[q, pl.ds(0, len(ROW) if stage == 3 else 6)]
                for sem in self.sems(stage, slot, q, i):
                    wait_for(whole, sem)
        if stage == SIDE:
            g, u, d = self.out
            ends = g.at[slot, :, me.y, me.z], u.at[slot, :, me.y, me.z], d.at[slot, block(me.y, PART), block(me.z, QUARTER)]
            for i, dst in enumerate(ends):
                act(pltpu.make_async_copy(self.b3[i].at[q], dst, self.ls.at[q, i]))

    def add(self, stage, q):
        me = self.me
        cols = block(me.z, QUARTER)
        if stage == 3:
            for r, b, own in zip(self.r3[:2], self.b3, self.b2):
                r[q, me.xc] = own[me.xc]
                for c in range(2):
                    total = r[q, c].astype(F32)
                    for x in OTHERS:
                        total += r[q, 2 * x + c].astype(F32)
                    b[q, c] = total.astype(BF)
            parts = ((self.b2[2].at[:, cols], self.r3[2], self.b3[2].at[q]),)
        elif stage == 2:
            own = self.b1[0].at[:, me.z], self.b1[1].at[me.y], self.b1[2].at[block(me.y, PART)]
            parts = zip(own, self.r2, self.b2)
        else:
            own = self.w[0].at[me.y], self.w[1].at[:, :, me.z], self.w[2].at[me.x]
            parts = zip(own, self.r1, self.b1)
        for own, r, b in parts:
            total = own[...].astype(F32)
            for n in range(3):
                total += r[q, n].astype(F32)
            b[...] = total.astype(BF)

    def turn(self, stage, slot, q):
        self.send(stage, WAIT, slot, q)
        if stage < SIDE:
            self.add(stage, q)
        self.send(stage + 1, START, slot, q)


def reduced_shapes(n):
    s = jax.ShapeDtypeStruct((n, 2, SIDE, SIDE, PART, LANES), BF)
    return [s, s, jax.ShapeDtypeStruct((n, LANES, D), BF)]


def gathered_shapes(n):
    s = jax.ShapeDtypeStruct((n,) + SLICED, BF)
    return [s, s, jax.ShapeDtypeStruct((n,) + BLOCKS, BF)]


def chunk_buffers():
    return [pltpu.VMEM((2,) + SLICED, BF)] * 2 + [pltpu.VMEM((2,) + BLOCKS, BF)]


def tile_of(i):
    k, t = i // TILES, i % TILES
    return jnp.where(k == CHUNKS - 1, (t + MINE) % TILES, t)


def rows_of(tile):
    return block(tile, TILE)


def params(collective_id):
    return pltpu.CompilerParams(collective_id=collective_id, has_side_effects=True, vmem_limit_bytes=67_000_000, dimension_semantics=("arbitrary",))


def forward_kernel(x, dy, wg, wu, wd, g_out, u_out, a_out, h_out, n_out, dys, gf, uf, df, a, xv, acc, prt, held, vg, vu, vd, ss, rs, ls, wsem, csem, esem, psem, dsem):
    i = pl.program_id(0)
    k, t = i // TILES, i % TILES
    me = Place()
    ga = Gather(me, (wg, wu, wd), (gf, uf, df), (ss, rs, ls))
    v = (vg, vu, vd)
    early = Gather(me, (wg, wu, wd), v, (ss, rs, ls))
    save_d = pltpu.make_async_copy(vd.at[0], df.at[0], csem.at[3])
    other = me.plus(core=1)
    mine, theirs = block(0, OWN), block(1, OWN)
    to_dy = remote(dy, dys.at[theirs], *pair(esem, 0), other)

    def stage(out, j):
        s = j % 2
        if out:
            return pltpu.make_async_copy(held.at[s], dys.at[block(j, QUARTER)], dsem.at[1, s])
        return pltpu.make_async_copy(dy.at[block(j, QUARTER)], held.at[s], dsem.at[0, s])

    to_a = remote(a.at[mine], a.at[theirs], *pair(esem, 1), other)
    save_a = pltpu.make_async_copy(a, a_out, csem.at[0])

    def spread(m, act, stage):
        to = getattr(early if isinstance(m, int) and m == 0 else ga, stage)
        if stage in ("first", "down"):
            to(act, m // CHUNKS, m % CHUNKS, m, m)
        else:
            to(act, m, m)

    def part(tile):
        return remote(acc.at[rows_of(tile)], prt.at[rows_of(tile - MINE)], *pair(psem, tile - MINE), other)

    @pl.when(i == 0)
    def _():
        fetch = pltpu.make_async_copy(x, xv, csem.at[1])
        fetch.start()
        greet(me)
        for m in range(3):
            spread(m, START, "first")
        spread(0, START, "down")
        for m in range(3, CHUNKS + 1):
            spread(m, START, "first")
        spread(1, START, "down")
        fetch.wait()

        def norm(j, _):
            r = block(j, QUARTER)
            a[r] = normed(xv[r])
            return 0

        lax.fori_loop(0, PIECES, norm, 0)
        spread(0, WAIT, "first")
        spread(0, START, "second")
        to_a.start()
        spread(1, WAIT, "first")
        spread(1, START, "second")
        spread(0, WAIT, "second")
        spread(0, START, "third")
        spread(2, WAIT, "first")
        spread(2, START, "second")
        spread(1, WAIT, "second")
        spread(1, START, "third")
        spread(0, WAIT, "third")
        spread(0, WAIT, "down")
        save_d.start()

    @when(t == 0)
    def _():
        @when(k < CHUNKS - 1)
        def _():
            spread(k + 2, START, "down")

        @when(k > 0)
        def _():
            ga.load(WAIT, (k, k % 2), v, wsem)

        @when(k == 1)
        def _():
            save_d.wait()

    @when(t == 1, k < 3)
    def _():
        @when(k < 2)
        def _():
            spread(k + 3, WAIT, "first")
            spread(k + 3, START, "second")

        spread(k + 2, WAIT, "second")
        spread(k + 2, START, "third")

    @pl.when(i == MINE)
    def _():
        to_a.wait()
        save_a.start()
        to_dy.start()

    j = i - MINE

    @when(j >= 2, j < PIECES)
    def _():
        stage(True, j - 2).wait()

    @when(j >= 0, j < PIECES)
    def _():
        stage(False, j).start()

    @when(j >= 1, j <= PIECES)
    def _():
        stage(False, j - 1).wait()
        stage(True, j - 1).start()


    @when(t == TILES - 1, k < CHUNKS - 1)
    def _():
        spread(k + 1, WAIT, "third")
        spread(k + 1, WAIT, "down")
        ga.load(START, (k + 1, (k + 1) % 2), v, wsem)

    @when(k == CHUNKS - 1, t >= 1, t <= MINE)
    def _():
        part(t - 1 + MINE).start()

    tile = tile_of(i)
    rows = rows_of(tile)
    s = k % 2
    at = a[rows]
    g = nn(at, matrix(vg, s))
    u = nn(at, matrix(vu, s))
    g_out[0] = g
    u_out[0] = u
    hidden = (g * sigmoid(g) * u).astype(BF)
    acc[rows] = jnp.where(k == 0, 0.0, acc[rows]) + nn(hidden, vd[s].reshape(WIDE, D))

    @pl.when(i == CHUNKS * TILES - 1)
    def _():
        save_a.wait()
        for j in range(MINE):
            part(MINE + j).wait()

        keep = pltpu.make_async_copy(xv, h_out, csem.at[1])
        keep_n = pltpu.make_async_copy(a.at[mine], n_out, csem.at[2])

        def end(j, _):
            r = block(j, QUARTER)
            h = (xv[r].astype(F32) + (acc[r] + prt[r]).astype(BF).astype(F32)).astype(BF)
            xv[r] = h
            a[r] = normed(h)
            pltpu.make_async_copy(xv.at[r], h_out.at[r], csem.at[1]).start()
            pltpu.make_async_copy(a.at[r], n_out.at[r], csem.at[2]).start()
            return 0

        lax.fori_loop(0, PIECES, end, 0)
        to_dy.wait()
        for j in (2, 1):
            stage(True, PIECES - j).wait()
        spread(CHUNKS, WAIT, "third")
        spread(CHUNKS, WAIT, "down")
        keep.wait()
        keep_n.wait()


def forward(x, dy, weights):
    steps = CHUNKS * TILES
    wide = pl.BlockSpec((1, TILE, WIDE), lambda i: (i // TILES, tile_of(i), 0))
    big = jax.ShapeDtypeStruct((CHUNKS, TOKENS, WIDE), F32)
    own = jax.ShapeDtypeStruct((OWN, D), BF)
    return pl.pallas_call(
        forward_kernel,
        grid=(steps,),
        in_specs=[ANY] * 5,
        out_specs=[wide, wide] + [ANY] * 7,
        out_shape=[big, big, jax.ShapeDtypeStruct((TOKENS, D), BF), own, own, jax.ShapeDtypeStruct((TOKENS, D), BF)] + gathered_shapes(CHUNKS + 1),
        scratch_shapes=[
            pltpu.VMEM((TOKENS, D), BF), pltpu.VMEM((OWN, D), BF), pltpu.VMEM((TOKENS, D), F32), pltpu.VMEM((OWN, D), F32), pltpu.VMEM((2, QUARTER, D), BF),
            *chunk_buffers(), *gather_scratch(CHUNKS + 1), DMA((3,)), DMA((4,)), DMA((2, 2)), DMA((2, MINE)), DMA((2, 2)),
        ],
        compiler_params=params(1),
        name="forward",
    )(x, dy, *weights)


def gradients_of(g, u, dh):
    s = sigmoid(g)
    si = g * s
    return (si * u).astype(BF), (dh * u * (s + si * (1 - s))).astype(BF), (dh * si).astype(BF)


def middle_kernel(dy, dys, h, n, g4, u4, d4, wg, wu, wd, dh, dar, rg, ru, rd, kg, ku, kd, gf, uf, df, *scratch):
    a, da, ag, au, ad, vg, vu, vd, ss, rs, ls, wsem, csem, esem, psem, dsem, *rest = scratch
    i = pl.program_id(0)
    k, t = i // TILES, i % TILES
    me = Place()
    ga = Gather(me, (wg, wu, wd), (gf, uf, df), (ss, rs, ls))
    re = Reduce(me, rest, (rg, ru, rd))
    v = (vg, vu, vd)
    other = me.plus(core=1)
    mine, theirs = block(0, OWN), block(1, OWN)
    to_a = remote(n, a.at[theirs], *pair(esem, 0), other)
    last = CHUNKS - 1

    def part(tile):
        return remote(da.at[rows_of(tile)], dar.at[rows_of(tile - MINE)], *pair(psem, tile - MINE), other)

    def bring(stage, act, c):
        if stage in ("first", "down"):
            getattr(ga, stage)(act, 1, c + 1, c, c)
        else:
            getattr(ga, stage)(act, c, c)

    @when(i == 0)
    def _():
        fetch = pltpu.make_async_copy(n, a.at[mine], csem.at[0])
        fetch.start()
        load(START, (g4, u4, d4), (CHUNKS, 0), v, wsem)
        greet(me)
        to_a.start()
        for c in range(last):
            bring("first", START, c)
        bring("down", START, 0)
        fetch.wait()
        load(WAIT, (g4, u4, d4), (CHUNKS, 0), v, wsem)

    now, before, q = k - 1, k - 2, k % 2

    @when(t == 0, k > 0)
    def _():
        ga.load(WAIT, (k - 1, k % 2), v, wsem)

        @when(k > 1)
        def _():
            re.turn(3, before, 1 - q)

        re.send(1, START, now, q)

    @when(t == 1, k > 1)
    def _():
        re.turn(4, before, 1 - q)

    for stage in (1, 2):

        @when(t == stage + 1, k > 0)
        def _(stage=stage):
            re.turn(stage, now, q)

    @when(t == 3, k > 1)
    def _():
        re.send(5, WAIT, before, 1 - q)

    @when(i == 1)
    def _():
        for c in range(last):
            bring("first", WAIT, c)
            bring("second", START, c)

    @when(i == MINE)
    def _():
        to_a.wait()
        bring("second", WAIT, 0)
        bring("third", START, 0)
        bring("down", START, 1)

    @when(i == TILES - 1)
    def _():
        for c in range(1, last):
            bring("second", WAIT, c)
        bring("third", START, 1)

    @when(i == TILES + 1)
    def _():
        bring("third", WAIT, 1)
        bring("down", WAIT, 1)
        bring("down", START, 2)

    @when(i == 2 * TILES - 1)
    def _():
        bring("third", START, 2)

    @when(i == 2 * TILES + 2)
    def _():
        bring("third", WAIT, 2)
        bring("down", WAIT, 2)

    @when(t == TILES - 1, k > 0, k < last)
    def _():
        ga.load(START, (k, (k + 1) % 2), v, wsem)

    @when(k == last, t >= 1, t <= MINE)
    def _():
        part(t - 1 + MINE).start()

    tile = tile_of(i)
    rows = rows_of(tile)
    s = k % 2
    at = a[rows]
    by = dy[...]
    mg, mu, md = matrix(vg, s), matrix(vu, s), vd[s].reshape(WIDE, D)
    parts = [gradients_of(nn(at, mg[:, c]), nn(at, mu[:, c]), nt(by, md[c]).astype(BF).astype(F32)) for c in HALVES]
    sum_up(t == 0, (ag, au, ad), at, by, parts)
    dg, du = (jnp.concatenate([p[j] for p in parts], axis=1) for j in (1, 2))
    da[rows] = jnp.where(k == 0, 0, da[rows]) + (nt(dg, mg) + nt(du, mu))

    @when(i == TILES - 1)
    def _():
        bring("third", WAIT, 0)
        bring("down", WAIT, 0)
        ga.load(START, (0, 1), v, wsem)

    @when(t == TILES - 1)
    def _():
        re.put(ag, au, ad)

    @when(i == CHUNKS * TILES - 1)
    def _():
        re.turn(3, last - 1, last % 2)
        outs = [pltpu.make_async_copy(re.w[j], (kg, ku, kd)[j], wsem.at[j]) for j in range(3)]
        for o in outs:
            o.start()
        for j in range(MINE):
            part(MINE + j).wait()

        def piece(act, j):
            r, s = block(j, LANES), j % SIDE
            for n, (src, dst) in enumerate(((dar, ad.at[block(s, LANES)]), (h, vd.at[0, s]), (dys, vd.at[1, s]))):
                act(pltpu.make_async_copy(src.at[r], dst, dsem.at[s, n]))

        count = OWN // LANES
        for j in range(SIDE - 1):
            piece(START, j)

        def one(j, _):
            @when(j + SIDE - 1 < count)
            def _():
                piece(START, j + SIDE - 1)

            piece(WAIT, j)
            r, s = block(j, LANES), j % SIDE
            by_h = norm_back(vd[0, s], (da[r] + ad[block(s, LANES)]).astype(BF))
            a[r] = (vd[1, s].astype(F32) + by_h.astype(F32)).astype(BF)
            pltpu.make_async_copy(a.at[r], dh.at[r], csem.at[0]).start()
            return 0

        lax.fori_loop(0, count, one, 0)
        for o in outs:
            o.wait()
        re.send(SIDE, WAIT, last - 1, last % 2)
        pltpu.make_async_copy(a.at[mine], dh, csem.at[0]).wait()


def middle(dy, h, n, f4, weights):
    raw = jax.ShapeDtypeStruct(SLICED, BF)
    outs = [jax.ShapeDtypeStruct((OWN, D), BF), jax.ShapeDtypeStruct((OWN, D), F32), *reduced_shapes(SLOTS), raw, raw, jax.ShapeDtypeStruct(BLOCKS, BF)]
    shapes = outs + gathered_shapes(CHUNKS - 1)
    return pl.pallas_call(
        middle_kernel,
        grid=(CHUNKS * TILES,),
        in_specs=[pl.BlockSpec((TILE, D), lambda i: (tile_of(i), 0))] + [ANY] * 9,
        out_specs=[ANY] * len(shapes),
        out_shape=shapes,
        scratch_shapes=[
            pltpu.VMEM((TOKENS, D), BF), pltpu.VMEM((TOKENS, D), F32), *sums(),
            *chunk_buffers(), *gather_scratch(CHUNKS - 1), DMA((3,)), DMA((1,)), DMA((2, 1)), DMA((2, MINE)),
            DMA((SIDE, 3)), *Reduce.scratch(),
        ],
        compiler_params=params(2),
        name="middle",
    )(dy, dy, h, n, *f4, *weights)[: len(outs)]


def sum_up(fresh, sums_, at, by, parts):
    ag, au, ad = sums_
    for c, (hidden, dg, du) in zip(HALVES, parts):
        ag[:, c] = jnp.where(fresh, 0, ag[:, c]) + tn(at, dg)
        au[:, c] = jnp.where(fresh, 0, au[:, c]) + tn(at, du)
        ad[c] = jnp.where(fresh, 0, ad[c]) + tn(hidden, by)


def sums():
    return [pltpu.VMEM((D, WIDE), F32), pltpu.VMEM((D, WIDE), F32), pltpu.VMEM((WIDE, D), F32)]


def back_kernel(g_in, u_in, a_in, down, dh, kg, ku, kd, *refs):
    sums_, scratch = refs[3:6], refs[6:]
    b, ag, au, ad, csem, esem, *scratch = scratch
    i = pl.program_id(0)
    k, t = i // TILES, i % TILES
    me = Place()
    re = Reduce(me, scratch, sums_)
    to_b = remote(dh, b.at[block(1, OWN)], *pair(esem, 0), me.plus(core=1))
    begun = CHUNKS - 1

    @when(i == 0)
    def _():
        raws = [pltpu.make_async_copy((kg, ku, kd)[j], re.w[j], csem.at[j]) for j in range(3)]
        raws.append(pltpu.make_async_copy(dh, b.at[block(0, OWN)], csem.at[3]))
        for o in raws:
            o.start()
        greet(me)
        to_b.start()
        for o in raws:
            o.wait()
        re.send(1, START, begun, 0)
        re.send(5, START, begun - 1, 1)

    @when(i == MINE)
    def _():
        to_b.wait()

    now, before, q = begun + k, begun + k - 1, k % 2

    @when(t == 0, k > 0)
    def _():
        re.send(1, START, now, q)

    @when(t == 1, k > 0)
    def _():
        re.turn(2, before, 1 - q)

        @when(k == 3)
        def _():
            re.send(5, WAIT, before - 2, 1 - q)

        @when(k > 1)
        def _():
            re.turn(4, before - 1, q)

    @when(t == 3)
    def _():
        @when(k == 1)
        def _():
            re.send(5, WAIT, before - 1, q)

        re.turn(1, now, q)

        @when(k > 0)
        def _():
            re.turn(3, before, 1 - q)

    at, by = a_in[...], b[rows_of(tile_of(i))]
    md = down[0].reshape(WIDE, D)
    parts = [gradients_of(g_in[0, :, c], u_in[0, :, c], nt(by, md[c]).astype(BF).astype(F32)) for c in HALVES]
    sum_up(t == 0, (ag, au, ad), at, by, parts)

    @when(t == TILES - 1)
    def _():
        re.put(ag, au, ad)

    @when(i == CHUNKS * TILES - 1)
    def _():
        end = SLOTS - 1
        q, p = CHUNKS % 2, 1 - CHUNKS % 2
        re.send(1, START, end, q)
        re.send(5, WAIT, end - 3, p)
        re.turn(2, end - 1, p)
        re.turn(4, end - 2, q)
        re.turn(1, end, q)
        re.turn(3, end - 1, p)
        re.turn(2, end, q)
        re.turn(4, end - 1, p)
        re.send(5, WAIT, end - 2, q)
        re.turn(3, end, q)
        re.turn(4, end, q)
        re.send(5, WAIT, end - 1, p)
        re.send(5, WAIT, end, q)


def backward(g, u, a, down, dh, raw, sums_):
    wide = pl.BlockSpec((1, TILE, WIDE), lambda i: (i // TILES, tile_of(i), 0))
    blocks = [wide, wide, pl.BlockSpec((TILE, D), lambda i: (tile_of(i), 0)), pl.BlockSpec((1,) + BLOCKS, lambda i: (i // TILES, 0, 0, 0))]
    args = (g, u, a, down, dh, *raw, *sums_)
    at = len(args) - len(sums_)
    return pl.pallas_call(
        back_kernel,
        grid=(CHUNKS * TILES,),
        in_specs=blocks + [ANY] * (len(args) - len(blocks)),
        out_specs=[ANY] * len(sums_),
        out_shape=reduced_shapes(SLOTS),
        input_output_aliases={at + i: i for i in range(len(sums_))},
        scratch_shapes=[
            pltpu.VMEM((TOKENS, D), BF), *sums(), DMA((4,)), DMA((2, 1)), *Reduce.scratch(),
        ],
        compiler_params=params(3),
        name="backward",
    )(*args)


def adamw(w, m, v, g):
    m = 0.9 * m + 0.1 * g
    v = 0.95 * v + 0.05 * g * g
    step = m * lax.rsqrt(v + 1e-8) + 0.1 * w
    return (w - 0.02 * step).astype(BF), m, v


def update_kernel(gg, gu, gd, *refs):
    ins, outs = refs[:9], refs[9:]

    def one(n, at, g):
        w, m, v = (r[at] for r in ins[n::3])
        for out, new in zip(outs[n::3], adamw(w.astype(F32), m, v, g.astype(F32))):
            out[at] = new

    for u in range(2):
        for n, r in enumerate((gg, gu)):
            g = jnp.concatenate([r[k, c, u].reshape(LANES, LANES) for c in range(2) for k in range(CHUNKS)], axis=1)
            one(n, (0, slice(None), slice(u * D, u * D + D)), g)
        one(2, (0, slice(u * LANES, u * LANES + LANES)), gd[u])


def update(sums_, arrays):
    side = pl.BlockSpec((1, LANES, 2 * D), lambda i: (i // 2, 0, i % 2))
    deep = pl.BlockSpec((1, 2 * LANES, D), lambda i: (i // 2, i % 2, 0))
    part = pl.BlockSpec((CHUNKS, 2, 2, SIDE, PART, LANES), lambda i: (1 - i // 2, 0, i % 2, 0, 0, 0))
    down = pl.BlockSpec((2, LANES, D), lambda i: (2 - i // 2 * 2 + i % 2, 0, 0))
    return pl.pallas_call(
        update_kernel,
        grid=(SIDE,),
        in_specs=[part, part, down] + [side, side, deep] * 3,
        out_specs=[side, side, deep] * 3,
        out_shape=[jax.ShapeDtypeStruct(x.shape, x.dtype) for x in arrays],
        compiler_params=pltpu.CompilerParams(vmem_limit_bytes=67_000_000, dimension_semantics=("arbitrary",)),
        name="update",
    )(*sums_, *arrays)


def solution(mesh):
    fine = Mesh(mesh.devices.reshape(SIDE, SIDE, SIDE, 2), AXES)

    def step(x, dy, *arrays):
        x, dy, weights = x[0], dy[0], arrays[:3]
        g0, u0, a0, h1, n1, dys, *f = forward(x, dy, weights)
        dh, _, *rest = middle(dys, h1, n1, f, weights)
        return update(backward(g0, u0, a0, f[2], dh, rest[3:], rest[:3]), arrays)

    states, cut = P(AXES, None, None), P(None, ("x", "core"), None)
    return jax.shard_map(
        step,
        mesh=fine,
        in_specs=(states, states) + (cut,) * 9,
        out_specs=(cut,) * 9,
        check_vma=False,
    )
```
